16 devices in a mesh: tp: 4 (over z, y), cp: 4 (over x, core).
Axes of the slice: x: 2, y: 2, z: 2, core: 2. Of those that a mesh axis runs over, the one named last changes fastest.
Arguments:
- x_in: bfloat16 [8, 512, 1024], P(None, 'cp')
- d_y: bfloat16 [8, 512, 1024], P(None, 'cp')
- key_mask: int32 [8, 512], P(None, 'cp')
- rel_bias: float32 [32, 16], P(None, 'tp')
- g_attn: float32 [2, 1024], replicated
- g_mlp: float32 [2, 1024], replicated
- w_q: bfloat16 [2, 1024, 1024], P(None, None, 'tp')
- w_k: bfloat16 [2, 1024, 1024], P(None, None, 'tp')
- w_v: bfloat16 [2, 1024, 1024], P(None, None, 'tp')
- w_o: bfloat16 [2, 1024, 1024], P(None, 'tp')
- w_gate: bfloat16 [2, 1024, 2816], P(None, None, 'tp')
- w_lin: bfloat16 [2, 1024, 2816], P(None, None, 'tp')
- w_out: bfloat16 [2, 2816, 1024], P(None, 'tp')
Outputs:
- output 1: bfloat16 [8, 512, 1024], P(None, 'cp')
- output 2: float32 [32, 16], P(None, 'tp')
- output 3: float32 [2, 1024], replicated
- output 4: float32 [2, 1024], replicated
- output 5: bfloat16 [2, 1024, 1024], P(None, None, 'tp')
- output 6: bfloat16 [2, 1024, 1024], P(None, None, 'tp')
- output 7: bfloat16 [2, 1024, 1024], P(None, None, 'tp')
- output 8: bfloat16 [2, 1024, 1024], P(None, 'tp')
- output 9: bfloat16 [2, 1024, 2816], P(None, None, 'tp')
- output 10: bfloat16 [2, 1024, 2816], P(None, None, 'tp')
- output 11: bfloat16 [2, 2816, 1024], P(None, 'tp')
All inputs are finite; a program needn't handle non-finite values.
Results may differ from the reference program's by a relative error of at most 0.02.
Values are sent between devices in bfloat16 or wider.
A program may use at most 1 GiB of HBM per device.

```python
import jax
import jax.numpy as jnp
from jax import lax

BATCH_SIZE = 8
SEQ_LEN = 512
D_MODEL = 1024
N_HEADS = 16
HEAD_DIM = 64
FF_DIM = 2816
N_LAYERS = 2
NUM_BUCKETS = 32
MAX_DISTANCE = 128
QUERY_ROWS = 128
NORM_EPS = 1e-6
MASK_NEG = -1e9


def rel_bucket(rel_pos):
    distance = jnp.minimum(jnp.abs(rel_pos), MAX_DISTANCE)
    distance_sq = distance * distance
    log_part = 8 + sum((distance_sq >= 64 * 2 ** power).astype(jnp.int32) for power in range(1, 8))
    return jnp.where(distance < 8, distance, log_part) + 16 * (rel_pos > 0).astype(jnp.int32)


def rms_scale(x_f, gain):
    inv_rms = lax.rsqrt(jnp.mean(x_f * x_f, axis=-1, keepdims=True) + NORM_EPS)
    return (x_f * inv_rms * gain).astype(jnp.bfloat16)


def mat_f32(lhs, rhs):
    return jnp.dot(lhs.astype(jnp.float32), rhs.astype(jnp.float32))


def attention(queries, key_rows, val_rows, rel_bias, key_add):
    q_f = queries.astype(jnp.float32)
    k_f = key_rows.astype(jnp.float32)
    v_f = val_rows.astype(jnp.float32)
    n_blocks = SEQ_LEN // QUERY_ROWS
    q_blocks = jnp.moveaxis(q_f.reshape(BATCH_SIZE, n_blocks, QUERY_ROWS, N_HEADS, HEAD_DIM), 1, 0)
    key_pos = jnp.arange(SEQ_LEN)
    bias_table = rel_bias.T

    def one_block(block_args):
        q_blk, start = block_args
        rel_pos = key_pos[None, :] - (start + jnp.arange(QUERY_ROWS))[:, None]
        bias = jnp.take(bias_table, rel_bucket(rel_pos), axis=1)
        scores = jnp.einsum('bqhd,bkhd->bhqk', q_blk, k_f) + bias[None] + key_add[:, None, None, :]
        probs = jax.nn.softmax(scores, axis=-1)
        return jnp.einsum('bhqk,bkhd->bqhd', probs, v_f)

    outs = lax.map(jax.checkpoint(one_block), (q_blocks, jnp.arange(n_blocks) * QUERY_ROWS))
    return jnp.moveaxis(outs, 0, 1).reshape(BATCH_SIZE, SEQ_LEN, N_HEADS * HEAD_DIM).astype(jnp.bfloat16)


def encoder_layer(hidden, weights, rel_bias, key_add):
    g_attn, g_mlp, w_q, w_k, w_v, w_o, w_gate, w_lin, w_out = weights
    head_shape = (BATCH_SIZE, SEQ_LEN, N_HEADS, HEAD_DIM)
    x_f = hidden.astype(jnp.float32)
    h_attn = rms_scale(x_f, g_attn)
    queries = mat_f32(h_attn, w_q).astype(jnp.bfloat16).reshape(head_shape)
    key_rows = mat_f32(h_attn, w_k).astype(jnp.bfloat16).reshape(head_shape)
    val_rows = mat_f32(h_attn, w_v).astype(jnp.bfloat16).reshape(head_shape)
    attn_flat = attention(queries, key_rows, val_rows, rel_bias, key_add)
    after_attn = (x_f + mat_f32(attn_flat, w_o)).astype(jnp.bfloat16)
    after_f = after_attn.astype(jnp.float32)
    h_mlp = rms_scale(after_f, g_mlp)
    gated = (jax.nn.gelu(mat_f32(h_mlp, w_gate), approximate=True) * mat_f32(h_mlp, w_lin)).astype(jnp.bfloat16)
    return (after_f + mat_f32(gated, w_out)).astype(jnp.bfloat16)


def setup_inputs(seed: int = 0) -> dict:
    base_key = jax.random.key(seed)
    sub_keys = jax.random.split(base_key, 13)
    width = N_HEADS * HEAD_DIM

    def normal(slot, shape, scale):
        return jax.random.normal(sub_keys[slot], shape, jnp.float32) * scale

    lengths = jax.random.randint(sub_keys[2], (BATCH_SIZE,), SEQ_LEN // 2, SEQ_LEN + 1)
    last_row = jnp.logical_and(jnp.arange(BATCH_SIZE) == BATCH_SIZE - 1, BATCH_SIZE > 1)
    lengths = jnp.where(last_row, SEQ_LEN // 2, lengths)
    key_mask = (jnp.arange(SEQ_LEN)[None, :] < lengths[:, None]).astype(jnp.int32)
    return {
        'x_in': normal(0, (BATCH_SIZE, SEQ_LEN, D_MODEL), 1.0).astype(jnp.bfloat16),
        'd_y': normal(1, (BATCH_SIZE, SEQ_LEN, D_MODEL), 1.0).astype(jnp.bfloat16),
        'key_mask': key_mask,
        'rel_bias': normal(3, (NUM_BUCKETS, N_HEADS), 1.0),
        'g_attn': 1.0 + normal(4, (N_LAYERS, D_MODEL), 0.3),
        'g_mlp': 1.0 + normal(5, (N_LAYERS, D_MODEL), 0.3),
        'w_q': normal(6, (N_LAYERS, D_MODEL, width), (D_MODEL * HEAD_DIM) ** -0.5).astype(jnp.bfloat16),
        'w_k': normal(7, (N_LAYERS, D_MODEL, width), D_MODEL ** -0.5).astype(jnp.bfloat16),
        'w_v': normal(8, (N_LAYERS, D_MODEL, width), D_MODEL ** -0.5).astype(jnp.bfloat16),
        'w_o': normal(9, (N_LAYERS, width, D_MODEL), width ** -0.5).astype(jnp.bfloat16),
        'w_gate': normal(10, (N_LAYERS, D_MODEL, FF_DIM), D_MODEL ** -0.5).astype(jnp.bfloat16),
        'w_lin': normal(11, (N_LAYERS, D_MODEL, FF_DIM), D_MODEL ** -0.5).astype(jnp.bfloat16),
        'w_out': normal(12, (N_LAYERS, FF_DIM, D_MODEL), FF_DIM ** -0.5).astype(jnp.bfloat16),
    }


def reference(x_in, d_y, key_mask, rel_bias, g_attn, g_mlp, w_q, w_k, w_v, w_o, w_gate, w_lin, w_out):
    key_add = jnp.where(key_mask > 0, 0.0, MASK_NEG).astype(jnp.float32)

    def forward(hidden, bias_tab, gain_a, gain_m, wq_all, wk_all, wv_all, wo_all, wg_all, wl_all, wf_all):
        def body(carry, weights):
            return encoder_layer(carry, weights, bias_tab, key_add), None
        final, _ = lax.scan(body, hidden, (gain_a, gain_m, wq_all, wk_all, wv_all, wo_all, wg_all, wl_all, wf_all))
        return final

    _, pull_back = jax.vjp(forward, x_in, rel_bias, g_attn, g_mlp, w_q, w_k, w_v, w_o, w_gate, w_lin, w_out)
    d_x, d_rel, d_gain_a, d_gain_m, d_wq, d_wk, d_wv, d_wo, d_wg, d_wl, d_wf = pull_back(d_y)
    return (d_x, d_rel, d_gain_a, d_gain_m, d_wq, d_wk, d_wv, d_wo, d_wg, d_wl, d_wf)
```

```python
import functools
import jax
import jax.numpy as jnp
from jax import lax
from jax.experimental import pallas as pl
from jax.experimental.pallas import tpu as pltpu
from jax.sharding import PartitionSpec as P

NORM_EPS = 1e-6
MASK_NEG = -1e9
HEAD = 64
F32 = jnp.float32
BF16 = jnp.bfloat16
NT = (((1,), (1,)), ((), ()))
TN = (((0,), (0,)), ((), ()))


def rel_bucket(rel_pos):
    distance = jnp.minimum(jnp.abs(rel_pos), 128)
    distance_sq = distance * distance
    log_part = 8 + sum((distance_sq >= 64 * 2 ** power).astype(jnp.int32) for power in range(1, 8))
    return jnp.where(distance < 8, distance, log_part) + 16 * (rel_pos > 0).astype(jnp.int32)


def bucket_onehot(seq):
    rel = jnp.arange(2 * seq) - seq
    return (rel_bucket(rel)[None, :] == jnp.arange(32)[:, None]) & (jnp.arange(2 * seq) > 0)[None, :]


def dot(a, b, dims=(((1,), (0,)), ((), ()))):
    return lax.dot_general(a, b, dims, preferred_element_type=F32)


def toeplitz(row, seq):
    base = pltpu.roll(row, seq, 1)
    rows = jnp.concatenate([base if i == 0 else pltpu.roll(base, i, 1) for i in range(8)], axis=0)
    size = 8
    while size < seq:
        rows = jnp.concatenate([rows, pltpu.roll(rows, size, 1)], axis=0)
        size *= 2
    return rows[:, :seq]


def diag_sums(mat, seq):
    wide = jnp.concatenate([mat, jnp.zeros_like(mat)], axis=1)
    size = seq
    while size > 1:
        half = size // 2
        wide = wide[:half] + pltpu.roll(wide[half:size], 2 * seq - half, 1)
        size = half
    return pltpu.roll(wide, seq, 1)


def attn_fwd_kernel(seq, batch, heads, x_ref, g_ref, wq_ref, wk_ref, wv_ref, t_ref, add_ref, h_ref, q_ref, k_ref, v_ref, o_ref, bias_ref):
    for blk in range(batch * seq // 256):
        rows = pl.ds(blk * 256, 256)
        xf = x_ref[rows, :].astype(F32)
        inv = lax.rsqrt(jnp.mean(xf * xf, axis=-1, keepdims=True) + NORM_EPS)
        h = (xf * inv * g_ref[...]).astype(BF16)
        h_ref[rows, :] = h
        q_ref[rows, :] = dot(h, wq_ref[...]).astype(BF16)
        k_ref[rows, :] = dot(h, wk_ref[...]).astype(BF16)
        v_ref[rows, :] = dot(h, wv_ref[...]).astype(BF16)
    for head in range(heads):
        bias_ref[...] = toeplitz(t_ref[head:head + 1, :], seq)
        cols = pl.ds(head * HEAD, HEAD)
        for b in range(batch):
            rows = pl.ds(b * seq, seq)
            s = dot(q_ref[rows, cols], k_ref[rows, cols], NT) + bias_ref[...] + add_ref[b:b + 1, :]
            e = jnp.exp(s - jnp.max(s, axis=-1, keepdims=True))
            total = jnp.sum(e, axis=-1, keepdims=True)
            o_ref[rows, cols] = (dot(e.astype(BF16), v_ref[rows, cols]) / total).astype(BF16)


def attn_bwd_kernel(seq, batch, heads, dm_ref, wo_ref, q_ref, k_ref, v_ref, o_ref, t_ref, add_ref, dq_ref, dk_ref, dv_ref, dt_ref, bias_ref, dout_ref, acc_ref):
    for blk in range(batch * seq // 256):
        rows = pl.ds(blk * 256, 256)
        dout_ref[rows, :] = dot(dm_ref[rows, :], wo_ref[...], NT).astype(BF16)
    dt_ref[...] = jnp.zeros_like(dt_ref)
    for head in range(heads):
        bias_ref[...] = toeplitz(t_ref[head:head + 1, :], seq)
        cols = pl.ds(head * HEAD, HEAD)
        for b in range(batch):
            rows = pl.ds(b * seq, seq)
            q, k, v, do = q_ref[rows, cols], k_ref[rows, cols], v_ref[rows, cols], dout_ref[rows, cols]
            s = dot(q, k, NT) + bias_ref[...] + add_ref[b:b + 1, :]
            e = jnp.exp(s - jnp.max(s, axis=-1, keepdims=True))
            p = e * (1.0 / jnp.sum(e, axis=-1, keepdims=True))
            row_dot = jnp.sum(do.astype(F32) * o_ref[rows, cols].astype(F32), axis=-1, keepdims=True)
            ds = p * (dot(do, v, NT) - row_dot)
            if b == 0:
                acc_ref[...] = ds
            else:
                acc_ref[...] += ds
            dsl = ds.astype(BF16)
            dq_ref[rows, cols] = dot(dsl, k).astype(BF16)
            dk_ref[rows, cols] = dot(dsl, q, TN).astype(BF16)
            dv_ref[rows, cols] = dot(p.astype(BF16), do, TN).astype(BF16)
        dt_ref[head:head + 1, :] = diag_sums(acc_ref[...], seq)


def vmem_specs(n):
    return [pl.BlockSpec(memory_space=pltpu.VMEM)] * n


def attn_fwd(x, gain, w_q, w_k, w_v, table, key_add, seq):
    rows, width = x.shape
    cols = w_q.shape[1]
    batch, heads = rows // seq, cols // HEAD
    flops = 2 * rows * width * cols * 3 + 4 * rows * seq * cols
    return pl.pallas_call(
        functools.partial(attn_fwd_kernel, seq, batch, heads),
        out_shape=[jax.ShapeDtypeStruct(x.shape, BF16)] + [jax.ShapeDtypeStruct((rows, cols), BF16)] * 4,
        in_specs=vmem_specs(7), out_specs=vmem_specs(5),
        scratch_shapes=[pltpu.VMEM((seq, seq), F32)],
        compiler_params=pltpu.CompilerParams(vmem_limit_bytes=48 * 1024 * 1024),
        cost_estimate=pl.CostEstimate(flops=flops, bytes_accessed=8 << 20, transcendentals=0),
        name="attn_fwd",
    )(x, gain[None, :], w_q, w_k, w_v, table, key_add)


def attn_bwd(d_mid, w_o, q, k, v, o, table, key_add, seq):
    rows, cols = q.shape
    batch, heads = rows // seq, cols // HEAD
    flops = 2 * rows * d_mid.shape[1] * cols + 10 * rows * seq * cols
    return pl.pallas_call(
        functools.partial(attn_bwd_kernel, seq, batch, heads),
        out_shape=[jax.ShapeDtypeStruct((rows, cols), BF16)] * 3 + [jax.ShapeDtypeStruct(table.shape, F32)],
        in_specs=vmem_specs(8), out_specs=vmem_specs(4),
        scratch_shapes=[pltpu.VMEM((seq, seq), F32), pltpu.VMEM((rows, cols), BF16), pltpu.VMEM((seq, seq), F32)],
        compiler_params=pltpu.CompilerParams(vmem_limit_bytes=48 * 1024 * 1024),
        cost_estimate=pl.CostEstimate(flops=flops, bytes_accessed=8 << 20, transcendentals=0),
        name="attn_bwd",
    )(d_mid, w_o, q, k, v, o, table, key_add)


def rms(x, gain):
    xf = x.astype(F32)
    inv = lax.rsqrt(jnp.mean(xf * xf, axis=-1, keepdims=True) + NORM_EPS)
    return (xf * inv * gain).astype(BF16)


def scatter_sum(partial):
    return lax.psum_scatter(partial, 'tp', scatter_dimension=0, tiled=True)


def gather_rows(own):
    return lax.all_gather(own, 'tp', axis=0, tiled=True)


def own_rows(full, rows):
    return lax.dynamic_slice_in_dim(full, lax.axis_index('tp') * rows, rows, axis=0)


def fwd_sum(partial, residual):
    total = scatter_sum(partial)
    return gather_rows((own_rows(residual, total.shape[0]).astype(F32) + total).astype(BF16))


def bwd_sum(partial, x, gain, d_res):
    total = scatter_sum(partial)
    xf = own_rows(x, total.shape[0]).astype(F32)
    inv = lax.rsqrt(jnp.mean(xf * xf, axis=-1, keepdims=True) + NORM_EPS)
    normed = xf * inv
    d_gain = jnp.sum(total * normed, axis=0)
    d_normed = total * gain
    d_x = inv * (d_normed - normed * jnp.mean(d_normed * normed, axis=-1, keepdims=True))
    return gather_rows((d_x + own_rows(d_res, total.shape[0]).astype(F32)).astype(BF16)), d_gain


def mlp_up(x1, gain, w_gate, w_lin):
    h2 = rms(x1, gain)
    gate_pre, lin_pre = dot(h2, w_gate), dot(h2, w_lin)
    gated = (jax.nn.gelu(gate_pre, approximate=True) * lin_pre).astype(BF16)
    return h2, gate_pre, lin_pre, gated


def cp_sum(part):
    own = lax.psum_scatter(part, 'cp', scatter_dimension=0, tiled=True).astype(BF16)
    return lax.all_gather(own, 'cp', axis=0, tiled=True)


def solution(mesh):
    seq_spec = P(None, 'cp', None)
    col_spec = P(None, None, 'tp')
    row_spec = P(None, 'tp', None)
    weight_specs = (P(), P(), col_spec, col_spec, col_spec, row_spec, col_spec, col_spec, row_spec)
    cp_size = mesh.shape['cp']

    def local_program(x_in, d_y, key_mask, rel_bias, g_attn, g_mlp, w_q, w_k, w_v, w_o, w_gate, w_lin, w_out):
        batch, blk, width = x_in.shape
        seq = blk * cp_size
        layers = w_q.shape[0]
        own_batch = batch // cp_size

        def to_batch(arr):
            return lax.all_to_all(arr, 'cp', split_axis=0, concat_axis=1, tiled=True).reshape(own_batch * seq, width)

        x = to_batch(x_in)
        dy = to_batch(d_y)
        mask_all = lax.all_gather(key_mask, 'cp', axis=1, tiled=True)
        mask = lax.dynamic_slice_in_dim(mask_all, lax.axis_index('cp') * own_batch, own_batch, axis=0)
        key_add = jnp.where(mask > 0, 0.0, MASK_NEG).astype(F32)
        onehot = bucket_onehot(seq)
        table = jnp.sum(jnp.where(onehot[None], rel_bias.T[:, :, None], 0.0), axis=1)

        saved = []
        for l in range(layers):
            h, q, k, v, o = attn_fwd(x, g_attn[l], w_q[l], w_k[l], w_v[l], table, key_add, seq)
            x1 = fwd_sum(dot(o, w_o[l]), x)
            h2, gate_pre, lin_pre, gated = mlp_up(x1, g_mlp[l], w_gate[l], w_lin[l])
            saved.append((x, h, q, k, v, o, x1, h2, gate_pre, lin_pre, gated))
            if l < layers - 1:
                x = fwd_sum(dot(gated, w_out[l]), x1)

        grads = [None] * layers
        d_table = jnp.zeros_like(table)
        for l in reversed(range(layers)):
            x, h, q, k, v, o, x1, h2, gate_pre, lin_pre, gated = saved[l]
            d_gated = dot(dy, w_out[l], NT)
            gelu_val, gelu_pull = jax.vjp(lambda gate_in: jax.nn.gelu(gate_in, approximate=True), gate_pre)
            d_lin = (d_gated * gelu_val).astype(BF16)
            d_gate = gelu_pull(d_gated * lin_pre)[0].astype(BF16)
            d_mid, d_gm = bwd_sum(dot(d_gate, w_gate[l], NT) + dot(d_lin, w_lin[l], NT), x1, g_mlp[l], dy)
            d_wout = cp_sum(dot(gated, dy, TN))
            d_wgate = cp_sum(dot(h2, d_gate, TN))
            d_wlin = cp_sum(dot(h2, d_lin, TN))
            dq, dk, dv, dt = attn_bwd(d_mid, w_o[l], q, k, v, o, table, key_add, seq)
            d_table = d_table + dt
            part = dot(dq, w_q[l], NT) + dot(dk, w_k[l], NT) + dot(dv, w_v[l], NT)
            d_x, d_ga = bwd_sum(part, x, g_attn[l], d_mid)
            d_wo = cp_sum(dot(o, d_mid, TN))
            d_wq = cp_sum(dot(h, dq, TN))
            d_wk = cp_sum(dot(h, dk, TN))
            d_wv = cp_sum(dot(h, dv, TN))
            grads[l] = (d_ga, d_gm, d_wq, d_wk, d_wv, d_wo, d_wgate, d_wlin, d_wout)
            dy = d_x
        stacked = [jnp.stack([g[i] for g in grads]) for i in range(9)]
        d_bias = jnp.sum(jnp.where(onehot[None], d_table[:, None, :], 0.0), axis=2)
        d_bias = lax.psum(d_bias, 'cp').T
        d_gains = lax.psum(jnp.stack(stacked[:2]), ('tp', 'cp'))
        d_x = lax.all_to_all(dy.reshape(own_batch, seq, width), 'cp', split_axis=1, concat_axis=0, tiled=True)
        return (d_x, d_bias, d_gains[0], d_gains[1]) + tuple(stacked[2:])

    return jax.shard_map(local_program, mesh=mesh, in_specs=(seq_spec, seq_spec, P(None, 'cp'), P(None, 'tp')) + weight_specs, out_specs=(seq_spec, P(None, 'tp')) + weight_specs, check_vma=False)
```

```python
import functools
import jax
import jax.numpy as jnp
from jax import lax
from jax.experimental import pallas as pl
from jax.experimental.pallas import tpu as pltpu
from jax.sharding import PartitionSpec as P

NORM_EPS = 1e-6
MASK_NEG = -1e9
HEAD = 64
F32 = jnp.float32
BF16 = jnp.bfloat16
NT = (((1,), (1,)), ((), ()))
TN = (((0,), (0,)), ((), ()))


def rel_bucket(rel_pos):
    distance = jnp.minimum(jnp.abs(rel_pos), 128)
    distance_sq = distance * distance
    log_part = 8 + sum((distance_sq >= 64 * 2 ** power).astype(jnp.int32) for power in range(1, 8))
    return jnp.where(distance < 8, distance, log_part) + 16 * (rel_pos > 0).astype(jnp.int32)


def bucket_onehot(seq):
    rel = jnp.arange(2 * seq) - seq
    return (rel_bucket(rel)[None, :] == jnp.arange(32)[:, None]) & (jnp.arange(2 * seq) > 0)[None, :]


def dot(a, b, dims=(((1,), (0,)), ((), ()))):
    return lax.dot_general(a, b, dims, preferred_element_type=F32)


def toeplitz(row, seq):
    base = pltpu.roll(row, seq, 1)
    rows = jnp.concatenate([base if i == 0 else pltpu.roll(base, i, 1) for i in range(8)], axis=0)
    size = 8
    while size < seq:
        rows = jnp.concatenate([rows, pltpu.roll(rows, size, 1)], axis=0)
        size *= 2
    return rows[:, :seq]


def diag_sums(mat, seq):
    wide = jnp.concatenate([mat, jnp.zeros_like(mat)], axis=1)
    size = seq
    while size > 1:
        half = size // 2
        wide = wide[:half] + pltpu.roll(wide[half:size], 2 * seq - half, 1)
        size = half
    return pltpu.roll(wide, seq, 1)


def attn_fwd_kernel(seq, batch, heads, x_ref, g_ref, wq_ref, wk_ref, wv_ref, t_ref, add_ref, h_ref, q_ref, k_ref, v_ref, o_ref, bias_ref):
    for blk in range(batch * seq // 256):
        rows = pl.ds(blk * 256, 256)
        xf = x_ref[rows, :].astype(F32)
        inv = lax.rsqrt(jnp.mean(xf * xf, axis=-1, keepdims=True) + NORM_EPS)
        h = (xf * inv * g_ref[...]).astype(BF16)
        h_ref[rows, :] = h
        q_ref[rows, :] = dot(h, wq_ref[...]).astype(BF16)
        k_ref[rows, :] = dot(h, wk_ref[...]).astype(BF16)
        v_ref[rows, :] = dot(h, wv_ref[...]).astype(BF16)
    for head in range(heads):
        bias_ref[...] = toeplitz(t_ref[head:head + 1, :], seq)
        cols = pl.ds(head * HEAD, HEAD)
        for b in range(batch):
            rows = pl.ds(b * seq, seq)
            s = dot(q_ref[rows, cols], k_ref[rows, cols], NT) + bias_ref[...] + add_ref[b:b + 1, :]
            e = jnp.exp(s - jnp.max(s, axis=-1, keepdims=True))
            total = jnp.sum(e, axis=-1, keepdims=True)
            o_ref[rows, cols] = (dot(e.astype(BF16), v_ref[rows, cols]) / total).astype(BF16)


def attn_bwd_kernel(seq, batch, heads, dm_ref, wo_ref, q_ref, k_ref, v_ref, o_ref, t_ref, add_ref, dq_ref, dk_ref, dv_ref, dt_ref, bias_ref, dout_ref, acc_ref):
    for blk in range(batch * seq // 256):
        rows = pl.ds(blk * 256, 256)
        dout_ref[rows, :] = dot(dm_ref[rows, :], wo_ref[...], NT).astype(BF16)
    dt_ref[...] = jnp.zeros_like(dt_ref)
    for head in range(heads):
        bias_ref[...] = toeplitz(t_ref[head:head + 1, :], seq)
        cols = pl.ds(head * HEAD, HEAD)
        for b in range(batch):
            rows = pl.ds(b * seq, seq)
            q, k, v, do = q_ref[rows, cols], k_ref[rows, cols], v_ref[rows, cols], dout_ref[rows, cols]
            s = dot(q, k, NT) + bias_ref[...] + add_ref[b:b + 1, :]
            e = jnp.exp(s - jnp.max(s, axis=-1, keepdims=True))
            p = e * (1.0 / jnp.sum(e, axis=-1, keepdims=True))
            row_dot = jnp.sum(do.astype(F32) * o_ref[rows, cols].astype(F32), axis=-1, keepdims=True)
            ds = p * (dot(do, v, NT) - row_dot)
            if b == 0:
                acc_ref[...] = ds
            else:
                acc_ref[...] += ds
            dsl = ds.astype(BF16)
            dq_ref[rows, cols] = dot(dsl, k).astype(BF16)
            dk_ref[rows, cols] = dot(dsl, q, TN).astype(BF16)
            dv_ref[rows, cols] = dot(p.astype(BF16), do, TN).astype(BF16)
        dt_ref[head:head + 1, :] = diag_sums(acc_ref[...], seq)


def vmem_specs(n):
    return [pl.BlockSpec(memory_space=pltpu.VMEM)] * n


def attn_fwd(x, gain, w_q, w_k, w_v, table, key_add, seq):
    rows, width = x.shape
    cols = w_q.shape[1]
    batch, heads = rows // seq, cols // HEAD
    flops = 2 * rows * width * cols * 3 + 4 * rows * seq * cols
    return pl.pallas_call(
        functools.partial(attn_fwd_kernel, seq, batch, heads),
        out_shape=[jax.ShapeDtypeStruct(x.shape, BF16)] + [jax.ShapeDtypeStruct((rows, cols), BF16)] * 4,
        in_specs=vmem_specs(7), out_specs=vmem_specs(5),
        scratch_shapes=[pltpu.VMEM((seq, seq), F32)],
        compiler_params=pltpu.CompilerParams(vmem_limit_bytes=48 * 1024 * 1024),
        cost_estimate=pl.CostEstimate(flops=flops, bytes_accessed=8 << 20, transcendentals=0),
        name="attn_fwd",
    )(x, gain[None, :], w_q, w_k, w_v, table, key_add)


def attn_bwd(d_mid, w_o, q, k, v, o, table, key_add, seq):
    rows, cols = q.shape
    batch, heads = rows // seq, cols // HEAD
    flops = 2 * rows * d_mid.shape[1] * cols + 10 * rows * seq * cols
    return pl.pallas_call(
        functools.partial(attn_bwd_kernel, seq, batch, heads),
        out_shape=[jax.ShapeDtypeStruct((rows, cols), BF16)] * 3 + [jax.ShapeDtypeStruct(table.shape, F32)],
        in_specs=vmem_specs(8), out_specs=vmem_specs(4),
        scratch_shapes=[pltpu.VMEM((seq, seq), F32), pltpu.VMEM((rows, cols), BF16), pltpu.VMEM((seq, seq), F32)],
        compiler_params=pltpu.CompilerParams(vmem_limit_bytes=48 * 1024 * 1024),
        cost_estimate=pl.CostEstimate(flops=flops, bytes_accessed=8 << 20, transcendentals=0),
        name="attn_bwd",
    )(d_mid, w_o, q, k, v, o, table, key_add)


def rms(x, gain):
    xf = x.astype(F32)
    inv = lax.rsqrt(jnp.mean(xf * xf, axis=-1, keepdims=True) + NORM_EPS)
    return (xf * inv * gain).astype(BF16)


class Stream:
    def __init__(self, part, near, far, out, send, recv, first, second, a, b, index):
        self.part, self.near, self.far, self.out = part, near, far, out
        self.send, self.recv = send, recv
        self.first, self.second = first, second
        self.own, self.pass_on = index(a, b), index(a, 1 - b)
        self.away_far, self.away = index(1 - a, 1 - b), index(1 - a, b)
        self.copies = [None] * 6

    def start(self, slot, src, dst, target):
        self.copies[slot] = pltpu.make_async_remote_copy(
            src_ref=src, dst_ref=dst, send_sem=self.send.at[slot], recv_sem=self.recv.at[slot],
            device_id=target, device_id_type=pl.DeviceIdType.MESH)
        self.copies[slot].start()

    def send_away(self, slot):
        quarter = self.away_far if slot == 0 else self.away
        self.start(slot, self.part(quarter), self.near.at[slot], self.first)

    def forward(self):
        self.copies[0].wait_recv()
        ref = self.part(self.pass_on)
        ref[...] += self.near[0]
        self.start(2, ref, self.far, self.second)

    def finish(self, epilogue):
        self.copies[1].wait_recv()
        self.copies[2].wait_recv()
        out = self.out(self.own)
        out[...] = epilogue(self.part(self.own)[...] + self.near[1] + self.far[...])
        self.start(3, out, out, self.first)
        self.start(4, out, out, self.second)

    def gather(self):
        self.copies[4].wait_recv()
        out = self.out(self.pass_on)
        self.start(5, out, out, self.first)

    def close(self):
        self.copies[3].wait_recv()
        self.copies[5].wait_recv()
        for copy in self.copies:
            copy.wait_send()


def sum_kernel(kind, transposed, n_pairs, n_grads, *refs):
    refs = list(refs)
    lhs = [refs.pop(0) for _ in range(n_pairs)]
    rhs = [refs.pop(0) for _ in range(n_pairs)]
    res_ref = refs.pop(0)
    if kind == 'bwd':
        x_ref, gain_ref = refs.pop(0), refs.pop(0)
    grad_in = [(refs.pop(0), refs.pop(0)) for _ in range(n_grads)]
    out_ref = refs.pop(0)
    if kind == 'bwd':
        d_gain_ref = refs.pop(0)
    grad_out = [refs.pop(0) for _ in range(n_grads)]
    part, near, far, send, recv = [refs.pop(0) for _ in range(5)]
    grad_scratch = [[refs.pop(0) for _ in range(3)] for _ in range(n_grads)]

    tp, cp = lax.axis_index('tp'), lax.axis_index('cp')
    z, y = tp // 2, tp % 2
    x, core = cp // 2, cp % 2
    z_peer = {'tp': (1 - z) * 2 + y, 'cp': cp}
    y_peer = {'tp': z * 2 + 1 - y, 'cp': cp}
    x_peer = {'tp': tp, 'cp': (1 - x) * 2 + core}
    core_peer = {'tp': tp, 'cp': x * 2 + 1 - core}
    peers = [z_peer, y_peer] + ([core_peer, x_peer] if n_grads else [])
    barrier = pltpu.get_barrier_semaphore()
    for peer in peers:
        pl.semaphore_signal(barrier, inc=1, device_id=peer, device_id_type=pl.DeviceIdType.MESH)
    pl.semaphore_wait(barrier, len(peers))

    def colour(c, first, second, a, b, index):
        return Stream(lambda q: part.at[q, c], near.at[c], far.at[c], lambda q: out_ref.at[q, c],
                      send.at[c], recv.at[c], first, second, a, b, index)

    zy = colour(0, z_peer, y_peer, z, y, lambda a, b: a * 2 + b)
    yz = colour(1, y_peer, z_peer, y, z, lambda a, b: b * 2 + a)
    streams = [zy, yz]
    grads = []
    for i in range(n_grads):
        g_part, g_near, g_far = grad_scratch[i]
        grads.append(Stream(lambda q, r=g_part: r.at[q], g_near, g_far, lambda q, r=grad_out[i]: r.at[q],
                            send.at[2 + i], recv.at[2 + i], core_peer, x_peer, core, x, lambda a, b: b * 2 + a))

    def compute(q):
        total = sum(dot(l[q], r[...], NT) if transposed else dot(l[q], r[...]) for l, r in zip(lhs, rhs))
        half = total.shape[0] // 2
        part[q, 0] = total[:half]
        part[q, 1] = total[half:]

    def compute_grad(i):
        a_ref, b_ref = grad_in[i]
        g_part = grad_scratch[i][0]
        quarter = g_part.shape[1]
        width = b_ref.shape[1]
        for lo in range(0, width, 256):
            hi = min(lo + 256, width)
            block = dot(a_ref[...], b_ref[:, lo:hi], TN)
            for q in range(4):
                g_part[q, :, lo:hi] = block[q * quarter:(q + 1) * quarter]
        grads[i].send_away(0)
        grads[i].send_away(1)

    compute(zy.away_far)
    zy.send_away(0)
    yz.send_away(0)
    compute(zy.away)
    zy.send_away(1)
    compute(yz.away)
    yz.send_away(1)
    compute(zy.own)
    if n_grads:
        compute_grad(0)
    for s in streams:
        s.forward()
    for i in range(1, n_grads):
        compute_grad(i)
    for g in grads:
        g.forward()

    if kind == 'bwd':
        d_gain = []

    def epilogue(c):
        def run(total):
            res = res_ref[zy.own, c].astype(F32)
            if kind == 'fwd':
                return (res + total).astype(BF16)
            xf = x_ref[zy.own, c].astype(F32)
            inv = lax.rsqrt(jnp.mean(xf * xf, axis=-1, keepdims=True) + NORM_EPS)
            normed = xf * inv
            d_gain.append(jnp.sum(total * normed, axis=0, keepdims=True))
            d_normed = total * gain_ref[...]
            d_x = inv * (d_normed - normed * jnp.mean(d_normed * normed, axis=-1, keepdims=True))
            return (d_x + res).astype(BF16)
        return run

    zy.finish(epilogue(0))
    yz.finish(epilogue(1))
    if kind == 'bwd':
        d_gain_ref[...] = d_gain[0] + d_gain[1]
    for g in grads[:1]:
        g.finish(lambda total: total.astype(BF16))
    for s in streams:
        s.gather()
    for g in grads[1:]:
        g.finish(lambda total: total.astype(BF16))
    for g in grads:
        g.gather()
    for s in streams + grads:
        s.close()


def tp_sum(kind, collective_id, pairs, residual, transposed=False, x=None, gain=None, grads=()):
    rows, width = residual.shape
    quarter = rows // 4
    halves = (4, 2, quarter // 2, width)
    operands = [l.reshape(4, quarter, l.shape[1]) for l, _ in pairs] + [r for _, r in pairs] + [residual.reshape(halves)]
    out_shape = [jax.ShapeDtypeStruct(halves, BF16)]
    if kind == 'bwd':
        operands += [x.reshape(halves), gain[None, :]]
        out_shape.append(jax.ShapeDtypeStruct((1, width), F32))
    scratch = [pltpu.VMEM(halves, F32), pltpu.VMEM((2, 2) + halves[2:], F32), pltpu.VMEM((2,) + halves[2:], F32),
               pltpu.SemaphoreType.DMA((2 + len(grads), 6)), pltpu.SemaphoreType.DMA((2 + len(grads), 6))]
    flops = sum(2 * rows * l.shape[1] * width for l, _ in pairs)
    for a, b in grads:
        operands += [a, b]
        block = (a.shape[1] // 4, b.shape[1])
        out_shape.append(jax.ShapeDtypeStruct((4,) + block, BF16))
        scratch += [pltpu.VMEM((4,) + block, F32), pltpu.VMEM((2,) + block, F32), pltpu.VMEM(block, F32)]
        flops += 2 * rows * a.shape[1] * b.shape[1]
    outs = pl.pallas_call(
        functools.partial(sum_kernel, kind, transposed, len(pairs), len(grads)),
        out_shape=out_shape,
        in_specs=vmem_specs(len(operands)), out_specs=vmem_specs(len(out_shape)),
        scratch_shapes=scratch,
        compiler_params=pltpu.CompilerParams(collective_id=collective_id, has_side_effects=True, vmem_limit_bytes=62 * 1024 * 1024),
        cost_estimate=pl.CostEstimate(flops=flops, bytes_accessed=16 << 20, transcendentals=0),
        name=f"tp_sum_{collective_id}",
    )(*operands)
    total = outs[0].reshape(rows, width)
    d_gain = outs[1][0] if kind == 'bwd' else None
    grad_outs = [o.reshape(a.shape[1], b.shape[1]) for o, (a, b) in zip(outs[len(outs) - len(grads):], grads)]
    return total, d_gain, grad_outs


def mlp_up(x1, gain, w_gate, w_lin):
    h2 = rms(x1, gain)
    gate_pre, lin_pre = dot(h2, w_gate), dot(h2, w_lin)
    gated = (jax.nn.gelu(gate_pre, approximate=True) * lin_pre).astype(BF16)
    return h2, gate_pre, lin_pre, gated


def cp_sum(part):
    own = lax.psum_scatter(part, 'cp', scatter_dimension=0, tiled=True).astype(BF16)
    return lax.all_gather(own, 'cp', axis=0, tiled=True)


def solution(mesh):
    seq_spec = P(None, 'cp', None)
    col_spec = P(None, None, 'tp')
    row_spec = P(None, 'tp', None)
    weight_specs = (P(), P(), col_spec, col_spec, col_spec, row_spec, col_spec, col_spec, row_spec)
    cp_size = mesh.shape['cp']

    def local_program(x_in, d_y, key_mask, rel_bias, g_attn, g_mlp, w_q, w_k, w_v, w_o, w_gate, w_lin, w_out):
        batch, blk, width = x_in.shape
        seq = blk * cp_size
        layers = w_q.shape[0]
        own_batch = batch // cp_size

        def to_batch(arr):
            return lax.all_to_all(arr, 'cp', split_axis=0, concat_axis=1, tiled=True).reshape(own_batch * seq, width)

        x = to_batch(x_in)
        dy = to_batch(d_y)
        mask_all = lax.all_gather(key_mask, 'cp', axis=1, tiled=True)
        mask = lax.dynamic_slice_in_dim(mask_all, lax.axis_index('cp') * own_batch, own_batch, axis=0)
        key_add = jnp.where(mask > 0, 0.0, MASK_NEG).astype(F32)
        onehot = bucket_onehot(seq)
        table = jnp.sum(jnp.where(onehot[None], rel_bias.T[:, :, None], 0.0), axis=1)

        saved = []
        for l in range(layers):
            h, q, k, v, o = attn_fwd(x, g_attn[l], w_q[l], w_k[l], w_v[l], table, key_add, seq)
            x1 = tp_sum('fwd', 0, [(o, w_o[l])], x)[0]
            h2, gate_pre, lin_pre, gated = mlp_up(x1, g_mlp[l], w_gate[l], w_lin[l])
            saved.append((x, h, q, k, v, o, x1, h2, gate_pre, lin_pre, gated))
            if l < layers - 1:
                x = tp_sum('fwd', 1, [(gated, w_out[l])], x1)[0]

        grads = [None] * layers
        d_table = jnp.zeros_like(table)
        waiting = None
        for l in reversed(range(layers)):
            x, h, q, k, v, o, x1, h2, gate_pre, lin_pre, gated = saved[l]
            d_gated = dot(dy, w_out[l], NT)
            gelu_val, gelu_pull = jax.vjp(lambda gate_in: jax.nn.gelu(gate_in, approximate=True), gate_pre)
            d_lin = (d_gated * gelu_val).astype(BF16)
            d_gate = gelu_pull(d_gated * lin_pre)[0].astype(BF16)
            work = [(gated, dy), (h2, d_gate)] if waiting is None else [(gated, dy)] + waiting
            d_mid, d_gm, done = tp_sum('bwd', 2 + 2 * (layers - 1 - l), [(d_gate, w_gate[l]), (d_lin, w_lin[l])], dy, True, x1, g_mlp[l], work)
            d_wout = done[0]
            if waiting is None:
                d_wgate = done[1]
                work = [(h2, d_lin), (o, d_mid)]
            else:
                grads[l + 1] += tuple(done[1:])
                work = [(h2, d_gate), (h2, d_lin)]
            dq, dk, dv, dt = attn_bwd(d_mid, w_o[l], q, k, v, o, table, key_add, seq)
            d_table = d_table + dt
            d_x, d_ga, done = tp_sum('bwd', 3 + 2 * (layers - 1 - l), [(dq, w_q[l]), (dk, w_k[l]), (dv, w_v[l])], d_mid, True, x, g_attn[l], work)
            if waiting is None:
                d_wlin, d_wo = done
                waiting = [(h, dq), (h, dk), (h, dv)]
                grads[l] = (d_ga, d_gm, d_wo, d_wgate, d_wlin, d_wout)
            else:
                d_wgate, d_wlin = done
                grads[l] = (d_ga, d_gm, cp_sum(dot(o, d_mid, TN)), d_wgate, d_wlin, d_wout)
                grads[l] += tuple(cp_sum(dot(h, d, TN)) for d in (dq, dk, dv))
            dy = d_x
        stacked = [jnp.stack([g[i] for g in grads]) for i in range(9)]
        d_bias = jnp.sum(jnp.where(onehot[None], d_table[:, None, :], 0.0), axis=2)
        d_bias = lax.psum(d_bias, 'cp').T
        d_gains = lax.psum(jnp.stack(stacked[:2]), ('tp', 'cp'))
        d_x = lax.all_to_all(dy.reshape(own_batch, seq, width), 'cp', split_axis=1, concat_axis=0, tiled=True)
        return (d_x, d_bias, d_gains[0], d_gains[1]) + tuple(stacked[6:]) + tuple(stacked[2:6])

    return jax.shard_map(local_program, mesh=mesh, in_specs=(seq_spec, seq_spec, P(None, 'cp'), P(None, 'tp')) + weight_specs, out_specs=(seq_spec, P(None, 'tp')) + weight_specs, check_vma=False)
```

```python
import functools
import jax
import jax.numpy as jnp
import numpy as np
from jax import lax
from jax.experimental import pallas as pl
from jax.experimental.pallas import tpu as pltpu
from jax.sharding import PartitionSpec as P

NORM_EPS = 1e-6
MASK_NEG = -1e9
HEAD = 64
F32 = jnp.float32
BF16 = jnp.bfloat16
NT = (((1,), (1,)), ((), ()))
TN = (((0,), (0,)), ((), ()))


def rel_bucket(rel_pos):
    distance = jnp.minimum(jnp.abs(rel_pos), 128)
    distance_sq = distance * distance
    log_part = 8 + sum((distance_sq >= 64 * 2 ** power).astype(jnp.int32) for power in range(1, 8))
    return jnp.where(distance < 8, distance, log_part) + 16 * (rel_pos > 0).astype(jnp.int32)


def bucket_onehot(seq):
    rel = jnp.arange(2 * seq) - seq
    return (rel_bucket(rel)[None, :] == jnp.arange(32)[:, None]) & (jnp.arange(2 * seq) > 0)[None, :]


def dot(a, b, dims=(((1,), (0,)), ((), ()))):
    return lax.dot_general(a, b, dims, preferred_element_type=F32)


def toeplitz(row, seq):
    base = pltpu.roll(row, seq, 1)
    rows = jnp.concatenate([base if i == 0 else pltpu.roll(base, i, 1) for i in range(8)], axis=0)
    size = 8
    while size < seq:
        rows = jnp.concatenate([rows, pltpu.roll(rows, size, 1)], axis=0)
        size *= 2
    return rows[:, :seq]


def diag_sums(mat, seq):
    wide = jnp.concatenate([mat, jnp.zeros_like(mat)], axis=1)
    size = seq
    while size > 1:
        half = size // 2
        wide = wide[:half] + pltpu.roll(wide[half:size], 2 * seq - half, 1)
        size = half
    return pltpu.roll(wide, seq, 1)


def place():
    tp, cp = lax.axis_index('tp'), lax.axis_index('cp')
    z, y = tp // 2, tp % 2
    x, core = cp // 2, cp % 2
    peers = {'z': (1 - z, y, x, core), 'y': (z, 1 - y, x, core), 'x': (z, y, 1 - x, core), 'core': (z, y, x, 1 - core),
             'zy': (1 - z, 1 - y, x, core), 'xc': (z, y, 1 - x, 1 - core)}
    ids = {name: {'tp': p[0] * 2 + p[1], 'cp': p[2] * 2 + p[3]} for name, p in peers.items()}
    return tp, cp, z, y, x, core, ids


def meet(ids, names):
    barrier = pltpu.get_barrier_semaphore()
    for name in names:
        pl.semaphore_signal(barrier, inc=1, device_id=ids[name], device_id_type=pl.DeviceIdType.MESH)
    pl.semaphore_wait(barrier, len(names))


def remote(src, dst, send, recv, target):
    copy = pltpu.make_async_remote_copy(src_ref=src, dst_ref=dst, send_sem=send, recv_sem=recv,
                                        device_id=target, device_id_type=pl.DeviceIdType.MESH)
    copy.start()
    return copy


class Stream:
    def __init__(self, part, near, far, out, send, recv, first, second, a, b, index):
        self.part, self.near, self.far, self.out = part, near, far, out
        self.send, self.recv = send, recv
        self.first, self.second = first, second
        self.own, self.pass_on = index(a, b), index(a, 1 - b)
        self.away_far, self.away = index(1 - a, 1 - b), index(1 - a, b)
        self.copies = {}

    def start(self, slot, src, dst, target):
        self.copies[slot] = remote(src, dst, self.send.at[slot], self.recv.at[slot], target)

    def send_away(self, slot):
        quarter = self.away_far if slot == 0 else self.away
        self.start(slot, self.part(quarter), self.near.at[slot], self.first)

    def forward(self):
        self.copies[0].wait_recv()
        ref = self.part(self.pass_on)
        ref[...] += self.near[0]
        self.start(2, ref, self.far, self.second)

    def total(self):
        self.copies[1].wait_recv()
        self.copies[2].wait_recv()
        return self.part(self.own)[...] + self.near[1] + self.far[...]

    def publish(self):
        out = self.out(self.own)
        self.start(3, out, out, self.first)
        self.start(4, out, out, self.second)

    def finish(self):
        self.out(self.own)[...] = self.total().astype(BF16)
        self.publish()

    def gather(self):
        self.copies[4].wait_recv()
        out = self.out(self.pass_on)
        self.start(5, out, out, self.first)

    def close(self):
        self.copies[3].wait_recv()
        self.copies[5].wait_recv()
        for copy in self.copies.values():
            copy.wait_send()


def colours(part, near, far, out, send, recv, ids, z, y):
    def make(c, first, second, a, b, index):
        return Stream(lambda q: part.at[q[0], q[1], c], None if near is None else near.at[c], None if far is None else far.at[c],
                      lambda q: out(q, c), send.at[c], recv.at[c], ids[first], ids[second], a, b, index)
    return [make(0, 'z', 'y', z, y, lambda a, b: (a, b)), make(1, 'y', 'z', y, z, lambda a, b: (b, a))]


def grad_stream(part, near, far, out, send, recv, ids, x, core):
    return Stream(lambda q: part.at[q], near, far, lambda q: out.at[q], send, recv, ids['core'], ids['x'], core, x, lambda a, b: b * 2 + a)


def grad_into(part, a, b):
    quarter, width = part.shape[1], part.shape[2]
    for lo in range(0, width, 256):
        block = dot(a, b[:, lo:lo + 256], TN)
        for q in range(4):
            part[q, :, lo:lo + 256] = block[q * quarter:(q + 1) * quarter]


def norm_parts(rows):
    xf = rows.astype(F32)
    inv = lax.rsqrt(jnp.mean(xf * xf, axis=-1, keepdims=True) + NORM_EPS)
    return inv, xf * inv


def norm(rows, gain):
    return (norm_parts(rows)[1] * gain).astype(BF16)


def norm_back(d_norm, rows, gain):
    inv, normed = norm_parts(rows)
    d_normed = d_norm * gain
    return inv * (d_normed - normed * jnp.mean(d_normed * normed, axis=-1, keepdims=True)), d_norm * normed


def exchange_kernel(x_ref, mask_ref, wo_ref, xo_ref, mo_ref, wf_ref, send, recv):
    tp, cp, z, y, x, core, ids = place()
    names = ['x', 'core', 'xc', 'z', 'y', 'zy']
    meet(ids, names)
    copies, weights = [], []
    for i, name in enumerate(names[:3]):
        copies.append(remote(mask_ref.at[ids[name]['cp']], mo_ref.at[cp], send.at[i], recv.at[i], ids[name]))
        copies.append(remote(x_ref.at[ids[name]['cp']], xo_ref.at[:, cp], send.at[3 + i], recv.at[3 + i], ids[name]))
    for i, name in enumerate(names[3:]):
        weights.append(remote(wo_ref.at[core], wf_ref.at[core, tp], send.at[6 + i], recv.at[6 + i], ids[name]))
    mo_ref[cp] = mask_ref[cp]
    for b in range(2):
        xo_ref[b, cp] = x_ref[cp, b]
    for layer in range(2):
        wf_ref[layer, tp] = wo_ref[layer]
    for i, name in enumerate(names[3:]):
        weights[i].wait_recv()
        got = wf_ref.at[core, ids[name]['tp']]
        copies.append(remote(got, got, send.at[9 + i], recv.at[9 + i], ids['core']))
    for copy in copies:
        copy.wait_recv()
    for copy in copies + weights:
        copy.wait_send()


def exchange(x_in, key_mask, w_o):
    batch, blk, width = x_in.shape
    return pl.pallas_call(
        exchange_kernel,
        out_shape=[jax.ShapeDtypeStruct((2, 4, blk, width), BF16), jax.ShapeDtypeStruct((4, 2, blk), jnp.int32),
                   jax.ShapeDtypeStruct((2, 4) + w_o.shape[1:], BF16)],
        in_specs=vmem_specs(3), out_specs=vmem_specs(3),
        scratch_shapes=[pltpu.SemaphoreType.DMA((12,)), pltpu.SemaphoreType.DMA((12,))],
        compiler_params=pltpu.CompilerParams(collective_id=0, has_side_effects=True, vmem_limit_bytes=40 << 20),
        name="exchange",
    )(x_in.reshape(4, 2, blk, width), key_mask.reshape(4, 2, blk), w_o)


def key_add(mask_ref, b):
    row = jnp.concatenate([mask_ref[j, pl.ds(b, 1), :] for j in range(4)], axis=1)
    return jnp.where(row > 0, 0.0, MASK_NEG).astype(F32)


def exp_scores(q, k, bias, add):
    s = dot(q, k, NT) + bias + add
    e = jnp.exp(s - jnp.max(s, axis=-1, keepdims=True))
    return e, jnp.sum(e, axis=-1, keepdims=True)


def attn_kernel(layer, seq, with_dy, *refs):
    refs = list(refs)
    x_ref, g_ref, wq_all, wk_all, wv_all, t_ref, mask_ref, wf_all = [refs.pop(0) for _ in range(8)]
    if with_dy:
        dy_ref = refs.pop(0)
    x1_ref, q_ref, k_ref, v_ref, o_ref = [refs.pop(0) for _ in range(5)]
    if with_dy:
        dyo_ref = refs.pop(0)
    wq_ref, wk_ref, wv_ref, wf_ref, wsem, bias_ref, of_ref, send, recv, osend, orecv = [refs.pop(0) for _ in range(11)]
    loads = load_layer(layer, [wq_all, wk_all, wv_all, wf_all], [wq_ref, wk_ref, wv_ref, wf_ref], wsem)
    tp, cp, z, y, x, core, ids = place()
    heads = t_ref.shape[0]
    meet(ids, ['z', 'y', 'zy'] + (['x', 'core', 'xc'] if with_dy else []))
    dys = []
    if with_dy:
        for i, name in enumerate(['x', 'core', 'xc']):
            dys.append(remote(dy_ref.at[ids[name]['cp']], dyo_ref.at[:, cp], osend.at[3 + i], orecv.at[3 + i], ids[name]))
        for b in range(2):
            dyo_ref[b, cp] = dy_ref[cp, b]
    out = []
    for copy in loads[:3]:
        copy.wait()
    for step in range(2):
        b = 1 - z if step == 0 else z
        for half in range(2):
            rows = pl.ds(half * 256, 256)
            h = norm(x_ref[b, rows, :], g_ref[layer:layer + 1, :])
            q_ref[b, rows, :] = dot(h, wq_ref[...]).astype(BF16)
            k_ref[b, rows, :] = dot(h, wk_ref[...]).astype(BF16)
            v_ref[b, rows, :] = dot(h, wv_ref[...]).astype(BF16)
        add = key_add(mask_ref, b)
        for head in range(heads):
            if step == 0:
                bias_ref[head] = toeplitz(t_ref[head:head + 1, :], seq)
            cols = pl.ds(head * HEAD, HEAD)
            e, total = exp_scores(q_ref[b, :, cols], k_ref[b, :, cols], bias_ref[head], add)
            o = (dot(e.astype(BF16), v_ref[b, :, cols]) / total).astype(BF16)
            o_ref[b, 0, :, cols] = o[:seq // 2]
            o_ref[b, 1, :, cols] = o[seq // 2:]
        if step == 0:
            out.append(remote(o_ref.at[b, 1 - y], of_ref.at[tp], osend.at[0], orecv.at[0], ids['zy']))
            out.append(remote(o_ref.at[b, y], of_ref.at[tp], osend.at[1], orecv.at[1], ids['z']))
        else:
            out.append(remote(o_ref.at[b, 1 - y], of_ref.at[tp], osend.at[2], orecv.at[2], ids['y']))
    of_ref[tp] = o_ref[z, y]
    loads[3].wait()
    for copy in out:
        copy.wait_recv()
    streams = colours(None, None, None, lambda q, c: x1_ref.at[q[0], q[1], c], send, recv, ids, z, y)
    for c, s in enumerate(streams):
        rows = pl.ds(c * 128, 128)
        total = sum(dot(of_ref[j, rows, :], wf_ref[j]) for j in range(4))
        res = x_ref[z, pl.ds(pl.multiple_of(y * 256 + c * 128, 128), 128), :].astype(F32)
        x1_ref[z, y, c] = (res + total).astype(BF16)
        s.publish()
    for s in streams:
        s.gather()
    for s in streams:
        s.close()
    for copy in out:
        copy.wait_send()
    for copy in dys:
        copy.wait()


def load_layer(layer, stacks, refs, sems):
    copies = [pltpu.make_async_copy(w.at[layer], r, sems.at[i]) for i, (w, r) in enumerate(zip(stacks, refs))]
    for copy in copies:
        copy.start()
    return copies


def layer_scratch(*stacks):
    return [pltpu.VMEM(w.shape[1:], w.dtype) for w in stacks] + [pltpu.SemaphoreType.DMA((len(stacks),))]


def any_specs(n):
    return [pl.BlockSpec(memory_space=pl.ANY)] * n


def attn_layer(layer, collective_id, x, gains, w_q, w_k, w_v, table, mask, w_full, d_y=None):
    seq = 512
    width, cols = w_q.shape[1], w_q.shape[2]
    operands = [x.reshape(2, seq, width), gains, w_q, w_k, w_v, table, mask, w_full]
    in_specs = vmem_specs(2) + any_specs(3) + vmem_specs(2) + any_specs(1)
    head_shape = jax.ShapeDtypeStruct((2, seq, cols), BF16)
    out_shape = [jax.ShapeDtypeStruct((2, 2, 2, 128, width), BF16)] + [head_shape] * 3 + [jax.ShapeDtypeStruct((2, 2, seq // 2, cols), BF16)]
    if d_y is not None:
        operands.append(d_y.reshape(4, 2, 128, width))
        in_specs += vmem_specs(1)
        out_shape.append(jax.ShapeDtypeStruct((2, 4, 128, width), BF16))
    dma = pltpu.SemaphoreType.DMA
    return pl.pallas_call(
        functools.partial(attn_kernel, layer, seq, d_y is not None),
        out_shape=out_shape, in_specs=in_specs, out_specs=vmem_specs(len(out_shape)),
        scratch_shapes=layer_scratch(w_q, w_k, w_v, w_full) + [pltpu.VMEM((table.shape[0], seq, seq), F32), pltpu.VMEM((4, 256, cols), BF16), dma((2, 6)), dma((2, 6)), dma((6,)), dma((6,))],
        compiler_params=pltpu.CompilerParams(collective_id=collective_id, has_side_effects=True, vmem_limit_bytes=48 << 20),
        cost_estimate=pl.CostEstimate(flops=4 << 30, bytes_accessed=16 << 20, transcendentals=0),
        name=f"attn_fwd_{layer}",
    )(*operands)


def gelu_parts(g):
    inner = np.float32(np.sqrt(2 / np.pi)) * (g + 0.044715 * (g * g * g))
    t = jnp.tanh(inner)
    cdf = 0.5 * (1.0 + t)
    slope = cdf + 0.5 * g * (1.0 - t * t) * np.float32(np.sqrt(2 / np.pi)) * (1.0 + 3 * 0.044715 * (g * g))
    return g * cdf, slope


def order(z, y):
    return [(1 - z, 1 - y), (1 - z, y), (z, 1 - y), (z, y)]


def mlp_fwd_kernel(layer, x1_ref, g_ref, wg_all, wl_all, wo_all, out_ref, wg_ref, wl_ref, wo_ref, wsem, part, near, far, send, recv):
    loads = load_layer(layer, [wg_all, wl_all, wo_all], [wg_ref, wl_ref, wo_ref], wsem)
    tp, cp, z, y, x, core, ids = place()
    meet(ids, ['z', 'y'])
    for copy in loads:
        copy.wait()
    zy, yz = streams = colours(part, near, far, lambda q, c: out_ref.at[q[0], q[1], c], send, recv, ids, z, y)

    def compute(q):
        h2 = norm(x1_ref[q].reshape(256, -1), g_ref[layer:layer + 1, :])
        gated = (gelu_parts(dot(h2, wg_ref[...], NT))[0] * dot(h2, wl_ref[...], NT)).astype(BF16)
        part[q] = dot(gated, wo_ref[...]).reshape(part.shape[2:])

    quarters = order(z, y)
    compute(quarters[0])
    zy.send_away(0)
    yz.send_away(0)
    compute(quarters[1])
    zy.send_away(1)
    compute(quarters[2])
    yz.send_away(1)
    compute(quarters[3])
    for s in streams:
        s.forward()
    for c, s in enumerate(streams):
        out_ref[z, y, c] = (x1_ref[z, y, c].astype(F32) + s.total()).astype(BF16)
        s.publish()
    for s in streams:
        s.gather()
    for s in streams:
        s.close()


def sum_scratch(width, blocks=()):
    return [pltpu.VMEM((2, 2, 2) + blocks, F32), pltpu.VMEM((2, 2) + blocks, F32), pltpu.VMEM((2,) + blocks, F32)]


def mlp_fwd(layer, collective_id, x1, gains, wg_t, wl_t, w_out):
    dma = pltpu.SemaphoreType.DMA
    return pl.pallas_call(
        functools.partial(mlp_fwd_kernel, layer),
        out_shape=jax.ShapeDtypeStruct(x1.shape, BF16),
        in_specs=vmem_specs(2) + any_specs(3), out_specs=pl.BlockSpec(memory_space=pltpu.VMEM),
        scratch_shapes=layer_scratch(wg_t, wl_t, w_out) + sum_scratch(0, x1.shape[3:]) + [dma((2, 6)), dma((2, 6))],
        compiler_params=pltpu.CompilerParams(collective_id=collective_id, has_side_effects=True, vmem_limit_bytes=48 << 20),
        cost_estimate=pl.CostEstimate(flops=5 << 30, bytes_accessed=16 << 20, transcendentals=0),
        name=f"mlp_fwd_{layer}",
    )(x1, gains, wg_t, wl_t, w_out)


def mlp_bwd_kernel(layer, x1_ref, dy_ref, g_ref, wg_all, wl_all, wo_all, dm_ref, dg_ref, lin_part, gout_ref, ggate_ref,
                   wg_ref, wl_ref, wo_ref, wsem, part, near, far, h2_ref, gated_ref, dgate_ref, dlin_ref, p0, n0, f0, p1, n1, f1, send, recv):
    loads = load_layer(layer, [wg_all, wl_all, wo_all], [wg_ref, wl_ref, wo_ref], wsem)
    tp, cp, z, y, x, core, ids = place()
    meet(ids, ['z', 'y', 'x', 'core'])
    zy, yz = streams = colours(part, near, far, lambda q, c: dm_ref.at[q[0], q[1], c], send, recv, ids, z, y)
    g_out = grad_stream(p0, n0, f0, gout_ref, send.at[2], recv.at[2], ids, x, core)
    g_gate = grad_stream(p1, n1, f1, ggate_ref, send.at[3], recv.at[3], ids, x, core)
    gain = g_ref[layer:layer + 1, :]
    for copy in loads:
        copy.wait()

    def compute(q):
        h2 = norm(x1_ref[q].reshape(256, -1), gain)
        rows = pl.ds(pl.multiple_of((q[0] * 2 + q[1]) * 256, 256), 256)
        h2_ref[rows, :] = h2
        value, slope = gelu_parts(dot(h2, wg_ref[...], NT))
        lin = dot(h2, wl_ref[...], NT)
        gated_ref[rows, :] = (value * lin).astype(BF16)
        d_gated = dot(dy_ref[q].reshape(256, -1), wo_ref[...], NT)
        d_lin = (d_gated * value).astype(BF16)
        d_gate = (d_gated * lin * slope).astype(BF16)
        dlin_ref[rows, :] = d_lin
        dgate_ref[rows, :] = d_gate
        part[q] = (dot(d_gate, wg_ref[...]) + dot(d_lin, wl_ref[...])).reshape(part.shape[2:])

    quarters = order(z, y)
    compute(quarters[0])
    zy.send_away(0)
    yz.send_away(0)
    compute(quarters[1])
    zy.send_away(1)
    compute(quarters[2])
    yz.send_away(1)
    compute(quarters[3])
    grad_into(p0, gated_ref[...], dy_ref[...].reshape(h2_ref.shape))
    g_out.send_away(0)
    g_out.send_away(1)
    for s in streams:
        s.forward()
    grad_into(p1, dgate_ref[...], h2_ref)
    g_gate.send_away(0)
    g_gate.send_away(1)
    g_out.forward()
    grad_into(lin_part, dlin_ref[...], h2_ref)
    g_gate.forward()
    d_gain = 0.0
    for c, s in enumerate(streams):
        d_x, dg = norm_back(s.total(), x1_ref[z, y, c], gain)
        dm_ref[z, y, c] = (d_x + dy_ref[z, y, c].astype(F32)).astype(BF16)
        s.publish()
        d_gain = d_gain + jnp.sum(dg, axis=0, keepdims=True)
    dg_ref[...] = d_gain
    g_out.finish()
    for s in streams:
        s.gather()
    g_out.gather()
    g_gate.finish()
    g_gate.gather()
    for s in streams + [g_out, g_gate]:
        s.close()


def mlp_bwd(layer, collective_id, x1, dy, gains, wg_t, wl_t, w_out):
    dma = pltpu.SemaphoreType.DMA
    ff, width = wg_t.shape[1:]
    block = (ff // 4, width)
    rows = 1024
    grad_scratch = [pltpu.VMEM((4,) + block, F32), pltpu.VMEM((2,) + block, F32), pltpu.VMEM(block, F32)]
    out_shape = [jax.ShapeDtypeStruct(x1.shape, BF16), jax.ShapeDtypeStruct((1, width), F32), jax.ShapeDtypeStruct((4,) + block, F32)]
    out_shape += [jax.ShapeDtypeStruct((4,) + block, BF16)] * 2
    return pl.pallas_call(
        functools.partial(mlp_bwd_kernel, layer),
        out_shape=out_shape,
        in_specs=vmem_specs(3) + any_specs(3), out_specs=vmem_specs(5),
        scratch_shapes=layer_scratch(wg_t, wl_t, w_out) + sum_scratch(0, x1.shape[3:]) + [pltpu.VMEM((rows, width), BF16)] + [pltpu.VMEM((rows, ff), BF16)] * 3
        + grad_scratch * 2 + [dma((4, 6)), dma((4, 6))],
        compiler_params=pltpu.CompilerParams(collective_id=collective_id, has_side_effects=True, vmem_limit_bytes=60 << 20),
        cost_estimate=pl.CostEstimate(flops=12 << 30, bytes_accessed=32 << 20, transcendentals=0),
        name=f"mlp_bwd_{layer}",
    )(x1, dy, gains, wg_t, wl_t, w_out)


def attn_bwd_kernel(layer, seq, last, *refs):
    refs = list(refs)
    x_ref, dm_ref, lin_part, q_ref, k_ref, v_ref, o_ref, g_ref, wq_all, wk_all, wv_all, wo_all, t_ref, mask_ref = [refs.pop(0) for _ in range(14)]
    if last:
        small_ref = refs.pop(0)
    dx_ref = refs.pop(0)
    if last:
        small_out = refs.pop(0)
    else:
        dg_ref, dt_ref = refs.pop(0), refs.pop(0)
    grad_out = [refs.pop(0) for _ in range(5)]
    wq_ref, wk_ref, wv_ref, wo_ref, wsem = [refs.pop(0) for _ in range(5)]
    loads = load_layer(layer, [wq_all, wk_all, wv_all, wo_all], [wq_ref, wk_ref, wv_ref, wo_ref], wsem)
    part, near, far = [refs.pop(0) for _ in range(3)]
    bias_ref, acc_ref, do_ref, dq_ref, dk_ref, dv_ref, h_ref = [refs.pop(0) for _ in range(7)]
    lin_near, lin_far = refs.pop(0), refs.pop(0)
    grad_scratch = [[refs.pop(0) for _ in range(3)] for _ in range(4)]
    send, recv = refs.pop(0), refs.pop(0)
    if last:
        own_ref, acc_small, got_small, csend, crecv = [refs.pop(0) for _ in range(5)]
    tp, cp, z, y, x, core, ids = place()
    heads = t_ref.shape[0]
    across, deep = part.shape[3], part.shape[4]
    meet(ids, ['z', 'y', 'x', 'core'] + (['xc'] if last else []))
    if last:
        def region(q, c):
            return dx_ref.at[:, q[0], q[1], c]
    else:
        def region(q, c):
            return dx_ref.at[q[0], :, q[1], c]
    zy, yz = streams = colours(part, near, far, region, send, recv, ids, z, y)
    g_lin = grad_stream(lin_part, lin_near, lin_far, grad_out[0], send.at[2], recv.at[2], ids, x, core)
    g_o, g_q, g_k, g_v = [grad_stream(s[0], s[1], s[2], out, send.at[3 + i], recv.at[3 + i], ids, x, core)
                          for i, (s, out) in enumerate(zip(grad_scratch, grad_out[1:]))]
    gain = g_ref[layer:layer + 1, :]
    g_lin.send_away(0)
    g_lin.send_away(1)
    for copy in loads:
        copy.wait()

    def attend(b, step):
        add = key_add(mask_ref, b)
        d_mid = dm_ref[b].reshape(seq, -1)
        do_ref[...] = dot(d_mid, wo_ref[...], NT).astype(BF16)
        for head in range(heads):
            if step == 0:
                bias_ref[head] = toeplitz(t_ref[head:head + 1, :], seq)
            cols = pl.ds(head * HEAD, HEAD)
            q, k, v, do = q_ref[b, :, cols], k_ref[b, :, cols], v_ref[b, :, cols], do_ref[:, cols]
            e, total = exp_scores(q, k, bias_ref[head], add)
            p = e * (1.0 / total)
            row_dot = jnp.sum(do.astype(F32) * o_ref[b, :, cols].astype(F32), axis=-1, keepdims=True)
            ds = p * (dot(do, v, NT) - row_dot)
            if step == 0:
                acc_ref[head] = ds
            else:
                sums = diag_sums(acc_ref[head] + ds, seq)
                if last:
                    acc_small[0, 8 + head:9 + head, :] = small_ref[8 + head:9 + head, :] + sums
                else:
                    dt_ref[head:head + 1, :] = sums
            dsl = ds.astype(BF16)
            dq_ref[b, :, cols] = dot(dsl, k).astype(BF16)
            dk_ref[b, :, cols] = dot(dsl, q, TN).astype(BF16)
            dv_ref[b, :, cols] = dot(p.astype(BF16), do, TN).astype(BF16)
            if step == 0 and head == 0:
                g_lin.forward()
        for half in range(2):
            rows = pl.ds(half * 256, 256)
            h_ref[pl.ds(pl.multiple_of(b * seq + half * 256, 256), 256), :] = norm(x_ref[b, rows, :], gain)

    def compute(q):
        def rows(ref):
            whole = ref[q[0]].reshape(across, 2, 2 * deep, ref.shape[-1]) if across > 1 else None
            if across == 1:
                return ref[q[0], pl.ds(pl.multiple_of(q[1] * 2 * deep, 2 * deep), 2 * deep), :]
            pieces = [ref[q[0], pl.ds(pl.multiple_of(j * 4 * deep + q[1] * 2 * deep, 2 * deep), 2 * deep), :] for j in range(across)]
            return jnp.concatenate(pieces, axis=0)
        total = dot(rows(dq_ref), wq_ref[...], NT) + dot(rows(dk_ref), wk_ref[...], NT) + dot(rows(dv_ref), wv_ref[...], NT)
        total = total.reshape(across, 2, deep, total.shape[-1])
        for c in range(2):
            part[q[0], q[1], c] = total[:, c]

    quarters = order(z, y)
    attend(1 - z, 0)
    compute(quarters[0])
    zy.send_away(0)
    yz.send_away(0)
    compute(quarters[1])
    zy.send_away(1)
    grad_into(grad_scratch[0][0], o_ref[...].reshape(2 * seq, -1), dm_ref[...].reshape(2 * seq, -1))
    g_o.send_away(0)
    g_o.send_away(1)
    attend(z, 1)
    compute(quarters[2])
    yz.send_away(1)
    g_o.forward()
    compute(quarters[3])
    for s in streams:
        s.forward()
    for g, scratch, d_ref in zip([g_q, g_k, g_v], grad_scratch[1:], [dq_ref, dk_ref, dv_ref]):
        grad_into(scratch[0], h_ref[...], d_ref[...].reshape(2 * seq, -1))
        g.send_away(0)
        g.send_away(1)
    g_lin.finish()
    g_o.finish()
    for g in [g_q, g_k, g_v]:
        g.forward()

    d_gain = 0.0
    moves = []
    for c, s in enumerate(streams):
        def own(ref):
            pieces = [ref[z, pl.ds(pl.multiple_of(j * 4 * deep + y * 2 * deep + c * deep, deep), deep), :] for j in range(across)]
            return jnp.concatenate(pieces, axis=0)
        d_x, dg = norm_back(s.total().reshape(across * deep, -1), own(x_ref), gain)
        d_gain = d_gain + jnp.sum(dg, axis=0, keepdims=True)
        d_x = (d_x + own(dm_ref).astype(F32)).astype(BF16).reshape(across, deep, -1)
        if last:
            own_ref[c] = d_x
            dx_ref[cp, z, y, c] = own_ref[c, cp]
            moves.append([remote(own_ref.at[c, ids[name]['cp']], dx_ref.at[cp, z, y, c], csend.at[c, i], crecv.at[c, i], ids[name])
                          for i, name in enumerate(['x', 'xc', 'core'])])
        else:
            dx_ref[z, :, y, c] = d_x
            s.publish()
    if last:
        acc_small[0, 0:4, :] = jnp.concatenate([small_ref[0:3, :], d_gain], axis=0)
        acc_small[0, 4:8, :] = jnp.zeros((4, d_gain.shape[1]), F32)
        acc_small[0, 12:16, :] = jnp.zeros((4, d_gain.shape[1]), F32)
        for c, s in enumerate(streams):
            for copy in moves[c]:
                copy.wait_recv()
            s.publish()
        smalls = []
        for i, name in enumerate(['x', 'core', 'z', 'y']):
            rows = pl.ds(0, 16 if i < 2 else 8)
            smalls.append(remote(acc_small.at[i, rows], got_small.at[i, rows], csend.at[2, i], crecv.at[2, i], ids[name]))
            smalls[i].wait_recv()
            acc_small[i + 1, rows, :] = acc_small[i, rows, :] + got_small[i, rows, :]
        small_out[0:8, :] = acc_small[4, 0:8, :]
        small_out[8:16, :] = acc_small[2, 8:16, :]
        for copy in smalls + moves[0] + moves[1]:
            copy.wait_send()
    else:
        dg_ref[...] = d_gain
    for s in streams:
        s.gather()
    g_lin.gather()
    g_o.gather()
    for g in [g_q, g_k, g_v]:
        g.finish()
    for g in [g_q, g_k, g_v]:
        g.gather()
    for s in streams + [g_lin, g_o, g_q, g_k, g_v]:
        s.close()


def attn_bwd(layer, collective_id, x, d_mid, lin_part, q, k, v, o, gains, w_q, w_k, w_v, w_o, table, mask, small=None):
    seq, width = 512, w_q.shape[1]
    cols = w_q.shape[2]
    last = small is not None
    dma = pltpu.SemaphoreType.DMA
    operands = [x.reshape(2, seq, width), d_mid.reshape(2, seq, width), lin_part, q, k, v, o.reshape(2, seq, cols), gains, w_q, w_k, w_v, w_o, table, mask]
    in_specs = vmem_specs(8) + any_specs(4) + vmem_specs(2)
    blocks = (4, 32, width) if last else (1, 128, width)
    if last:
        operands.append(small)
        in_specs += vmem_specs(1)
        out_shape = [jax.ShapeDtypeStruct((4, 2, 2, 2, 32, width), BF16), jax.ShapeDtypeStruct((16, width), F32)]
    else:
        out_shape = [jax.ShapeDtypeStruct((2, 1, 2, 2, 128, width), BF16), jax.ShapeDtypeStruct((1, width), F32), jax.ShapeDtypeStruct(table.shape, F32)]
    shapes = [(cols // 4, width)] + [(width // 4, cols)] * 3
    lin_block = lin_part.shape[1:]
    out_shape += [jax.ShapeDtypeStruct((4,) + s, BF16) for s in [lin_block] + shapes]
    scratch = layer_scratch(w_q, w_k, w_v, w_o) + sum_scratch(0, blocks) + [pltpu.VMEM((table.shape[0], seq, seq), F32)] * 2 + [pltpu.VMEM((seq, cols), BF16)]
    scratch += [pltpu.VMEM((2, seq, cols), BF16)] * 3 + [pltpu.VMEM((2 * seq, width), BF16)]
    scratch += [pltpu.VMEM((2,) + lin_block, F32), pltpu.VMEM(lin_block, F32)]
    for s in shapes:
        scratch += [pltpu.VMEM((4,) + s, F32), pltpu.VMEM((2,) + s, F32), pltpu.VMEM(s, F32)]
    scratch += [dma((7, 6)), dma((7, 6))]
    if last:
        scratch += [pltpu.VMEM((2, 4, 32, width), BF16), pltpu.VMEM((5, 16, width), F32), pltpu.VMEM((4, 16, width), F32), dma((3, 4)), dma((3, 4))]
    return pl.pallas_call(
        functools.partial(attn_bwd_kernel, layer, seq, last),
        out_shape=out_shape, in_specs=in_specs, out_specs=vmem_specs(len(out_shape)),
        scratch_shapes=scratch,
        compiler_params=pltpu.CompilerParams(collective_id=collective_id, has_side_effects=True, vmem_limit_bytes=62 << 20),
        cost_estimate=pl.CostEstimate(flops=8 << 30, bytes_accessed=32 << 20, transcendentals=0),
        name=f"attn_bwd_{layer}",
    )(*operands)


def vmem_specs(n):
    return [pl.BlockSpec(memory_space=pltpu.VMEM)] * n


def solution(mesh):
    seq_spec = P(None, 'cp', None)
    col_spec = P(None, None, 'tp')
    row_spec = P(None, 'tp', None)
    weight_specs = (P(), P(), col_spec, col_spec, col_spec, row_spec, col_spec, col_spec, row_spec)

    def local_program(x_in, d_y, key_mask, rel_bias, g_attn, g_mlp, w_q, w_k, w_v, w_o, w_gate, w_lin, w_out):
        width = x_in.shape[2]
        quarters = (2, 2, 2, 128, width)
        onehot = bucket_onehot(512)
        table = jnp.sum(jnp.where(onehot[None], rel_bias.T[:, :, None], 0.0), axis=1)
        wg_t, wl_t = jnp.swapaxes(w_gate, 1, 2), jnp.swapaxes(w_lin, 1, 2)
        x0, mask, w_full = exchange(x_in, key_mask, w_o)

        a0, q0, k0, v0, o0, dy = attn_layer(0, 1, x0, g_attn, w_q, w_k, w_v, table, mask, w_full, d_y)
        x1 = mlp_fwd(0, 2, a0, g_mlp, wg_t, wl_t, w_out)
        a1, q1, k1, v1, o1 = attn_layer(1, 3, x1, g_attn, w_q, w_k, w_v, table, mask, w_full)

        dm, dgm1, lin, out1, gate1 = mlp_bwd(1, 4, a1, dy.reshape(quarters), g_mlp, wg_t, wl_t, w_out)
        dx, dga1, dt1, lin1, wo1, wq1, wk1, wv1 = attn_bwd(1, 5, x1, dm, lin, q1, k1, v1, o1, g_attn, w_q, w_k, w_v, w_o, table, mask)
        dm, dgm0, lin, out0, gate0 = mlp_bwd(0, 6, a0, dx.reshape(quarters), g_mlp, wg_t, wl_t, w_out)
        small = jnp.concatenate([dga1, dgm1, dgm0, jnp.zeros((5, width), F32), dt1, jnp.zeros((4, width), F32)], axis=0)
        d_x, small, lin0, wo0, wq0, wk0, wv0 = attn_bwd(0, 7, x0, dm, lin, q0, k0, v0, o0, g_attn, w_q, w_k, w_v, w_o, table, mask, small)

        def both(first, second, like, swap=False):
            shape = (like.shape[2], like.shape[1]) if swap else like.shape[1:]
            pair = jnp.stack([first.reshape(shape), second.reshape(shape)])
            return jnp.swapaxes(pair, 1, 2) if swap else pair

        d_bias = jnp.sum(jnp.where(onehot[None], small[8:12][:, None, :], 0.0), axis=2).T
        d_ga = jnp.stack([small[3], small[0]])
        d_gm = jnp.stack([small[2], small[1]])
        return (d_x.reshape(x_in.shape), d_bias, d_ga, d_gm, both(wq0, wq1, w_q), both(wk0, wk1, w_k), both(wv0, wv1, w_v),
                both(wo0, wo1, w_o), both(gate0, gate1, w_gate, True), both(lin0, lin1, w_lin, True), both(out0, out1, w_out))

    return jax.shard_map(local_program, mesh=mesh, in_specs=(seq_spec, seq_spec, P(None, 'cp'), P(None, 'tp')) + weight_specs, out_specs=(seq_spec, P(None, 'tp')) + weight_specs, check_vma=False)
```

```python
import functools
import jax
import jax.numpy as jnp
import numpy as np
from jax import lax
from jax.experimental import pallas as pl
from jax.experimental.pallas import tpu as pltpu
from jax.sharding import PartitionSpec as P

NORM_EPS = 1e-6
MASK_NEG = -1e9
HEAD = 64
F32 = jnp.float32
BF16 = jnp.bfloat16
NT = (((1,), (1,)), ((), ()))
TN = (((0,), (0,)), ((), ()))


def rel_bucket(rel_pos):
    distance = jnp.minimum(jnp.abs(rel_pos), 128)
    distance_sq = distance * distance
    log_part = 8 + sum((distance_sq >= 64 * 2 ** power).astype(jnp.int32) for power in range(1, 8))
    return jnp.where(distance < 8, distance, log_part) + 16 * (rel_pos > 0).astype(jnp.int32)


def bucket_onehot(seq):
    rel = jnp.arange(2 * seq) - seq
    return (rel_bucket(rel)[None, :] == jnp.arange(32)[:, None]) & (jnp.arange(2 * seq) > 0)[None, :]


def dot(a, b, dims=(((1,), (0,)), ((), ()))):
    return lax.dot_general(a, b, dims, preferred_element_type=F32)


def toeplitz(row, seq):
    base = pltpu.roll(row, seq, 1)
    rows = jnp.concatenate([base if i == 0 else pltpu.roll(base, i, 1) for i in range(8)], axis=0)
    size = 8
    while size < seq:
        rows = jnp.concatenate([rows, pltpu.roll(rows, size, 1)], axis=0)
        size *= 2
    return rows[:, :seq]


def diag_sums(mat, seq):
    wide = jnp.concatenate([mat, jnp.zeros_like(mat)], axis=1)
    size = seq
    while size > 1:
        half = size // 2
        wide = wide[:half] + pltpu.roll(wide[half:size], 2 * seq - half, 1)
        size = half
    return pltpu.roll(wide, seq, 1)


def place():
    tp, cp = lax.axis_index('tp'), lax.axis_index('cp')
    z, y = tp // 2, tp % 2
    x, core = cp // 2, cp % 2
    peers = {'z': (1 - z, y, x, core), 'y': (z, 1 - y, x, core), 'x': (z, y, 1 - x, core), 'core': (z, y, x, 1 - core),
             'zy': (1 - z, 1 - y, x, core), 'xc': (z, y, 1 - x, 1 - core)}
    ids = {name: {'tp': p[0] * 2 + p[1], 'cp': p[2] * 2 + p[3]} for name, p in peers.items()}
    return tp, cp, z, y, x, core, ids


def meet(ids, names):
    barrier = pltpu.get_barrier_semaphore()
    for name in names:
        pl.semaphore_signal(barrier, inc=1, device_id=ids[name], device_id_type=pl.DeviceIdType.MESH)
    pl.semaphore_wait(barrier, len(names))


def remote(src, dst, send, recv, target):
    copy = pltpu.make_async_remote_copy(src_ref=src, dst_ref=dst, send_sem=send, recv_sem=recv,
                                        device_id=target, device_id_type=pl.DeviceIdType.MESH)
    copy.start()
    return copy


class Stream:
    def __init__(self, part, near, far, out, send, recv, first, second, a, b, index):
        self.part, self.near, self.far, self.out = part, near, far, out
        self.send, self.recv = send, recv
        self.first, self.second = first, second
        self.own, self.pass_on = index(a, b), index(a, 1 - b)
        self.away_far, self.away = index(1 - a, 1 - b), index(1 - a, b)
        self.copies = {}

    def start(self, slot, src, dst, target):
        self.copies[slot] = remote(src, dst, self.send.at[slot], self.recv.at[slot], target)

    def send_away(self, slot):
        quarter = self.away_far if slot == 0 else self.away
        self.start(slot, self.part(quarter), self.near.at[slot], self.first)

    def forward(self):
        self.copies[0].wait_recv()
        ref = self.part(self.pass_on)
        ref[...] += self.near[0]
        self.start(2, ref, self.far, self.second)

    def total(self):
        self.copies[1].wait_recv()
        self.copies[2].wait_recv()
        return self.part(self.own)[...] + self.near[1] + self.far[...]

    def publish(self):
        out = self.out(self.own)
        self.start(3, out, out, self.first)
        self.start(4, out, out, self.second)

    def finish(self):
        self.out(self.own)[...] = self.total().astype(BF16)
        self.publish()

    def gather(self):
        self.copies[4].wait_recv()
        out = self.out(self.pass_on)
        self.start(5, out, out, self.first)

    def close(self):
        self.copies[3].wait_recv()
        self.copies[5].wait_recv()
        for copy in self.copies.values():
            copy.wait_send()


def colours(part, near, far, out, send, recv, ids, z, y):
    def make(c, first, second, a, b, index):
        return Stream(lambda q: part.at[q[0], q[1], c], None if near is None else near.at[c], None if far is None else far.at[c],
                      lambda q: out(q, c), send.at[c], recv.at[c], ids[first], ids[second], a, b, index)
    return [make(0, 'z', 'y', z, y, lambda a, b: (a, b)), make(1, 'y', 'z', y, z, lambda a, b: (b, a))]


def grad_stream(part, near, far, out, send, recv, ids, x, core):
    return Stream(lambda q: part.at[q], near, far, lambda q: out.at[q], send, recv, ids['core'], ids['x'], core, x, lambda a, b: b * 2 + a)


def grad_into(part, a, b):
    quarter, width = part.shape[1], part.shape[2]
    for lo in range(0, width, 256):
        block = dot(a, b[:, lo:lo + 256], TN)
        for q in range(4):
            part[q, :, lo:lo + 256] = block[q * quarter:(q + 1) * quarter]


def norm_parts(rows):
    xf = rows.astype(F32)
    inv = lax.rsqrt(jnp.mean(xf * xf, axis=-1, keepdims=True) + NORM_EPS)
    return inv, xf * inv


def norm(rows, gain):
    return (norm_parts(rows)[1] * gain).astype(BF16)


def norm_back(d_norm, rows, gain):
    inv, normed = norm_parts(rows)
    d_normed = d_norm * gain
    return inv * (d_normed - normed * jnp.mean(d_normed * normed, axis=-1, keepdims=True)), d_norm * normed


def exchange_kernel(x_ref, mask_ref, wo_ref, xo_ref, mo_ref, wf_ref, send, recv):
    tp, cp, z, y, x, core, ids = place()
    names = ['x', 'core', 'xc', 'z', 'y', 'zy']
    meet(ids, names)
    copies, weights = [], []
    for i, name in enumerate(names[:3]):
        copies.append(remote(mask_ref.at[ids[name]['cp']], mo_ref.at[cp], send.at[i], recv.at[i], ids[name]))
        copies.append(remote(x_ref.at[ids[name]['cp']], xo_ref.at[:, cp], send.at[3 + i], recv.at[3 + i], ids[name]))
    for i, name in enumerate(names[3:]):
        weights.append(remote(wo_ref.at[core], wf_ref.at[core, tp], send.at[6 + i], recv.at[6 + i], ids[name]))
    mo_ref[cp] = mask_ref[cp]
    for b in range(2):
        xo_ref[b, cp] = x_ref[cp, b]
    for layer in range(2):
        wf_ref[layer, tp] = wo_ref[layer]
    for i, name in enumerate(names[3:]):
        weights[i].wait_recv()
        got = wf_ref.at[core, ids[name]['tp']]
        copies.append(remote(got, got, send.at[9 + i], recv.at[9 + i], ids['core']))
    for copy in copies:
        copy.wait_recv()
    for copy in copies + weights:
        copy.wait_send()


def exchange(x_in, key_mask, w_o):
    batch, blk, width = x_in.shape
    return pl.pallas_call(
        exchange_kernel,
        out_shape=[jax.ShapeDtypeStruct((2, 4, blk, width), BF16), jax.ShapeDtypeStruct((4, 2, blk), jnp.int32),
                   jax.ShapeDtypeStruct((2, 4) + w_o.shape[1:], BF16)],
        in_specs=vmem_specs(3), out_specs=vmem_specs(3),
        scratch_shapes=[pltpu.SemaphoreType.DMA((12,)), pltpu.SemaphoreType.DMA((12,))],
        compiler_params=pltpu.CompilerParams(collective_id=0, has_side_effects=True, vmem_limit_bytes=40 << 20),
        name="exchange",
    )(x_in.reshape(4, 2, blk, width), key_mask.reshape(4, 2, blk), w_o)


def key_add(mask_ref, b):
    row = jnp.concatenate([mask_ref[j, pl.ds(b, 1), :] for j in range(4)], axis=1)
    return jnp.where(row > 0, 0.0, MASK_NEG).astype(F32)


def exp_scores(q, k, bias, add):
    s = dot(q, k, NT) + bias + add
    e = jnp.exp(s - jnp.max(s, axis=-1, keepdims=True))
    return e, jnp.sum(e, axis=-1, keepdims=True)


def attn_kernel(layer, seq, x_ref, g_ref, wq_all, wk_all, wv_all, t_ref, mask_ref, wf_all, x1_ref, q_out, k_out, v_out, o_out,
                wq_ref, wk_ref, wv_ref, wf_ref, wsem, q_ref, k_ref, v_ref, o_ref, ssem, bias_ref, of_ref, send, recv, osend, orecv):
    loads = load_layer(layer, [wq_all, wk_all, wv_all, wf_all], [wq_ref, wk_ref, wv_ref, wf_ref], wsem)
    tp, cp, z, y, x, core, ids = place()
    heads = t_ref.shape[0]
    meet(ids, ['z', 'y', 'zy'])
    out = []
    for copy in loads[:3]:
        copy.wait()
    for step in range(2):
        b = 1 - z if step == 0 else z
        for half in range(2):
            rows = pl.ds(half * 256, 256)
            h = norm(x_ref[b, rows, :], g_ref[layer:layer + 1, :])
            q_ref[b, rows, :] = dot(h, wq_ref[...]).astype(BF16)
            k_ref[b, rows, :] = dot(h, wk_ref[...]).astype(BF16)
            v_ref[b, rows, :] = dot(h, wv_ref[...]).astype(BF16)
        add = key_add(mask_ref, b)
        for head in range(heads):
            if step == 0:
                bias_ref[head] = toeplitz(t_ref[head:head + 1, :], seq)
            cols = pl.ds(head * HEAD, HEAD)
            e, total = exp_scores(q_ref[b, :, cols], k_ref[b, :, cols], bias_ref[head], add)
            o = (dot(e.astype(BF16), v_ref[b, :, cols]) / total).astype(BF16)
            o_ref[b, 0, :, cols] = o[:seq // 2]
            o_ref[b, 1, :, cols] = o[seq // 2:]
        if step == 0:
            out.append(remote(o_ref.at[b, 1 - y], of_ref.at[tp], osend.at[0], orecv.at[0], ids['zy']))
            out.append(remote(o_ref.at[b, y], of_ref.at[tp], osend.at[1], orecv.at[1], ids['z']))
        else:
            out.append(remote(o_ref.at[b, 1 - y], of_ref.at[tp], osend.at[2], orecv.at[2], ids['y']))
    of_ref[tp] = o_ref[z, y]
    saves = [pltpu.make_async_copy(src, dst, ssem.at[i]) for i, (src, dst) in
             enumerate([(q_ref, q_out), (k_ref, k_out), (v_ref, v_out), (o_ref, o_out)])]
    for copy in saves:
        copy.start()
    loads[3].wait()
    for copy in out:
        copy.wait_recv()
    streams = colours(None, None, None, lambda q, c: x1_ref.at[q[0], q[1], c], send, recv, ids, z, y)
    for c, s in enumerate(streams):
        rows = pl.ds(c * 128, 128)
        total = sum(dot(of_ref[j, rows, :], wf_ref[j]) for j in range(4))
        res = x_ref[z, pl.ds(pl.multiple_of(y * 256 + c * 128, 128), 128), :].astype(F32)
        x1_ref[z, y, c] = (res + total).astype(BF16)
        s.publish()
    for s in streams:
        s.gather()
    for s in streams:
        s.close()
    for copy in out:
        copy.wait_send()
    for copy in saves:
        copy.wait()


def load_layer(layer, stacks, refs, sems):
    copies = [pltpu.make_async_copy(w.at[layer], r, sems.at[i]) for i, (w, r) in enumerate(zip(stacks, refs))]
    for copy in copies:
        copy.start()
    return copies


def layer_scratch(*stacks):
    return [pltpu.VMEM(w.shape[1:], w.dtype) for w in stacks] + [pltpu.SemaphoreType.DMA((len(stacks),))]


def any_specs(n):
    return [pl.BlockSpec(memory_space=pl.ANY)] * n


def attn_layer(layer, collective_id, x, gains, w_q, w_k, w_v, table, mask, w_full):
    seq = 512
    width, cols = w_q.shape[1], w_q.shape[2]
    head_shape = (2, seq, cols)
    o_shape = (2, 2, seq // 2, cols)
    out_shape = [jax.ShapeDtypeStruct((2, 2, 2, 128, width), BF16)] + [jax.ShapeDtypeStruct(h, BF16) for h in [head_shape] * 3 + [o_shape]]
    dma = pltpu.SemaphoreType.DMA
    return pl.pallas_call(
        functools.partial(attn_kernel, layer, seq),
        out_shape=out_shape, in_specs=vmem_specs(2) + any_specs(3) + vmem_specs(2) + any_specs(1), out_specs=vmem_specs(1) + any_specs(4),
        scratch_shapes=layer_scratch(w_q, w_k, w_v, w_full) + [pltpu.VMEM(head_shape, BF16)] * 3 + [pltpu.VMEM(o_shape, BF16), dma((4,))]
        + [pltpu.VMEM((table.shape[0], seq, seq), F32), pltpu.VMEM((4, 256, cols), BF16), dma((2, 6)), dma((2, 6)), dma((3,)), dma((3,))],
        compiler_params=pltpu.CompilerParams(collective_id=collective_id, has_side_effects=True, vmem_limit_bytes=40 << 20),
        cost_estimate=pl.CostEstimate(flops=4 << 30, bytes_accessed=16 << 20, transcendentals=0),
        name=f"attn_fwd_{layer}",
    )(x.reshape(2, seq, width), gains, w_q, w_k, w_v, table, mask, w_full)


def gelu_parts(g):
    inner = np.float32(np.sqrt(2 / np.pi)) * (g + 0.044715 * (g * g * g))
    t = jnp.tanh(inner)
    cdf = 0.5 * (1.0 + t)
    slope = cdf + 0.5 * g * (1.0 - t * t) * np.float32(np.sqrt(2 / np.pi)) * (1.0 + 3 * 0.044715 * (g * g))
    return g * cdf, slope


def order(z, y):
    return [(1 - z, 1 - y), (1 - z, y), (z, 1 - y), (z, y)]


def mlp_fwd_kernel(layer, x1_ref, dy_ref, g_ref, wg_all, wl_all, wo_all, out_ref, dyo_ref, wg_ref, wl_ref, wo_ref, wsem,
                   part, near, far, send, recv, dsend, drecv, own_sem):
    loads = load_layer(layer, [wg_all, wl_all, wo_all], [wg_ref, wl_ref, wo_ref], wsem)
    tp, cp, z, y, x, core, ids = place()
    meet(ids, ['z', 'y', 'x', 'core', 'xc'])
    moves = [remote(dy_ref.at[ids[name]['cp']], dyo_ref.at[:, cp], dsend.at[i], drecv.at[i], ids[name])
             for i, name in enumerate(['x', 'xc', 'core'])]
    own = pltpu.make_async_copy(dy_ref.at[cp], dyo_ref.at[:, cp], own_sem)
    own.start()
    for copy in loads:
        copy.wait()
    zy, yz = streams = colours(part, near, far, lambda q, c: out_ref.at[q[0], q[1], c], send, recv, ids, z, y)

    def compute(q):
        h2 = norm(x1_ref[q].reshape(256, -1), g_ref[layer:layer + 1, :])
        gated = (gelu_parts(dot(h2, wg_ref[...], NT))[0] * dot(h2, wl_ref[...], NT)).astype(BF16)
        part[q] = dot(gated, wo_ref[...]).reshape(part.shape[2:])

    quarters = order(z, y)
    compute(quarters[0])
    zy.send_away(0)
    yz.send_away(0)
    compute(quarters[1])
    zy.send_away(1)
    compute(quarters[2])
    yz.send_away(1)
    compute(quarters[3])
    for s in streams:
        s.forward()
    for c, s in enumerate(streams):
        out_ref[z, y, c] = (x1_ref[z, y, c].astype(F32) + s.total()).astype(BF16)
        s.publish()
    for s in streams:
        s.gather()
    for s in streams:
        s.close()
    for copy in moves + [own]:
        copy.wait()


def sum_scratch(width, blocks=()):
    return [pltpu.VMEM((2, 2, 2) + blocks, F32), pltpu.VMEM((2, 2) + blocks, F32), pltpu.VMEM((2,) + blocks, F32)]


def mlp_fwd(layer, collective_id, x1, d_y, gains, wg_t, wl_t, w_out):
    dma = pltpu.SemaphoreType.DMA
    width = x1.shape[-1]
    return pl.pallas_call(
        functools.partial(mlp_fwd_kernel, layer),
        out_shape=[jax.ShapeDtypeStruct(x1.shape, BF16), jax.ShapeDtypeStruct((2, 4, 128, width), BF16)],
        in_specs=vmem_specs(3) + any_specs(3), out_specs=vmem_specs(1) + any_specs(1),
        scratch_shapes=layer_scratch(wg_t, wl_t, w_out) + sum_scratch(0, x1.shape[3:]) + [dma((2, 6)), dma((2, 6)), dma((3,)), dma((3,)), dma],
        compiler_params=pltpu.CompilerParams(collective_id=collective_id, has_side_effects=True, vmem_limit_bytes=40 << 20),
        cost_estimate=pl.CostEstimate(flops=5 << 30, bytes_accessed=16 << 20, transcendentals=0),
        name=f"mlp_fwd_{layer}",
    )(x1, d_y.reshape(4, 2, 128, width), gains, wg_t, wl_t, w_out)


def mlp_bwd_kernel(layer, n_carry, *refs):
    refs = list(refs)
    x1_ref, dy_ref, g_ref, wg_all, wl_all, wo_all = [refs.pop(0) for _ in range(6)]
    carried = [refs.pop(0) for _ in range(n_carry)]
    dm_ref, dg_ref, lin_out, gout_ref, ggate_ref = [refs.pop(0) for _ in range(5)]
    carried_out = [refs.pop(0) for _ in range(n_carry)]
    wg_ref, wl_ref, wo_ref, wsem, part, near, far, h2_ref, gated_ref, dgate_ref, dlin_ref = [refs.pop(0) for _ in range(11)]
    lin_part, lin_sem, p0, n0, f0, p1, n1, f1 = [refs.pop(0) for _ in range(8)]
    carry_scratch = [[refs.pop(0) for _ in range(2)] for _ in range(n_carry)]
    send, recv = refs
    loads = load_layer(layer, [wg_all, wl_all, wo_all], [wg_ref, wl_ref, wo_ref], wsem)
    tp, cp, z, y, x, core, ids = place()
    meet(ids, ['z', 'y', 'x', 'core'])
    zy, yz = streams = colours(part, near, far, lambda q, c: dm_ref.at[q[0], q[1], c], send, recv, ids, z, y)
    g_out = grad_stream(p0, n0, f0, gout_ref, send.at[2], recv.at[2], ids, x, core)
    g_gate = grad_stream(p1, n1, f1, ggate_ref, send.at[3], recv.at[3], ids, x, core)
    g_carry = [grad_stream(p, s[0], s[1], out, send.at[4 + i], recv.at[4 + i], ids, x, core)
               for i, (p, s, out) in enumerate(zip(carried, carry_scratch, carried_out))]
    gain = g_ref[layer:layer + 1, :]
    for g in g_carry:
        g.send_away(0)
        g.send_away(1)
    for copy in loads:
        copy.wait()

    def compute(q):
        h2 = norm(x1_ref[q].reshape(256, -1), gain)
        rows = pl.ds(pl.multiple_of((q[0] * 2 + q[1]) * 256, 256), 256)
        h2_ref[rows, :] = h2
        value, slope = gelu_parts(dot(h2, wg_ref[...], NT))
        lin = dot(h2, wl_ref[...], NT)
        gated_ref[rows, :] = (value * lin).astype(BF16)
        d_gated = dot(dy_ref[q].reshape(256, -1), wo_ref[...], NT)
        d_lin = (d_gated * value).astype(BF16)
        d_gate = (d_gated * lin * slope).astype(BF16)
        dlin_ref[rows, :] = d_lin
        dgate_ref[rows, :] = d_gate
        part[q] = (dot(d_gate, wg_ref[...]) + dot(d_lin, wl_ref[...])).reshape(part.shape[2:])

    quarters = order(z, y)
    compute(quarters[0])
    zy.send_away(0)
    yz.send_away(0)
    for g in g_carry:
        g.forward()
    compute(quarters[1])
    zy.send_away(1)
    compute(quarters[2])
    yz.send_away(1)
    compute(quarters[3])
    grad_into(p0, gated_ref[...], dy_ref[...].reshape(h2_ref.shape))
    g_out.send_away(0)
    g_out.send_away(1)
    grad_into(p1, dgate_ref[...], h2_ref)
    g_out.forward()
    g_gate.send_away(0)
    g_gate.send_away(1)
    for s in streams:
        s.forward()
    g_gate.forward()
    grad_into(lin_part, dlin_ref[...], h2_ref)
    save = pltpu.make_async_copy(lin_part, lin_out, lin_sem)
    save.start()
    for g in g_carry:
        g.finish()
    g_out.finish()
    d_gain = 0.0
    for c, s in enumerate(streams):
        d_x, dg = norm_back(s.total(), x1_ref[z, y, c], gain)
        dm_ref[z, y, c] = (d_x + dy_ref[z, y, c].astype(F32)).astype(BF16)
        s.publish()
        d_gain = d_gain + jnp.sum(dg, axis=0, keepdims=True)
    dg_ref[...] = d_gain
    for g in g_carry:
        g.gather()
    g_gate.finish()
    for s in streams:
        s.gather()
    g_out.gather()
    g_gate.gather()
    for s in g_carry + streams + [g_out, g_gate]:
        s.close()
    save.wait()


def grad_scratch_of(block):
    return [pltpu.VMEM((4,) + block, F32), pltpu.VMEM((2,) + block, F32), pltpu.VMEM(block, F32)]


def mlp_bwd(layer, collective_id, x1, dy, gains, wg_t, wl_t, w_out, carried=()):
    dma = pltpu.SemaphoreType.DMA
    ff, width = wg_t.shape[1:]
    block = (ff // 4, width)
    rows = 1024
    out_shape = [jax.ShapeDtypeStruct(x1.shape, BF16), jax.ShapeDtypeStruct((1, width), F32), jax.ShapeDtypeStruct((4,) + block, F32)]
    out_shape += [jax.ShapeDtypeStruct((4,) + block, BF16)] * 2 + [jax.ShapeDtypeStruct(c.shape, BF16) for c in carried]
    scratch = layer_scratch(wg_t, wl_t, w_out) + sum_scratch(0, x1.shape[3:]) + [pltpu.VMEM((rows, width), BF16)] + [pltpu.VMEM((rows, ff), BF16)] * 3
    scratch += [pltpu.VMEM((4,) + block, F32), dma] + grad_scratch_of(block) * 2
    for c in carried:
        scratch += grad_scratch_of(c.shape[1:])[1:]
    n = 4 + len(carried)
    return pl.pallas_call(
        functools.partial(mlp_bwd_kernel, layer, len(carried)),
        out_shape=out_shape,
        in_specs=vmem_specs(3) + any_specs(3) + vmem_specs(len(carried)), out_specs=vmem_specs(2) + any_specs(1) + vmem_specs(2 + len(carried)),
        scratch_shapes=scratch + [dma((n, 6)), dma((n, 6))],
        compiler_params=pltpu.CompilerParams(collective_id=collective_id, has_side_effects=True, vmem_limit_bytes=58 << 20),
        cost_estimate=pl.CostEstimate(flops=12 << 30, bytes_accessed=32 << 20, transcendentals=0),
        name=f"mlp_bwd_{layer}",
    )(x1, dy, gains, wg_t, wl_t, w_out, *carried)


def attn_bwd_kernel(layer, seq, last, *refs):
    refs = list(refs)
    x_ref, dm_ref, lin_part, q_ref, k_ref, v_ref, o_ref, g_ref, wq_all, wk_all, wv_all, wo_all, t_ref, mask_ref = [refs.pop(0) for _ in range(14)]
    if last:
        small_ref = refs.pop(0)
    dx_ref = refs.pop(0)
    if last:
        small_out = refs.pop(0)
    else:
        dg_ref, dt_ref, q_part, k_part = [refs.pop(0) for _ in range(4)]
    n_grads = 4 if last else 2
    grad_out = [refs.pop(0) for _ in range(1 + n_grads)]
    wq_ref, wk_ref, wv_ref, wo_ref, wsem = [refs.pop(0) for _ in range(5)]
    loads = load_layer(layer, [wq_all, wk_all, wv_all, wo_all], [wq_ref, wk_ref, wv_ref, wo_ref], wsem)
    part, near, far = [refs.pop(0) for _ in range(3)]
    bias_ref, acc_ref, do_ref, dq_ref, dk_ref, dv_ref, h_ref = [refs.pop(0) for _ in range(7)]
    lin_near, lin_far = refs.pop(0), refs.pop(0)
    grad_scratch = [[refs.pop(0) for _ in range(3)] for _ in range(n_grads)]
    send, recv = refs.pop(0), refs.pop(0)
    if last:
        own_ref, acc_small, got_small, csend, crecv = [refs.pop(0) for _ in range(5)]
    tp, cp, z, y, x, core, ids = place()
    heads = t_ref.shape[0]
    across, deep = part.shape[3], part.shape[4]
    meet(ids, ['z', 'y', 'x', 'core'] + (['xc'] if last else []))
    if last:
        def region(q, c):
            return dx_ref.at[:, q[0], q[1], c]
    else:
        def region(q, c):
            return dx_ref.at[q[0], :, q[1], c]
    zy, yz = streams = colours(part, near, far, region, send, recv, ids, z, y)
    g_lin = grad_stream(lin_part, lin_near, lin_far, grad_out[0], send.at[2], recv.at[2], ids, x, core)
    g_o, *g_qkv = [grad_stream(s[0], s[1], s[2], out, send.at[3 + i], recv.at[3 + i], ids, x, core)
                          for i, (s, out) in enumerate(zip(grad_scratch, grad_out[1:]))]
    gain = g_ref[layer:layer + 1, :]
    g_lin.send_away(0)
    g_lin.send_away(1)
    for copy in loads:
        copy.wait()

    def attend(b, step):
        add = key_add(mask_ref, b)
        d_mid = dm_ref[b].reshape(seq, -1)
        do_ref[...] = dot(d_mid, wo_ref[...], NT).astype(BF16)
        for head in range(heads):
            if step == 0:
                bias_ref[head] = toeplitz(t_ref[head:head + 1, :], seq)
            cols = pl.ds(head * HEAD, HEAD)
            q, k, v, do = q_ref[b, :, cols], k_ref[b, :, cols], v_ref[b, :, cols], do_ref[:, cols]
            e, total = exp_scores(q, k, bias_ref[head], add)
            p = e * (1.0 / total)
            row_dot = jnp.sum(do.astype(F32) * o_ref[b, :, cols].astype(F32), axis=-1, keepdims=True)
            ds = p * (dot(do, v, NT) - row_dot)
            if step == 0:
                acc_ref[head] = ds
            else:
                sums = diag_sums(acc_ref[head] + ds, seq)
                if last:
                    acc_small[0, 8 + head:9 + head, :] = small_ref[8 + head:9 + head, :] + sums
                else:
                    dt_ref[head:head + 1, :] = sums
            dsl = ds.astype(BF16)
            dq_ref[b, :, cols] = dot(dsl, k).astype(BF16)
            dk_ref[b, :, cols] = dot(dsl, q, TN).astype(BF16)
            dv_ref[b, :, cols] = dot(p.astype(BF16), do, TN).astype(BF16)
            if step == 0 and head == 0:
                g_lin.forward()
        for half in range(2):
            rows = pl.ds(half * 256, 256)
            h_ref[pl.ds(pl.multiple_of(b * seq + half * 256, 256), 256), :] = norm(x_ref[b, rows, :], gain)

    def compute(q):
        def rows(ref):
            whole = ref[q[0]].reshape(across, 2, 2 * deep, ref.shape[-1]) if across > 1 else None
            if across == 1:
                return ref[q[0], pl.ds(pl.multiple_of(q[1] * 2 * deep, 2 * deep), 2 * deep), :]
            pieces = [ref[q[0], pl.ds(pl.multiple_of(j * 4 * deep + q[1] * 2 * deep, 2 * deep), 2 * deep), :] for j in range(across)]
            return jnp.concatenate(pieces, axis=0)
        total = dot(rows(dq_ref), wq_ref[...], NT) + dot(rows(dk_ref), wk_ref[...], NT) + dot(rows(dv_ref), wv_ref[...], NT)
        total = total.reshape(across, 2, deep, total.shape[-1])
        for c in range(2):
            part[q[0], q[1], c] = total[:, c]

    quarters = order(z, y)
    attend(1 - z, 0)
    compute(quarters[0])
    zy.send_away(0)
    yz.send_away(0)
    compute(quarters[1])
    zy.send_away(1)
    grad_into(grad_scratch[0][0], o_ref[...].reshape(2 * seq, -1), dm_ref[...].reshape(2 * seq, -1))
    g_o.send_away(0)
    g_o.send_away(1)
    attend(z, 1)
    compute(quarters[2])
    yz.send_away(1)
    g_o.forward()
    compute(quarters[3])
    for g, scratch, d_ref in zip(g_qkv, grad_scratch[1:], [dv_ref, dk_ref, dq_ref]):
        grad_into(scratch[0], h_ref[...], d_ref[...].reshape(2 * seq, -1))
        g.send_away(0)
        g.send_away(1)
    for s in streams:
        s.forward()
    for g in g_qkv:
        g.forward()
    if not last:
        for p, d_ref in zip([q_part, k_part], [dq_ref, dk_ref]):
            grad_into(p, h_ref[...], d_ref[...].reshape(2 * seq, -1))
    g_lin.finish()
    g_o.finish()

    d_gain = 0.0
    moves = []
    for c, s in enumerate(streams):
        def own(ref):
            pieces = [ref[z, pl.ds(pl.multiple_of(j * 4 * deep + y * 2 * deep + c * deep, deep), deep), :] for j in range(across)]
            return jnp.concatenate(pieces, axis=0)
        d_x, dg = norm_back(s.total().reshape(across * deep, -1), own(x_ref), gain)
        d_gain = d_gain + jnp.sum(dg, axis=0, keepdims=True)
        d_x = (d_x + own(dm_ref).astype(F32)).astype(BF16).reshape(across, deep, -1)
        if last:
            own_ref[c] = d_x
            dx_ref[cp, z, y, c] = own_ref[c, cp]
            moves.append([remote(own_ref.at[c, ids[name]['cp']], dx_ref.at[cp, z, y, c], csend.at[c, i], crecv.at[c, i], ids[name])
                          for i, name in enumerate(['x', 'xc', 'core'])])
        else:
            dx_ref[z, :, y, c] = d_x
            s.publish()
    for g in g_qkv:
        g.finish()
    if last:
        acc_small[0, 0:4, :] = jnp.concatenate([small_ref[0:3, :], d_gain], axis=0)
        acc_small[0, 4:8, :] = jnp.zeros((4, d_gain.shape[1]), F32)
        acc_small[0, 12:16, :] = jnp.zeros((4, d_gain.shape[1]), F32)
        for c, s in enumerate(streams):
            for copy in moves[c]:
                copy.wait_recv()
            s.publish()
        smalls = []
        for i, name in enumerate(['x', 'core', 'z', 'y']):
            rows = pl.ds(0, 16 if i < 2 else 8)
            smalls.append(remote(acc_small.at[i, rows], got_small.at[i, rows], csend.at[2, i], crecv.at[2, i], ids[name]))
            smalls[i].wait_recv()
            acc_small[i + 1, rows, :] = acc_small[i, rows, :] + got_small[i, rows, :]
        small_out[0:8, :] = acc_small[4, 0:8, :]
        small_out[8:16, :] = acc_small[2, 8:16, :]
        for copy in smalls + moves[0] + moves[1]:
            copy.wait_send()
    else:
        dg_ref[...] = d_gain
    for s in streams:
        s.gather()
    g_lin.gather()
    g_o.gather()
    for g in g_qkv:
        g.gather()
    for s in streams + [g_lin, g_o] + g_qkv:
        s.close()


def attn_bwd(layer, collective_id, x, d_mid, lin_part, q, k, v, o, gains, w_q, w_k, w_v, w_o, table, mask, small=None):
    seq, width = 512, w_q.shape[1]
    cols = w_q.shape[2]
    last = small is not None
    dma = pltpu.SemaphoreType.DMA
    operands = [x.reshape(2, seq, width), d_mid.reshape(2, seq, width), lin_part, q, k, v, o.reshape(2, seq, cols), gains, w_q, w_k, w_v, w_o, table, mask]
    in_specs = vmem_specs(8) + any_specs(4) + vmem_specs(2)
    blocks = (4, 32, width) if last else (1, 128, width)
    if last:
        operands.append(small)
        in_specs += vmem_specs(1)
        out_shape = [jax.ShapeDtypeStruct((4, 2, 2, 2, 32, width), BF16), jax.ShapeDtypeStruct((16, width), F32)]
    else:
        out_shape = [jax.ShapeDtypeStruct((2, 1, 2, 2, 128, width), BF16), jax.ShapeDtypeStruct((1, width), F32), jax.ShapeDtypeStruct(table.shape, F32)]
        out_shape += [jax.ShapeDtypeStruct((4, width // 4, cols), F32)] * 2
    shapes = [(cols // 4, width)] + [(width // 4, cols)] * (3 if last else 1)
    lin_block = lin_part.shape[1:]
    out_shape += [jax.ShapeDtypeStruct((4,) + s, BF16) for s in [lin_block] + shapes]
    scratch = layer_scratch(w_q, w_k, w_v, w_o) + sum_scratch(0, blocks) + [pltpu.VMEM((table.shape[0], seq, seq), F32)] * 2 + [pltpu.VMEM((seq, cols), BF16)]
    scratch += [pltpu.VMEM((2, seq, cols), BF16)] * 3 + [pltpu.VMEM((2 * seq, width), BF16)]
    scratch += [pltpu.VMEM((2,) + lin_block, F32), pltpu.VMEM(lin_block, F32)]
    for s in shapes:
        scratch += grad_scratch_of(s)
    scratch += [dma((7, 6)), dma((7, 6))]
    if last:
        scratch += [pltpu.VMEM((2, 4, 32, width), BF16), pltpu.VMEM((5, 16, width), F32), pltpu.VMEM((4, 16, width), F32), dma((3, 4)), dma((3, 4))]
    return pl.pallas_call(
        functools.partial(attn_bwd_kernel, layer, seq, last),
        out_shape=out_shape, in_specs=in_specs, out_specs=vmem_specs(len(out_shape)),
        scratch_shapes=scratch,
        compiler_params=pltpu.CompilerParams(collective_id=collective_id, has_side_effects=True, vmem_limit_bytes=62 << 20),
        cost_estimate=pl.CostEstimate(flops=8 << 30, bytes_accessed=32 << 20, transcendentals=0),
        name=f"attn_bwd_{layer}",
    )(*operands)


def vmem_specs(n):
    return [pl.BlockSpec(memory_space=pltpu.VMEM)] * n


def solution(mesh):
    seq_spec = P(None, 'cp', None)
    col_spec = P(None, None, 'tp')
    row_spec = P(None, 'tp', None)
    weight_specs = (P(), P(), col_spec, col_spec, col_spec, row_spec, col_spec, col_spec, row_spec)

    def local_program(x_in, d_y, key_mask, rel_bias, g_attn, g_mlp, w_q, w_k, w_v, w_o, w_gate, w_lin, w_out):
        width = x_in.shape[2]
        quarters = (2, 2, 2, 128, width)
        onehot = bucket_onehot(512)
        table = jnp.sum(jnp.where(onehot[None], rel_bias.T[:, :, None], 0.0), axis=1)
        wg_t, wl_t = jnp.swapaxes(w_gate, 1, 2), jnp.swapaxes(w_lin, 1, 2)
        x0, mask, w_full = exchange(x_in, key_mask, w_o)

        a0, q0, k0, v0, o0 = attn_layer(0, 1, x0, g_attn, w_q, w_k, w_v, table, mask, w_full)
        x1, dy = mlp_fwd(0, 2, a0, d_y, g_mlp, wg_t, wl_t, w_out)
        a1, q1, k1, v1, o1 = attn_layer(1, 3, x1, g_attn, w_q, w_k, w_v, table, mask, w_full)

        dm, dgm1, lin, out1, gate1 = mlp_bwd(1, 4, a1, dy.reshape(quarters), g_mlp, wg_t, wl_t, w_out)
        dx, dga1, dt1, q_part, k_part, lin1, wo1, wv1 = attn_bwd(1, 5, x1, dm, lin, q1, k1, v1, o1, g_attn, w_q, w_k, w_v, w_o, table, mask)
        dm, dgm0, lin, out0, gate0, wq1, wk1 = mlp_bwd(0, 6, a0, dx.reshape(quarters), g_mlp, wg_t, wl_t, w_out, (q_part, k_part))
        small = jnp.concatenate([dga1, dgm1, dgm0, jnp.zeros((5, width), F32), dt1, jnp.zeros((4, width), F32)], axis=0)
        d_x, small, lin0, wo0, wv0, wk0, wq0 = attn_bwd(0, 7, x0, dm, lin, q0, k0, v0, o0, g_attn, w_q, w_k, w_v, w_o, table, mask, small)

        def both(first, second, like, swap=False):
            shape = (like.shape[2], like.shape[1]) if swap else like.shape[1:]
            pair = jnp.stack([first.reshape(shape), second.reshape(shape)])
            return jnp.swapaxes(pair, 1, 2) if swap else pair

        d_bias = jnp.sum(jnp.where(onehot[None], small[8:12][:, None, :], 0.0), axis=2).T
        d_ga = jnp.stack([small[3], small[0]])
        d_gm = jnp.stack([small[2], small[1]])
        return (d_x.reshape(x_in.shape), d_bias, d_ga, d_gm, both(wq0, wq1, w_q), both(wk0, wk1, w_k), both(wv0, wv1, w_v),
                both(wo0, wo1, w_o), both(gate0, gate1, w_gate, True), both(lin0, lin1, w_lin, True), both(out0, out1, w_out))

    return jax.shard_map(local_program, mesh=mesh, in_specs=(seq_spec, seq_spec, P(None, 'cp'), P(None, 'tp')) + weight_specs, out_specs=(seq_spec, P(None, 'tp')) + weight_specs, check_vma=False)
```

```python
import functools
import jax
import jax.numpy as jnp
import numpy as np
from jax import lax
from jax.experimental import pallas as pl
from jax.experimental.pallas import tpu as pltpu
from jax.sharding import PartitionSpec as P

NORM_EPS = 1e-6
MASK_NEG = -1e9
HEAD = 64
F32 = jnp.float32
BF16 = jnp.bfloat16
NT = (((1,), (1,)), ((), ()))
TN = (((0,), (0,)), ((), ()))


def rel_bucket(rel_pos):
    distance = jnp.minimum(jnp.abs(rel_pos), 128)
    distance_sq = distance * distance
    log_part = 8 + sum((distance_sq >= 64 * 2 ** power).astype(jnp.int32) for power in range(1, 8))
    return jnp.where(distance < 8, distance, log_part) + 16 * (rel_pos > 0).astype(jnp.int32)


def bucket_onehot(seq):
    rel = jnp.arange(2 * seq) - seq
    return (rel_bucket(rel)[None, :] == jnp.arange(32)[:, None]) & (jnp.arange(2 * seq) > 0)[None, :]


def dot(a, b, dims=(((1,), (0,)), ((), ()))):
    return lax.dot_general(a, b, dims, preferred_element_type=F32)


def toeplitz(row, seq):
    base = pltpu.roll(row, seq, 1)
    rows = jnp.concatenate([base if i == 0 else pltpu.roll(base, i, 1) for i in range(8)], axis=0)
    size = 8
    while size < seq:
        rows = jnp.concatenate([rows, pltpu.roll(rows, size, 1)], axis=0)
        size *= 2
    return rows[:, :seq]


def diag_sums(mat, seq):
    wide = jnp.concatenate([mat, jnp.zeros_like(mat)], axis=1)
    size = seq
    while size > 1:
        half = size // 2
        wide = wide[:half] + pltpu.roll(wide[half:size], 2 * seq - half, 1)
        size = half
    return pltpu.roll(wide, seq, 1)


def place():
    tp, cp = lax.axis_index('tp'), lax.axis_index('cp')
    z, y = tp // 2, tp % 2
    x, core = cp // 2, cp % 2
    peers = {'z': (1 - z, y, x, core), 'y': (z, 1 - y, x, core), 'x': (z, y, 1 - x, core), 'core': (z, y, x, 1 - core),
             'zy': (1 - z, 1 - y, x, core), 'xc': (z, y, 1 - x, 1 - core)}
    ids = {name: {'tp': p[0] * 2 + p[1], 'cp': p[2] * 2 + p[3]} for name, p in peers.items()}
    return tp, cp, z, y, x, core, ids


def meet(ids, names):
    barrier = pltpu.get_barrier_semaphore()
    for name in names:
        pl.semaphore_signal(barrier, inc=1, device_id=ids[name], device_id_type=pl.DeviceIdType.MESH)
    pl.semaphore_wait(barrier, len(names))


def remote(src, dst, send, recv, target):
    copy = pltpu.make_async_remote_copy(src_ref=src, dst_ref=dst, send_sem=send, recv_sem=recv,
                                        device_id=target, device_id_type=pl.DeviceIdType.MESH)
    copy.start()
    return copy


class Stream:
    def __init__(self, part, near, far, out, send, recv, first, second, a, b, index):
        self.part, self.near, self.far, self.out = part, near, far, out
        self.send, self.recv = send, recv
        self.first, self.second = first, second
        self.own, self.pass_on = index(a, b), index(a, 1 - b)
        self.away_far, self.away = index(1 - a, 1 - b), index(1 - a, b)
        self.copies = {}

    def start(self, slot, src, dst, target):
        self.copies[slot] = remote(src, dst, self.send.at[slot], self.recv.at[slot], target)

    def send_away(self, slot):
        quarter = self.away_far if slot == 0 else self.away
        self.start(slot, self.part(quarter), self.near.at[slot], self.first)

    def forward(self):
        self.copies[0].wait_recv()
        ref = self.part(self.pass_on)
        ref[...] += self.near[0]
        self.start(2, ref, self.far, self.second)

    def total(self):
        self.copies[1].wait_recv()
        self.copies[2].wait_recv()
        return self.part(self.own)[...] + self.near[1] + self.far[...]

    def publish(self):
        out = self.out(self.own)
        self.start(3, out, out, self.first)
        self.start(4, out, out, self.second)

    def finish(self):
        self.out(self.own)[...] = self.total().astype(BF16)
        self.publish()

    def gather(self):
        self.copies[4].wait_recv()
        out = self.out(self.pass_on)
        self.start(5, out, out, self.first)

    def close(self):
        self.copies[3].wait_recv()
        self.copies[5].wait_recv()
        for copy in self.copies.values():
            copy.wait_send()


def colours(part, near, far, out, send, recv, ids, z, y):
    def make(c, first, second, a, b, index):
        return Stream(lambda q: part.at[q[0], q[1], c], None if near is None else near.at[c], None if far is None else far.at[c],
                      lambda q: out(q, c), send.at[c], recv.at[c], ids[first], ids[second], a, b, index)
    return [make(0, 'z', 'y', z, y, lambda a, b: (a, b)), make(1, 'y', 'z', y, z, lambda a, b: (b, a))]


class GradStream(Stream):
    def __init__(self, part, near, far, own_ref, out, send, recv, local, ids, x, core):
        super().__init__(lambda q: part.at[q], near, far, lambda q: out.at[q], send, recv,
                         ids['core'], ids['x'], core, x, lambda a, b: b * 2 + a)
        self.own_ref, self.local = own_ref, local

    def send_both(self):
        self.send_away(0)
        self.send_away(1)

    def finish(self):
        self.own_ref[...] = self.total().astype(BF16)
        out = self.out(self.own)
        self.start(4, self.own_ref, out, self.second)
        self.start(3, self.own_ref, out, self.first)
        self.kept = pltpu.make_async_copy(self.own_ref, out, self.local)
        self.kept.start()

    def close(self):
        super().close()
        self.kept.wait()


def grad_into(part, a, b):
    quarter, width = part.shape[1], part.shape[2]
    for lo in range(0, width, 256):
        block = dot(a, b[:, lo:lo + 256], TN)
        for q in range(4):
            part[q, :, lo:lo + 256] = block[q * quarter:(q + 1) * quarter]


def norm_parts(rows):
    xf = rows.astype(F32)
    inv = lax.rsqrt(jnp.mean(xf * xf, axis=-1, keepdims=True) + NORM_EPS)
    return inv, xf * inv


def norm(rows, gain):
    return (norm_parts(rows)[1] * gain).astype(BF16)


def norm_back(d_norm, rows, gain):
    inv, normed = norm_parts(rows)
    d_normed = d_norm * gain
    return inv * (d_normed - normed * jnp.mean(d_normed * normed, axis=-1, keepdims=True)), d_norm * normed


def exchange_kernel(x_ref, mask_ref, wo_ref, xo_ref, mo_ref, wf_ref, send, recv):
    tp, cp, z, y, x, core, ids = place()
    names = ['x', 'core', 'xc', 'z', 'y', 'zy']
    meet(ids, names)
    copies, weights = [], []
    for i, name in enumerate(names[:3]):
        copies.append(remote(mask_ref.at[ids[name]['cp']], mo_ref.at[cp], send.at[i], recv.at[i], ids[name]))
        copies.append(remote(x_ref.at[ids[name]['cp']], xo_ref.at[:, cp], send.at[3 + i], recv.at[3 + i], ids[name]))
    for i, name in enumerate(names[3:]):
        weights.append(remote(wo_ref.at[core], wf_ref.at[core, tp], send.at[6 + i], recv.at[6 + i], ids[name]))
    mo_ref[cp] = mask_ref[cp]
    for b in range(2):
        xo_ref[b, cp] = x_ref[cp, b]
    for layer in range(2):
        wf_ref[layer, tp] = wo_ref[layer]
    for i, name in enumerate(names[3:]):
        weights[i].wait_recv()
        got = wf_ref.at[core, ids[name]['tp']]
        copies.append(remote(got, got, send.at[9 + i], recv.at[9 + i], ids['core']))
    for copy in copies:
        copy.wait_recv()
    for copy in copies + weights:
        copy.wait_send()


def exchange(x_in, key_mask, w_o):
    batch, blk, width = x_in.shape
    return pl.pallas_call(
        exchange_kernel,
        out_shape=[jax.ShapeDtypeStruct((2, 4, blk, width), BF16), jax.ShapeDtypeStruct((4, 2, blk), jnp.int32),
                   jax.ShapeDtypeStruct((2, 4) + w_o.shape[1:], BF16)],
        in_specs=vmem_specs(3), out_specs=vmem_specs(3),
        scratch_shapes=[pltpu.SemaphoreType.DMA((12,)), pltpu.SemaphoreType.DMA((12,))],
        compiler_params=pltpu.CompilerParams(collective_id=0, has_side_effects=True, vmem_limit_bytes=40 << 20),
        name="exchange",
    )(x_in.reshape(4, 2, blk, width), key_mask.reshape(4, 2, blk), w_o)


def key_add(mask_ref, b):
    row = jnp.concatenate([mask_ref[j, pl.ds(b, 1), :] for j in range(4)], axis=1)
    return jnp.where(row > 0, 0.0, MASK_NEG).astype(F32)


def exp_scores(q, k, bias, add):
    s = dot(q, k, NT) + bias + add
    e = jnp.exp(s - jnp.max(s, axis=-1, keepdims=True))
    return e, jnp.sum(e, axis=-1, keepdims=True)


def attn_kernel(layer, seq, x_ref, g_ref, wq_all, wk_all, wv_all, t_ref, mask_ref, wf_all, x1_ref, q_out, k_out, v_out, o_out,
                wq_ref, wk_ref, wv_ref, wf_ref, wsem, q_ref, k_ref, v_ref, o_ref, ssem, bias_ref, of_ref, send, recv, osend, orecv):
    loads = load_layer(layer, [wq_all, wk_all, wv_all, wf_all], [wq_ref, wk_ref, wv_ref, wf_ref], wsem)
    tp, cp, z, y, x, core, ids = place()
    heads = t_ref.shape[0]
    meet(ids, ['z', 'y', 'zy'])
    out = []
    for copy in loads[:3]:
        copy.wait()
    for step in range(2):
        b = 1 - z if step == 0 else z
        for half in range(2):
            rows = pl.ds(half * 256, 256)
            h = norm(x_ref[b, rows, :], g_ref[layer:layer + 1, :])
            q_ref[b, rows, :] = dot(h, wq_ref[...]).astype(BF16)
            k_ref[b, rows, :] = dot(h, wk_ref[...]).astype(BF16)
            v_ref[b, rows, :] = dot(h, wv_ref[...]).astype(BF16)
        add = key_add(mask_ref, b)
        for head in range(heads):
            if step == 0:
                bias_ref[head] = toeplitz(t_ref[head:head + 1, :], seq)
            cols = pl.ds(head * HEAD, HEAD)
            e, total = exp_scores(q_ref[b, :, cols], k_ref[b, :, cols], bias_ref[head], add)
            o = (dot(e.astype(BF16), v_ref[b, :, cols]) / total).astype(BF16)
            o_ref[b, 0, :, cols] = o[:seq // 2]
            o_ref[b, 1, :, cols] = o[seq // 2:]
        if step == 0:
            out.append(remote(o_ref.at[b, 1 - y], of_ref.at[tp], osend.at[0], orecv.at[0], ids['zy']))
            out.append(remote(o_ref.at[b, y], of_ref.at[tp], osend.at[1], orecv.at[1], ids['z']))
        else:
            out.append(remote(o_ref.at[b, 1 - y], of_ref.at[tp], osend.at[2], orecv.at[2], ids['y']))
    of_ref[tp] = o_ref[z, y]
    saves = [pltpu.make_async_copy(src, dst, ssem.at[i]) for i, (src, dst) in
             enumerate([(q_ref, q_out), (k_ref, k_out), (v_ref, v_out), (o_ref, o_out)])]
    for copy in saves:
        copy.start()
    loads[3].wait()
    for copy in out:
        copy.wait_recv()
    streams = colours(None, None, None, lambda q, c: x1_ref.at[q[0], q[1], c], send, recv, ids, z, y)
    for c, s in enumerate(streams):
        rows = pl.ds(c * 128, 128)
        total = sum(dot(of_ref[j, rows, :], wf_ref[j]) for j in range(4))
        res = x_ref[z, pl.ds(pl.multiple_of(y * 256 + c * 128, 128), 128), :].astype(F32)
        x1_ref[z, y, c] = (res + total).astype(BF16)
        s.publish()
    for s in streams:
        s.gather()
    for s in streams:
        s.close()
    for copy in out:
        copy.wait_send()
    for copy in saves:
        copy.wait()


def load_layer(layer, stacks, refs, sems):
    copies = [pltpu.make_async_copy(w.at[layer], r, sems.at[i]) for i, (w, r) in enumerate(zip(stacks, refs))]
    for copy in copies:
        copy.start()
    return copies


def layer_scratch(*stacks):
    return [pltpu.VMEM(w.shape[1:], w.dtype) for w in stacks] + [pltpu.SemaphoreType.DMA((len(stacks),))]


def any_specs(n):
    return [pl.BlockSpec(memory_space=pl.ANY)] * n


def attn_layer(layer, collective_id, x, gains, w_q, w_k, w_v, table, mask, w_full):
    seq = 512
    width, cols = w_q.shape[1], w_q.shape[2]
    head_shape = (2, seq, cols)
    o_shape = (2, 2, seq // 2, cols)
    out_shape = [jax.ShapeDtypeStruct((2, 2, 2, 128, width), BF16)] + [jax.ShapeDtypeStruct(h, BF16) for h in [head_shape] * 3 + [o_shape]]
    dma = pltpu.SemaphoreType.DMA
    return pl.pallas_call(
        functools.partial(attn_kernel, layer, seq),
        out_shape=out_shape, in_specs=vmem_specs(2) + any_specs(3) + vmem_specs(2) + any_specs(1), out_specs=vmem_specs(1) + any_specs(4),
        scratch_shapes=layer_scratch(w_q, w_k, w_v, w_full) + [pltpu.VMEM(head_shape, BF16)] * 3 + [pltpu.VMEM(o_shape, BF16), dma((4,))]
        + [pltpu.VMEM((table.shape[0], seq, seq), F32), pltpu.VMEM((4, 256, cols), BF16), dma((2, 6)), dma((2, 6)), dma((3,)), dma((3,))],
        compiler_params=pltpu.CompilerParams(collective_id=collective_id, has_side_effects=True, vmem_limit_bytes=40 << 20),
        cost_estimate=pl.CostEstimate(flops=4 << 30, bytes_accessed=16 << 20, transcendentals=0),
        name=f"attn_fwd_{layer}",
    )(x.reshape(2, seq, width), gains, w_q, w_k, w_v, table, mask, w_full)


def gelu_parts(g):
    inner = np.float32(np.sqrt(2 / np.pi)) * (g + 0.044715 * (g * g * g))
    t = jnp.tanh(inner)
    cdf = 0.5 * (1.0 + t)
    slope = cdf + 0.5 * g * (1.0 - t * t) * np.float32(np.sqrt(2 / np.pi)) * (1.0 + 3 * 0.044715 * (g * g))
    return g * cdf, slope


def order(z, y):
    return [(1 - z, 1 - y), (1 - z, y), (z, 1 - y), (z, y)]


def mlp_fwd_kernel(layer, x1_ref, dy_ref, g_ref, wg_all, wl_all, wo_all, out_ref, dyo_ref, wg_ref, wl_ref, wo_ref, wsem,
                   part, near, far, send, recv, dsend, drecv, own_sem):
    loads = load_layer(layer, [wg_all, wl_all, wo_all], [wg_ref, wl_ref, wo_ref], wsem)
    tp, cp, z, y, x, core, ids = place()
    meet(ids, ['z', 'y', 'x', 'core', 'xc'])
    moves = [remote(dy_ref.at[ids[name]['cp']], dyo_ref.at[:, cp], dsend.at[i], drecv.at[i], ids[name])
             for i, name in enumerate(['x', 'xc', 'core'])]
    own = pltpu.make_async_copy(dy_ref.at[cp], dyo_ref.at[:, cp], own_sem)
    own.start()
    for copy in loads:
        copy.wait()
    zy, yz = streams = colours(part, near, far, lambda q, c: out_ref.at[q[0], q[1], c], send, recv, ids, z, y)

    def compute(q):
        h2 = norm(x1_ref[q].reshape(256, -1), g_ref[layer:layer + 1, :])
        gated = (gelu_parts(dot(h2, wg_ref[...], NT))[0] * dot(h2, wl_ref[...], NT)).astype(BF16)
        part[q] = dot(gated, wo_ref[...]).reshape(part.shape[2:])

    quarters = order(z, y)
    compute(quarters[0])
    zy.send_away(0)
    yz.send_away(0)
    compute(quarters[1])
    zy.send_away(1)
    compute(quarters[2])
    yz.send_away(1)
    compute(quarters[3])
    for s in streams:
        s.forward()
    for c, s in enumerate(streams):
        out_ref[z, y, c] = (x1_ref[z, y, c].astype(F32) + s.total()).astype(BF16)
        s.publish()
    for s in streams:
        s.gather()
    for s in streams:
        s.close()
    for copy in moves + [own]:
        copy.wait()


def sum_scratch(width, blocks=()):
    return [pltpu.VMEM((2, 2, 2) + blocks, F32), pltpu.VMEM((2, 2) + blocks, F32), pltpu.VMEM((2,) + blocks, F32)]


def mlp_fwd(layer, collective_id, x1, d_y, gains, wg_t, wl_t, w_out):
    dma = pltpu.SemaphoreType.DMA
    width = x1.shape[-1]
    return pl.pallas_call(
        functools.partial(mlp_fwd_kernel, layer),
        out_shape=[jax.ShapeDtypeStruct(x1.shape, BF16), jax.ShapeDtypeStruct((2, 4, 128, width), BF16)],
        in_specs=vmem_specs(3) + any_specs(3), out_specs=vmem_specs(1) + any_specs(1),
        scratch_shapes=layer_scratch(wg_t, wl_t, w_out) + sum_scratch(0, x1.shape[3:]) + [dma((2, 6)), dma((2, 6)), dma((3,)), dma((3,)), dma],
        compiler_params=pltpu.CompilerParams(collective_id=collective_id, has_side_effects=True, vmem_limit_bytes=40 << 20),
        cost_estimate=pl.CostEstimate(flops=5 << 30, bytes_accessed=16 << 20, transcendentals=0),
        name=f"mlp_fwd_{layer}",
    )(x1, d_y.reshape(4, 2, 128, width), gains, wg_t, wl_t, w_out)


def layer_bwd_kernel(layer, seq, last, *refs):
    refs = list(refs)
    take = lambda n: [refs.pop(0) for _ in range(n)]
    stacks = take(7)
    arrays = take(7)
    ga_ref, gm_ref, t_ref, mask_ref = take(4)
    if last:
        small_ref, = take(1)
    dx_ref, small_out = take(2)
    grad_out = take(7)
    weights, holds = take(7), take(7)
    wsem, hsem = take(2)
    wg_ref, wl_ref, wd_ref, wq_ref, wk_ref, wv_ref, wo_ref = weights
    x1_ref, dy_ref, x_ref, q_ref, k_ref, v_ref, o_ref = holds
    part, near, far, dm_ref, h_ref, gated_ref, dgate_ref, dlin_ref = take(8)
    bias_ref, do_ref, dq_ref, dk_ref, dv_ref, dt_ref = take(6)
    grad_scratch = [take(4) for _ in range(7)]
    send, recv, local = take(3)
    if last:
        own_ref, acc_small, got_small, csend, crecv = take(5)
    tp, cp, z, y, x, core, ids = place()
    w_loads = [pltpu.make_async_copy(w.at[layer], r, wsem.at[i]) for i, (w, r) in enumerate(zip(stacks, weights))]
    a_loads = [pltpu.make_async_copy(w, r, hsem.at[i]) for i, (w, r) in enumerate(zip(arrays, holds))]
    first_loads = [a_loads[0], w_loads[0], w_loads[1], a_loads[1], w_loads[2]]
    later_loads = a_loads[2:] + w_loads[3:]
    for copy in first_loads + later_loads:
        copy.start()
    meet(ids, ['z', 'y', 'x', 'core'] + (['xc'] if last else []))
    heads = t_ref.shape[0]
    width = x_ref.shape[-1]
    deep = 32 if last else 128
    across = 128 // deep
    g_out, g_gate, g_lin, g_o, g_q, g_k, g_v = grads = [
        GradStream(*grad_scratch[i], grad_out[i], send.at[4 + i], recv.at[4 + i], local.at[i], ids, x, core) for i in range(7)]
    p_out, p_gate, p_lin, p_o, p_q, p_k, p_v = [g[0] for g in grad_scratch]
    zy, yz = mlp_sum = colours(part, near, far, lambda q, c: dm_ref.at[q[0], q[1], c], send.at[0:2], recv.at[0:2], ids, z, y)
    for copy in first_loads:
        copy.wait()
    gain = gm_ref[layer:layer + 1, :]

    def mlp_quarter(q):
        h2 = norm(x1_ref[q].reshape(256, -1), gain)
        rows = pl.ds(pl.multiple_of((q[0] * 2 + q[1]) * 256, 256), 256)
        h_ref[rows, :] = h2
        value, slope = gelu_parts(dot(h2, wg_ref[...], NT))
        lin = dot(h2, wl_ref[...], NT)
        gated_ref[rows, :] = (value * lin).astype(BF16)
        d_gated = dot(dy_ref[q].reshape(256, -1), wd_ref[...], NT)
        d_lin = (d_gated * value).astype(BF16)
        d_gate = (d_gated * lin * slope).astype(BF16)
        dlin_ref[rows, :] = d_lin
        dgate_ref[rows, :] = d_gate
        part[q] = (dot(d_gate, wg_ref[...]) + dot(d_lin, wl_ref[...])).reshape(part.shape[2:])

    quarters = order(z, y)
    mlp_quarter(quarters[0])
    zy.send_away(0)
    yz.send_away(0)
    mlp_quarter(quarters[1])
    zy.send_away(1)
    mlp_quarter(quarters[2])
    yz.send_away(1)
    mlp_quarter(quarters[3])
    grad_into(p_out, gated_ref[...], dy_ref[...].reshape(h_ref.shape))
    g_out.send_both()
    grad_into(p_gate, dgate_ref[...], h_ref)
    g_gate.send_both()
    g_out.forward()
    for s in mlp_sum:
        s.forward()
    grad_into(p_lin, dlin_ref[...], h_ref)
    g_lin.send_both()
    g_gate.forward()
    for copy in later_loads:
        copy.wait()
    gain_a = ga_ref[layer:layer + 1, :]
    for b in range(2):
        h_ref[b * seq:(b + 1) * seq, :] = norm(x_ref[b], gain_a)
    g_lin.forward()
    g_out.finish()
    dg_m = 0.0
    for c, s in enumerate(mlp_sum):
        d_x, dg = norm_back(s.total(), x1_ref[z, y, c], gain)
        dm_ref[z, y, c] = (d_x + dy_ref[z, y, c].astype(F32)).astype(BF16)
        s.publish()
        dg_m = dg_m + jnp.sum(dg, axis=0, keepdims=True)
    g_gate.finish()
    for s in mlp_sum:
        s.gather()
    g_out.gather()
    for s in mlp_sum:
        s.close()

    if last:
        def region(q, c):
            return dx_ref.at[:, q[0], q[1], c]
    else:
        def region(q, c):
            return dx_ref.at[q[0], q[1], c]
    zy, yz = attn_sum = colours(part, near, far, region, send.at[2:4], recv.at[2:4], ids, z, y)

    def attend(b, step):
        add = key_add(mask_ref, b)
        do_ref[...] = dot(dm_ref[b].reshape(seq, width), wo_ref[...], NT).astype(BF16)
        for head in range(heads):
            bias_ref[...] = toeplitz(t_ref[head:head + 1, :], seq)
            cols = pl.ds(head * HEAD, HEAD)
            q, k, v, do = q_ref[b, :, cols], k_ref[b, :, cols], v_ref[b, :, cols], do_ref[:, cols]
            e, total = exp_scores(q, k, bias_ref[...], add)
            p = e * (1.0 / total)
            row_dot = jnp.sum(do.astype(F32) * o_ref[b, :, cols].astype(F32), axis=-1, keepdims=True)
            ds = p * (dot(do, v, NT) - row_dot)
            sums = diag_sums(ds, seq)
            dt_ref[head:head + 1, :] = sums if step == 0 else dt_ref[head:head + 1, :] + sums
            dsl = ds.astype(BF16)
            dq_ref[b, :, cols] = dot(dsl, k).astype(BF16)
            dk_ref[b, :, cols] = dot(dsl, q, TN).astype(BF16)
            dv_ref[b, :, cols] = dot(p.astype(BF16), do, TN).astype(BF16)
            if step == 1 and head == 0:
                g_o.forward()

    def pick(ref, q, offset, size):
        pieces = [ref[q[0], pl.ds(pl.multiple_of(j * 4 * deep + q[1] * 2 * deep + offset, deep), size), :] for j in range(across)]
        return pieces[0] if across == 1 else jnp.concatenate(pieces, axis=0)

    def attn_quarter(q):
        total = sum(dot(pick(d, q, 0, 2 * deep), w[...], NT) for d, w in [(dq_ref, wq_ref), (dk_ref, wk_ref), (dv_ref, wv_ref)])
        total = total.reshape(across, 2, deep, width)
        for c in range(2):
            part[q[0], q[1], c] = total[:, c].reshape(across * deep, width)

    attend(1 - z, 0)
    attn_quarter(quarters[0])
    zy.send_away(0)
    yz.send_away(0)
    attn_quarter(quarters[1])
    zy.send_away(1)
    grad_into(p_o, o_ref[...].reshape(2 * seq, -1), dm_ref[...].reshape(2 * seq, width))
    g_o.send_both()
    g_lin.finish()
    attend(z, 1)
    attn_quarter(quarters[2])
    yz.send_away(1)
    attn_quarter(quarters[3])
    for g, p, d in [(g_q, p_q, dq_ref), (g_k, p_k, dk_ref), (g_v, p_v, dv_ref)]:
        grad_into(p, h_ref[...], d[...].reshape(2 * seq, -1))
        g.send_both()
    for s in attn_sum:
        s.forward()
    for g in [g_q, g_k, g_v]:
        g.forward()
    g_gate.gather()
    g_lin.gather()
    g_o.finish()
    dg_a = 0.0
    moves = []
    dm_flat = dm_ref
    for c, s in enumerate(attn_sum):
        d_x, dg = norm_back(s.total(), pick(x_ref, (z, y), c * deep, deep), gain_a)
        dg_a = dg_a + jnp.sum(dg, axis=0, keepdims=True)
        if last:
            res = jnp.concatenate([dm_ref[z, j // 2, j % 2, pl.ds(pl.multiple_of(y * 2 * deep + c * deep, deep), deep), :] for j in range(4)], axis=0)
        else:
            res = dm_ref[z, y, c]
        d_x = (d_x + res.astype(F32)).astype(BF16)
        if last:
            own_ref[c] = d_x.reshape(across, deep, width)
            dx_ref[cp, z, y, c] = own_ref[c, cp]
            moves.append([remote(own_ref.at[c, ids[name]['cp']], dx_ref.at[cp, z, y, c], csend.at[c, i], crecv.at[c, i], ids[name])
                          for i, name in enumerate(['x', 'xc', 'core'])])
        else:
            dx_ref[z, y, c] = d_x
            s.publish()
    if not last:
        small_out[0:1, :] = dg_a
        small_out[1:2, :] = dg_m
        small_out[2:4, :] = jnp.zeros((2, width), F32)
        small_out[4:8, :] = dt_ref[0:4, :]
        for g in [g_q, g_k, g_v]:
            g.finish()
        for s in attn_sum:
            s.gather()
    else:
        acc_small[0, 0:2, :] = small_ref[0:2, :]
        acc_small[0, 2:3, :] = dg_a
        acc_small[0, 3:4, :] = dg_m
        acc_small[0, 4:8, :] = jnp.zeros((4, width), F32)
        acc_small[0, 8:12, :] = small_ref[4:8, :] + dt_ref[0:4, :]
        acc_small[0, 12:16, :] = jnp.zeros((4, width), F32)
        smalls = []

        def small_start(i):
            rows = pl.ds(0, 16 if i < 2 else 8)
            smalls.append(remote(acc_small.at[i, rows], got_small.at[i, rows], csend.at[2, i], crecv.at[2, i], ids[['z', 'y', 'core', 'x'][3 - i]]))

        def small_end(i):
            rows = pl.ds(0, 16 if i < 2 else 8)
            smalls[i].wait_recv()
            acc_small[i + 1, rows, :] = acc_small[i, rows, :] + got_small[i, rows, :]

        small_start(0)
        for c, s in enumerate(attn_sum):
            for copy in moves[c]:
                copy.wait_recv()
            s.publish()
        g_q.finish()
        small_end(0)
        small_start(1)
        g_k.finish()
        small_end(1)
        small_start(2)
        g_v.finish()
        for s in attn_sum:
            s.gather()
        small_end(2)
        small_start(3)
    g_o.gather()
    for g in [g_q, g_k, g_v]:
        g.gather()
    if last:
        small_end(3)
        small_out[0:8, :] = acc_small[4, 0:8, :]
        small_out[8:16, :] = acc_small[2, 8:16, :]
        for copy in smalls + moves[0] + moves[1]:
            copy.wait_send()
    for s in attn_sum + grads:
        s.close()


def layer_bwd(layer, collective_id, x1, dy, x, q, k, v, o, gains_a, gains_m, wg_t, wl_t, w_out, w_q, w_k, w_v, w_o, table, mask, small=None):
    seq, width, cols = 512, w_q.shape[1], w_q.shape[2]
    ff = w_out.shape[1]
    rows = 2 * seq
    last = small is not None
    dma = pltpu.SemaphoreType.DMA
    blocks = (2, 2, 2, 128, width)
    stacks = [wg_t, wl_t, w_out, w_q, w_k, w_v, w_o]
    arrays = [x1.reshape(blocks), dy.reshape(blocks), x.reshape(2, seq, width), q, k, v, o.reshape(2, seq, cols)]
    operands = stacks + arrays + [gains_a, gains_m, table, mask] + ([small] if last else [])
    in_specs = any_specs(14) + vmem_specs(5 if last else 4)
    out_shape = [jax.ShapeDtypeStruct((4, 2, 2, 2, 32, width) if last else blocks, BF16), jax.ShapeDtypeStruct((16 if last else 8, width), F32)]
    grads = [(ff // 4, width)] * 3 + [(cols // 4, width)] + [(width // 4, cols)] * 3
    out_shape += [jax.ShapeDtypeStruct((4,) + g, BF16) for g in grads]
    scratch = [pltpu.VMEM(w.shape[1:], BF16) for w in stacks] + [pltpu.VMEM(a.shape, BF16) for a in arrays] + [dma((7,)), dma((7,))]
    scratch += sum_scratch(0, blocks[3:]) + [pltpu.VMEM(blocks, BF16), pltpu.VMEM((rows, width), BF16)] + [pltpu.VMEM((rows, ff), BF16)] * 3
    scratch += [pltpu.VMEM((seq, seq), F32), pltpu.VMEM((seq, cols), BF16)] + [pltpu.VMEM((2, seq, cols), BF16)] * 3 + [pltpu.VMEM((8, 2 * seq), F32)]
    for g in grads:
        scratch += [pltpu.VMEM((4,) + g, F32), pltpu.VMEM((2,) + g, F32), pltpu.VMEM(g, F32), pltpu.VMEM(g, BF16)]
    scratch += [dma((11, 6)), dma((11, 6)), dma((7,))]
    if last:
        scratch += [pltpu.VMEM((2, 4, 32, width), BF16), pltpu.VMEM((5, 16, width), F32), pltpu.VMEM((4, 16, width), F32), dma((3, 4)), dma((3, 4))]
    return pl.pallas_call(
        functools.partial(layer_bwd_kernel, layer, seq, last),
        out_shape=out_shape, in_specs=in_specs, out_specs=vmem_specs(2) + any_specs(7),
        scratch_shapes=scratch,
        compiler_params=pltpu.CompilerParams(collective_id=collective_id, has_side_effects=True, vmem_limit_bytes=67043328),
        cost_estimate=pl.CostEstimate(flops=20 << 30, bytes_accessed=48 << 20, transcendentals=0),
        name=f"layer_bwd_{layer}",
    )(*operands)


def vmem_specs(n):
    return [pl.BlockSpec(memory_space=pltpu.VMEM)] * n


def solution(mesh):
    seq_spec = P(None, 'cp', None)
    col_spec = P(None, None, 'tp')
    row_spec = P(None, 'tp', None)
    weight_specs = (P(), P(), col_spec, col_spec, col_spec, row_spec, col_spec, col_spec, row_spec)

    def local_program(x_in, d_y, key_mask, rel_bias, g_attn, g_mlp, w_q, w_k, w_v, w_o, w_gate, w_lin, w_out):
        width = x_in.shape[2]
        quarters = (2, 2, 2, 128, width)
        onehot = bucket_onehot(512)
        table = jnp.sum(jnp.where(onehot[None], rel_bias.T[:, :, None], 0.0), axis=1)
        wg_t, wl_t = jnp.swapaxes(w_gate, 1, 2), jnp.swapaxes(w_lin, 1, 2)
        x0, mask, w_full = exchange(x_in, key_mask, w_o)

        a0, q0, k0, v0, o0 = attn_layer(0, 1, x0, g_attn, w_q, w_k, w_v, table, mask, w_full)
        x1, dy = mlp_fwd(0, 2, a0, d_y, g_mlp, wg_t, wl_t, w_out)
        a1, q1, k1, v1, o1 = attn_layer(1, 3, x1, g_attn, w_q, w_k, w_v, table, mask, w_full)

        rest = (g_attn, g_mlp, wg_t, wl_t, w_out, w_q, w_k, w_v, w_o, table, mask)
        dx, small, out1, gate1, lin1, wo1, wq1, wk1, wv1 = layer_bwd(1, 4, a1, dy, x1, q1, k1, v1, o1, *rest)
        d_x, small, out0, gate0, lin0, wo0, wq0, wk0, wv0 = layer_bwd(0, 5, a0, dx, x0, q0, k0, v0, o0, *rest, small)

        def both(first, second, like, swap=False):
            shape = (like.shape[2], like.shape[1]) if swap else like.shape[1:]
            pair = jnp.stack([first.reshape(shape), second.reshape(shape)])
            return jnp.swapaxes(pair, 1, 2) if swap else pair

        d_bias = jnp.sum(jnp.where(onehot[None], small[8:12][:, None, :], 0.0), axis=2).T
        d_ga = jnp.stack([small[2], small[0]])
        d_gm = jnp.stack([small[3], small[1]])
        return (d_x.reshape(x_in.shape), d_bias, d_ga, d_gm, both(wq0, wq1, w_q), both(wk0, wk1, w_k), both(wv0, wv1, w_v),
                both(wo0, wo1, w_o), both(gate0, gate1, w_gate, True), both(lin0, lin1, w_lin, True), both(out0, out1, w_out))

    return jax.shard_map(local_program, mesh=mesh, in_specs=(seq_spec, seq_spec, P(None, 'cp'), P(None, 'tp')) + weight_specs, out_specs=(seq_spec, P(None, 'tp')) + weight_specs, check_vma=False)
```

```python
import functools
import jax
import jax.numpy as jnp
import numpy as np
from jax import lax
from jax.experimental import pallas as pl
from jax.experimental.pallas import tpu as pltpu
from jax.sharding import PartitionSpec as P

NORM_EPS = 1e-6
MASK_NEG = -1e9
HEAD = 64
F32 = jnp.float32
BF16 = jnp.bfloat16
NT = (((1,), (1,)), ((), ()))
TN = (((0,), (0,)), ((), ()))


def rel_bucket(rel_pos):
    distance = jnp.minimum(jnp.abs(rel_pos), 128)
    distance_sq = distance * distance
    log_part = 8 + sum((distance_sq >= 64 * 2 ** power).astype(jnp.int32) for power in range(1, 8))
    return jnp.where(distance < 8, distance, log_part) + 16 * (rel_pos > 0).astype(jnp.int32)


def bucket_onehot(seq):
    rel = jnp.arange(2 * seq) - seq
    return (rel_bucket(rel)[None, :] == jnp.arange(32)[:, None]) & (jnp.arange(2 * seq) > 0)[None, :]


def dot(a, b, dims=(((1,), (0,)), ((), ()))):
    return lax.dot_general(a, b, dims, preferred_element_type=F32)


def toeplitz(row, seq):
    base = pltpu.roll(row, seq, 1)
    rows = jnp.concatenate([base if i == 0 else pltpu.roll(base, i, 1) for i in range(8)], axis=0)
    size = 8
    while size < seq:
        rows = jnp.concatenate([rows, pltpu.roll(rows, size, 1)], axis=0)
        size *= 2
    return rows[:, :seq]


def diag_sums(mat, seq):
    wide = jnp.concatenate([mat, jnp.zeros_like(mat)], axis=1)
    size = seq
    while size > 1:
        half = size // 2
        wide = wide[:half] + pltpu.roll(wide[half:size], 2 * seq - half, 1)
        size = half
    return pltpu.roll(wide, seq, 1)


def place():
    tp, cp = lax.axis_index('tp'), lax.axis_index('cp')
    z, y = tp // 2, tp % 2
    x, core = cp // 2, cp % 2
    peers = {'z': (1 - z, y, x, core), 'y': (z, 1 - y, x, core), 'x': (z, y, 1 - x, core), 'core': (z, y, x, 1 - core),
             'zy': (1 - z, 1 - y, x, core), 'xc': (z, y, 1 - x, 1 - core)}
    ids = {name: {'tp': p[0] * 2 + p[1], 'cp': p[2] * 2 + p[3]} for name, p in peers.items()}
    return tp, cp, z, y, x, core, ids


def meet(ids, names):
    barrier = pltpu.get_barrier_semaphore()
    for name in names:
        pl.semaphore_signal(barrier, inc=1, device_id=ids[name], device_id_type=pl.DeviceIdType.MESH)
    pl.semaphore_wait(barrier, len(names))


def remote(src, dst, send, recv, target):
    copy = pltpu.make_async_remote_copy(src_ref=src, dst_ref=dst, send_sem=send, recv_sem=recv,
                                        device_id=target, device_id_type=pl.DeviceIdType.MESH)
    copy.start()
    return copy


class Stream:
    def __init__(self, part, near, far, out, send, recv, first, second, a, b, index):
        self.part, self.near, self.far, self.out = part, near, far, out
        self.send, self.recv = send, recv
        self.first, self.second = first, second
        self.own, self.pass_on = index(a, b), index(a, 1 - b)
        self.away_far, self.away = index(1 - a, 1 - b), index(1 - a, b)
        self.copies = {}

    def start(self, slot, src, dst, target):
        self.copies[slot] = remote(src, dst, self.send.at[slot], self.recv.at[slot], target)

    def send_away(self, slot):
        quarter = self.away_far if slot == 0 else self.away
        self.start(slot, self.part(quarter), self.near.at[slot], self.first)

    def forward(self):
        self.copies[0].wait_recv()
        ref = self.part(self.pass_on)
        ref[...] += self.near[0]
        self.start(2, ref, self.far, self.second)

    def total(self):
        self.copies[1].wait_recv()
        self.copies[2].wait_recv()
        return self.part(self.own)[...] + self.near[1] + self.far[...]

    def publish(self):
        out = self.out(self.own)
        self.start(3, out, out, self.first)
        self.start(4, out, out, self.second)

    def finish(self):
        self.out(self.own)[...] = self.total().astype(BF16)
        self.publish()

    def gather(self):
        self.copies[4].wait_recv()
        out = self.out(self.pass_on)
        self.start(5, out, out, self.first)

    def close(self):
        self.copies[3].wait_recv()
        self.copies[5].wait_recv()
        for copy in self.copies.values():
            copy.wait_send()


def colours(part, near, far, out, send, recv, ids, z, y):
    def make(c, first, second, a, b, index):
        return Stream(lambda q: part.at[q[0], q[1], c], None if near is None else near.at[c], None if far is None else far.at[c],
                      lambda q: out(q, c), send.at[c], recv.at[c], ids[first], ids[second], a, b, index)
    return [make(0, 'z', 'y', z, y, lambda a, b: (a, b)), make(1, 'y', 'z', y, z, lambda a, b: (b, a))]


class GradStream(Stream):
    def __init__(self, part, near, far, own_ref, out, send, recv, local, ids, x, core):
        super().__init__(lambda q: part.at[q], near, far, lambda q: out.at[q], send, recv,
                         ids['core'], ids['x'], core, x, lambda a, b: b * 2 + a)
        self.own_ref, self.local = own_ref, local

    def send_both(self):
        self.send_away(0)
        self.send_away(1)

    def finish(self):
        self.own_ref[...] = self.total().astype(BF16)
        out = self.out(self.own)
        self.start(4, self.own_ref, out, self.second)
        self.start(3, self.own_ref, out, self.first)
        self.kept = pltpu.make_async_copy(self.own_ref, out, self.local)
        self.kept.start()

    def close(self):
        super().close()
        self.kept.wait()


def grad_into(part, a, b):
    quarter, width = part.shape[1], part.shape[2]
    for lo in range(0, width, 256):
        block = dot(a, b[:, lo:lo + 256], TN)
        for q in range(4):
            part[q, :, lo:lo + 256] = block[q * quarter:(q + 1) * quarter]


def norm_parts(rows):
    xf = rows.astype(F32)
    inv = lax.rsqrt(jnp.mean(xf * xf, axis=-1, keepdims=True) + NORM_EPS)
    return inv, xf * inv


def norm(rows, gain):
    return (norm_parts(rows)[1] * gain).astype(BF16)


def norm_back(d_norm, rows, gain):
    inv, normed = norm_parts(rows)
    d_normed = d_norm * gain
    return inv * (d_normed - normed * jnp.mean(d_normed * normed, axis=-1, keepdims=True)), d_norm * normed


def key_add(mask_ref, b):
    row = jnp.concatenate([mask_ref[j, pl.ds(b, 1), :] for j in range(4)], axis=1)
    return jnp.where(row > 0, 0.0, MASK_NEG).astype(F32)


def exp_scores(q, k, bias, add):
    s = dot(q, k, NT) + bias + add
    e = jnp.exp(s - jnp.max(s, axis=-1, keepdims=True))
    return e, jnp.sum(e, axis=-1, keepdims=True)


def any_specs(n):
    return [pl.BlockSpec(memory_space=pl.ANY)] * n


def gelu_parts(g):
    inner = np.float32(np.sqrt(2 / np.pi)) * (g + 0.044715 * (g * g * g))
    t = jnp.tanh(inner)
    cdf = 0.5 * (1.0 + t)
    slope = cdf + 0.5 * g * (1.0 - t * t) * np.float32(np.sqrt(2 / np.pi)) * (1.0 + 3 * 0.044715 * (g * g))
    return g * cdf, slope


def order(z, y):
    return [(1 - z, 1 - y), (1 - z, y), (z, 1 - y), (z, y)]


def sum_scratch(width, blocks=()):
    return [pltpu.VMEM((2, 2, 2) + blocks, F32), pltpu.VMEM((2, 2) + blocks, F32), pltpu.VMEM((2,) + blocks, F32)]


def forward_kernel(seq, *refs):
    refs = list(refs)
    take = lambda n: [refs.pop(0) for _ in range(n)]
    x_in, d_y, wo_in, wq_in, wk_in, wv_in, wg_in, wl_in, wd_in, mask_in, ga_ref, gm_ref, t_ref = take(13)
    x0_out, a0_out, x1_out, a1_out, dy_out, q_out, k_out, v_out, o_out, mask_ref = take(10)
    x0_ref, a0_ref, x1_ref, a1_ref, dyo_ref, q_ref, k_ref, v_ref, o_ref = take(9)
    wq_ref, wk_ref, wv_ref, wg_ref, wl_ref, wd_ref, wf_ref = take(7)
    bias_ref, of_ref, part, near, far = take(5)
    xsend, xrecv, osend, orecv, send, recv, lsem, ssem = refs
    tp, cp, z, y, x, core, ids = place()
    near_by, far_by = ['core', 'x', 'xc'], ['z', 'y', 'zy']

    def local(src, dst, sem):
        copy = pltpu.make_async_copy(src, dst, sem)
        copy.start()
        return copy

    own_x = local(x_in.at[cp], x0_ref.at[:, cp], lsem.at[0])
    qkv_loads = [local(w, r, lsem.at[1 + i]) for i, (w, r) in enumerate([(wq_in, wq_ref), (wk_in, wk_ref), (wv_in, wv_ref)])]
    own_w = [local(wo_in.at[layer], wf_ref.at[layer, tp], lsem.at[4 + layer]) for layer in range(2)]
    mlp_loads = [local(w.at[0], r, lsem.at[6 + i]) for i, (w, r) in enumerate([(wg_in, wg_ref), (wl_in, wl_ref), (wd_in, wd_ref)])]
    own_dy = local(d_y.at[cp], dyo_ref, lsem.at[9])
    meet(ids, near_by + far_by)
    masks, xs = [], []
    for i, name in enumerate(near_by):
        masks.append(remote(mask_in.at[ids[name]['cp']], mask_ref.at[cp], xsend.at[i], xrecv.at[i], ids[name]))
        xs.append(remote(x_in.at[ids[name]['cp']], x0_ref.at[:, cp], xsend.at[3 + i], xrecv.at[3 + i], ids[name]))
    weights = [remote(wo_in.at[core], wf_ref.at[core, tp], xsend.at[6 + i], xrecv.at[6 + i], ids[name]) for i, name in enumerate(far_by)]
    mask_ref[cp] = mask_in[cp]
    for head in range(t_ref.shape[0]):
        bias_ref[head] = toeplitz(t_ref[head:head + 1, :], seq)

    def project(layer, rows):
        h = norm(rows, ga_ref[layer:layer + 1, :])
        return [dot(h, w[layer]).astype(BF16) for w in (wq_ref, wk_ref, wv_ref)]

    def attention(layer, b):
        add = key_add(mask_ref, b)
        for head in range(t_ref.shape[0]):
            cols = pl.ds(head * HEAD, HEAD)
            e, total = exp_scores(q_ref[layer, b, :, cols], k_ref[layer, b, :, cols], bias_ref[head], add)
            o = (dot(e.astype(BF16), v_ref[layer, b, :, cols]) / total).astype(BF16)
            o_ref[layer, b, 0, :, cols] = o[:seq // 2]
            o_ref[layer, b, 1, :, cols] = o[seq // 2:]

    def ship(layer, name, b, half):
        i = layer * 3 + far_by.index(name)
        return remote(o_ref.at[layer, b, half], of_ref.at[layer, tp], osend.at[i], orecv.at[i], ids[name])

    def project_out(layer, sent, residual, out_ref):
        of_ref[layer, tp] = o_ref[layer, z, y]
        for copy in sent:
            copy.wait_recv()
        streams = colours(None, None, None, lambda q, c: out_ref.at[q[0], q[1], c], send.at[4 * layer:4 * layer + 2], recv.at[4 * layer:4 * layer + 2], ids, z, y)
        for c, s in enumerate(streams):
            rows = pl.ds(c * 128, 128)
            total = sum(dot(of_ref[layer, j, rows, :], wf_ref[layer, j]) for j in range(4))
            out_ref[z, y, c] = (residual(c).astype(F32) + total).astype(BF16)
            s.publish()
        for s in streams:
            s.gather()
        for s in streams:
            s.close()

    for copy in qkv_loads:
        copy.wait()
    for i, name in enumerate(['own'] + near_by):
        if i == 0:
            own_x.wait()
            blk = cp
        else:
            xs[i - 1].wait_recv()
            blk = ids[name]['cp']
        for d_ref, value in zip((q_ref, k_ref, v_ref), project(0, x0_ref[:, blk].reshape(2 * 128, -1))):
            for b in range(2):
                d_ref[0, b, pl.ds(pl.multiple_of(blk * 128, 128), 128), :] = value[b * 128:(b + 1) * 128]
    own_dy.wait()
    saves = [local(x0_ref, x0_out, ssem.at[0]), local(dyo_ref, dy_out.at[:, cp], ssem.at[1])]
    moves = [remote(d_y.at[ids[name]['cp']], dy_out.at[:, cp], xsend.at[12 + i], xrecv.at[12 + i], ids[name]) for i, name in enumerate(near_by)]
    for copy in masks:
        copy.wait_recv()
    attention(0, 1 - z)
    sent = [ship(0, 'zy', 1 - z, 1 - y), ship(0, 'z', 1 - z, y)]
    passed = []
    for i, name in enumerate(far_by):
        weights[i].wait_recv()
        got = wf_ref.at[core, ids[name]['tp']]
        passed.append(remote(got, got, xsend.at[9 + i], xrecv.at[9 + i], ids['core']))
    attention(0, z)
    sent.append(ship(0, 'y', z, 1 - y))
    for copy in own_w:
        copy.wait()
    for copy in passed:
        copy.wait_recv()
    project_out(0, sent, lambda c: x0_ref[z, y * 2 + c], a0_ref)
    saves.append(local(a0_ref, a0_out, ssem.at[2]))

    for copy in mlp_loads:
        copy.wait()
    zy, yz = streams = colours(part, near, far, lambda q, c: x1_ref.at[q[0], q[1], c], send.at[2:4], recv.at[2:4], ids, z, y)

    def mlp_quarter(q):
        h2 = norm(a0_ref[q].reshape(256, -1), gm_ref[0:1, :])
        gated = (gelu_parts(dot(h2, wg_ref[...], NT))[0] * dot(h2, wl_ref[...], NT)).astype(BF16)
        part[q] = dot(gated, wd_ref[...]).reshape(part.shape[2:])

    quarters = order(z, y)
    mlp_quarter(quarters[0])
    zy.send_away(0)
    yz.send_away(0)
    mlp_quarter(quarters[1])
    zy.send_away(1)
    mlp_quarter(quarters[2])
    yz.send_away(1)
    mlp_quarter(quarters[3])
    for s in streams:
        s.forward()
    for c, s in enumerate(streams):
        x1_ref[z, y, c] = (a0_ref[z, y, c].astype(F32) + s.total()).astype(BF16)
        s.publish()
    for s in streams:
        s.gather()
    for s in streams:
        s.close()
    saves.append(local(x1_ref, x1_out, ssem.at[3]))

    late = []
    for step in range(2):
        b = 1 - z if step == 0 else z
        for half in range(2):
            rows = pl.ds(half * 256, 256)
            for d_ref, value in zip((q_ref, k_ref, v_ref), project(1, x1_ref[b, half].reshape(256, -1))):
                d_ref[1, b, rows, :] = value
        attention(1, b)
        if step == 0:
            late += [ship(1, 'zy', b, 1 - y), ship(1, 'z', b, y)]
        else:
            late.append(ship(1, 'y', b, 1 - y))
    saves += [local(src, dst, ssem.at[4 + i]) for i, (src, dst) in enumerate([(q_ref, q_out), (k_ref, k_out), (v_ref, v_out), (o_ref, o_out)])]
    project_out(1, late, lambda c: x1_ref[z, y, c], a1_ref)
    saves.append(local(a1_ref, a1_out, ssem.at[8]))
    for copy in masks + xs + weights + passed + sent + late:
        copy.wait_send()
    for copy in moves + saves:
        copy.wait()


def forward(x_in, d_y, key_mask, gains_a, gains_m, w_q, w_k, w_v, w_o, wg_t, wl_t, w_out, table):
    batch, blk, width = x_in.shape
    seq, cols = 4 * blk, w_q.shape[2]
    dma = pltpu.SemaphoreType.DMA
    blocks = (2, 2, 2, blk, width)
    arrived = (2, 4, blk, width)
    heads = (2, 2, seq, cols)
    halves = (2, 2, 2, seq // 2, cols)
    hbm = [arrived, blocks, blocks, blocks, arrived, heads, heads, heads, halves]
    operands = [x_in.reshape(4, 2, blk, width), d_y.reshape(4, 2, blk, width), w_o, w_q, w_k, w_v, wg_t, wl_t, w_out,
                key_mask.reshape(4, 2, blk), gains_a, gains_m, table]
    scratch = [pltpu.VMEM(h, BF16) for h in hbm[:4] + [(2, blk, width)] + hbm[5:]]
    scratch += [pltpu.VMEM(w.shape, BF16) for w in (w_q, w_k, w_v)] + [pltpu.VMEM(w.shape[1:], BF16) for w in (wg_t, wl_t, w_out)]
    scratch += [pltpu.VMEM((2, 4) + w_o.shape[1:], BF16), pltpu.VMEM((table.shape[0], seq, seq), F32), pltpu.VMEM((2, 4, 2 * blk, cols), BF16)]
    scratch += sum_scratch(0, blocks[3:])
    scratch += [dma((15,)), dma((15,)), dma((6,)), dma((6,)), dma((6, 6)), dma((6, 6)), dma((10,)), dma((9,))]
    return pl.pallas_call(
        functools.partial(forward_kernel, seq),
        out_shape=[jax.ShapeDtypeStruct(h, BF16) for h in hbm] + [jax.ShapeDtypeStruct((4, 2, blk), jnp.int32)],
        in_specs=any_specs(9) + vmem_specs(4), out_specs=any_specs(9) + vmem_specs(1),
        scratch_shapes=scratch,
        compiler_params=pltpu.CompilerParams(collective_id=0, has_side_effects=True, vmem_limit_bytes=62 << 20),
        cost_estimate=pl.CostEstimate(flops=15 << 30, bytes_accessed=48 << 20, transcendentals=0),
        name="forward",
    )(*operands)


def layer_bwd_kernel(layer, seq, last, *refs):
    refs = list(refs)
    take = lambda n: [refs.pop(0) for _ in range(n)]
    stacks = take(7)
    arrays = take(7)
    ga_ref, gm_ref, t_ref, mask_ref = take(4)
    if last:
        small_ref, = take(1)
    dx_ref, small_out = take(2)
    grad_out = take(7)
    weights, holds = take(7), take(7)
    wsem, hsem = take(2)
    wg_ref, wl_ref, wd_ref, wq_ref, wk_ref, wv_ref, wo_ref = weights
    x1_ref, dy_ref, x_ref, q_ref, k_ref, v_ref, o_ref = holds
    part, near, far, dm_ref, h_ref, gated_ref, dgate_ref, dlin_ref = take(8)
    bias_ref, do_ref, dq_ref, dk_ref, dv_ref, dt_ref = take(6)
    grad_scratch = [take(4) for _ in range(7)]
    send, recv, local = take(3)
    if last:
        own_ref, acc_small, got_small, csend, crecv = take(5)
    tp, cp, z, y, x, core, ids = place()
    w_loads = [pltpu.make_async_copy(w.at[layer], r, wsem.at[i]) for i, (w, r) in enumerate(zip(stacks, weights))]
    a_loads = [pltpu.make_async_copy(w if i < 3 else w.at[layer], r, hsem.at[i]) for i, (w, r) in enumerate(zip(arrays, holds))]
    first_loads = [a_loads[0], w_loads[0], w_loads[1], a_loads[1], w_loads[2]]
    later_loads = a_loads[2:] + w_loads[3:]
    for copy in first_loads + later_loads:
        copy.start()
    meet(ids, ['z', 'y', 'x', 'core'] + (['xc'] if last else []))
    heads = t_ref.shape[0]
    width = x_ref.shape[-1]
    deep = 32 if last else 128
    across = 128 // deep
    g_out, g_gate, g_lin, g_o, g_q, g_k, g_v = grads = [
        GradStream(*grad_scratch[i], grad_out[i], send.at[4 + i], recv.at[4 + i], local.at[i], ids, x, core) for i in range(7)]
    p_out, p_gate, p_lin, p_o, p_q, p_k, p_v = [g[0] for g in grad_scratch]
    zy, yz = mlp_sum = colours(part, near, far, lambda q, c: dm_ref.at[q[0], q[1], c], send.at[0:2], recv.at[0:2], ids, z, y)
    for copy in first_loads:
        copy.wait()
    gain = gm_ref[layer:layer + 1, :]

    def mlp_quarter(q):
        h2 = norm(x1_ref[q].reshape(256, -1), gain)
        rows = pl.ds(pl.multiple_of((q[0] * 2 + q[1]) * 256, 256), 256)
        h_ref[rows, :] = h2
        value, slope = gelu_parts(dot(h2, wg_ref[...], NT))
        lin = dot(h2, wl_ref[...], NT)
        gated_ref[rows, :] = (value * lin).astype(BF16)
        d_gated = dot(dy_ref[q].reshape(256, -1), wd_ref[...], NT)
        d_lin = (d_gated * value).astype(BF16)
        d_gate = (d_gated * lin * slope).astype(BF16)
        dlin_ref[rows, :] = d_lin
        dgate_ref[rows, :] = d_gate
        part[q] = (dot(d_gate, wg_ref[...]) + dot(d_lin, wl_ref[...])).reshape(part.shape[2:])

    quarters = order(z, y)
    mlp_quarter(quarters[0])
    zy.send_away(0)
    yz.send_away(0)
    mlp_quarter(quarters[1])
    zy.send_away(1)
    mlp_quarter(quarters[2])
    yz.send_away(1)
    mlp_quarter(quarters[3])
    grad_into(p_out, gated_ref[...], dy_ref[...].reshape(h_ref.shape))
    g_out.send_both()
    grad_into(p_gate, dgate_ref[...], h_ref)
    g_gate.send_both()
    g_out.forward()
    for s in mlp_sum:
        s.forward()
    grad_into(p_lin, dlin_ref[...], h_ref)
    g_lin.send_both()
    g_gate.forward()
    for copy in later_loads:
        copy.wait()
    gain_a = ga_ref[layer:layer + 1, :]
    for b in range(2):
        h_ref[b * seq:(b + 1) * seq, :] = norm(x_ref[b], gain_a)
    g_lin.forward()
    g_out.finish()
    dg_m = 0.0
    for c, s in enumerate(mlp_sum):
        d_x, dg = norm_back(s.total(), x1_ref[z, y, c], gain)
        dm_ref[z, y, c] = (d_x + dy_ref[z, y, c].astype(F32)).astype(BF16)
        s.publish()
        dg_m = dg_m + jnp.sum(dg, axis=0, keepdims=True)
    g_gate.finish()
    for s in mlp_sum:
        s.gather()
    for s in mlp_sum:
        s.close()

    if last:
        def region(q, c):
            return dx_ref.at[:, q[0], q[1], c]
    else:
        def region(q, c):
            return dx_ref.at[q[0], q[1], c]
    zy, yz = attn_sum = colours(part, near, far, region, send.at[2:4], recv.at[2:4], ids, z, y)

    def attend(b, step):
        add = key_add(mask_ref, b)
        do_ref[...] = dot(dm_ref[b].reshape(seq, width), wo_ref[...], NT).astype(BF16)
        for head in range(heads):
            bias_ref[...] = toeplitz(t_ref[head:head + 1, :], seq)
            cols = pl.ds(head * HEAD, HEAD)
            q, k, v, do = q_ref[b, :, cols], k_ref[b, :, cols], v_ref[b, :, cols], do_ref[:, cols]
            e, total = exp_scores(q, k, bias_ref[...], add)
            p = e * (1.0 / total)
            row_dot = jnp.sum(do.astype(F32) * o_ref[b, :, cols].astype(F32), axis=-1, keepdims=True)
            ds = p * (dot(do, v, NT) - row_dot)
            sums = diag_sums(ds, seq)
            dt_ref[head:head + 1, :] = sums if step == 0 else dt_ref[head:head + 1, :] + sums
            dsl = ds.astype(BF16)
            dq_ref[b, :, cols] = dot(dsl, k).astype(BF16)
            dk_ref[b, :, cols] = dot(dsl, q, TN).astype(BF16)
            dv_ref[b, :, cols] = dot(p.astype(BF16), do, TN).astype(BF16)
            if step == 1 and head == 0:
                g_o.forward()

    def pick(ref, q, offset, size):
        pieces = [ref[q[0], pl.ds(pl.multiple_of(j * 4 * deep + q[1] * 2 * deep + offset, deep), size), :] for j in range(across)]
        return pieces[0] if across == 1 else jnp.concatenate(pieces, axis=0)

    def attn_quarter(q):
        total = sum(dot(pick(d, q, 0, 2 * deep), w[...], NT) for d, w in [(dq_ref, wq_ref), (dk_ref, wk_ref), (dv_ref, wv_ref)])
        total = total.reshape(across, 2, deep, width)
        for c in range(2):
            part[q[0], q[1], c] = total[:, c].reshape(across * deep, width)

    attend(1 - z, 0)
    attn_quarter(quarters[0])
    zy.send_away(0)
    yz.send_away(0)
    attn_quarter(quarters[1])
    zy.send_away(1)
    grad_into(p_o, o_ref[...].reshape(2 * seq, -1), dm_ref[...].reshape(2 * seq, width))
    g_o.send_both()
    g_lin.finish()
    g_out.gather()
    attend(z, 1)
    attn_quarter(quarters[2])
    yz.send_away(1)
    attn_quarter(quarters[3])
    for g, p, d in [(g_q, p_q, dq_ref), (g_k, p_k, dk_ref), (g_v, p_v, dv_ref)]:
        grad_into(p, h_ref[...], d[...].reshape(2 * seq, -1))
        g.send_both()
    for s in attn_sum:
        s.forward()
    for g in [g_q, g_k, g_v]:
        g.forward()
    g_gate.gather()
    g_lin.gather()
    g_o.finish()
    dg_a = 0.0
    moves = []
    dm_flat = dm_ref
    for c, s in enumerate(attn_sum):
        d_x, dg = norm_back(s.total(), pick(x_ref, (z, y), c * deep, deep), gain_a)
        dg_a = dg_a + jnp.sum(dg, axis=0, keepdims=True)
        if last:
            res = jnp.concatenate([dm_ref[z, j // 2, j % 2, pl.ds(pl.multiple_of(y * 2 * deep + c * deep, deep), deep), :] for j in range(4)], axis=0)
        else:
            res = dm_ref[z, y, c]
        d_x = (d_x + res.astype(F32)).astype(BF16)
        if last:
            own_ref[c] = d_x.reshape(across, deep, width)
            dx_ref[cp, z, y, c] = own_ref[c, cp]
            moves.append([remote(own_ref.at[c, ids[name]['cp']], dx_ref.at[cp, z, y, c], csend.at[c, i], crecv.at[c, i], ids[name])
                          for i, name in enumerate(['x', 'xc', 'core'])])
        else:
            dx_ref[z, y, c] = d_x
            s.publish()
    if not last:
        small_out[0:1, :] = dg_a
        small_out[1:2, :] = dg_m
        small_out[2:4, :] = jnp.zeros((2, width), F32)
        small_out[4:8, :] = dt_ref[0:4, :]
        for g in [g_q, g_k, g_v]:
            g.finish()
        for s in attn_sum:
            s.gather()
    else:
        acc_small[0, 0:2, :] = small_ref[0:2, :]
        acc_small[0, 2:3, :] = dg_a
        acc_small[0, 3:4, :] = dg_m
        acc_small[0, 4:8, :] = jnp.zeros((4, width), F32)
        acc_small[0, 8:12, :] = small_ref[4:8, :] + dt_ref[0:4, :]
        acc_small[0, 12:16, :] = jnp.zeros((4, width), F32)
        smalls = []

        def small_start(i):
            rows = pl.ds(0, 16 if i < 2 else 8)
            smalls.append(remote(acc_small.at[i, rows], got_small.at[i, rows], csend.at[2, i], crecv.at[2, i], ids[['z', 'y', 'core', 'x'][3 - i]]))

        def small_end(i):
            rows = pl.ds(0, 16 if i < 2 else 8)
            smalls[i].wait_recv()
            acc_small[i + 1, rows, :] = acc_small[i, rows, :] + got_small[i, rows, :]

        small_start(0)
        for c, s in enumerate(attn_sum):
            for copy in moves[c]:
                copy.wait_recv()
            s.publish()
        g_q.finish()
        small_end(0)
        small_start(1)
        g_k.finish()
        small_end(1)
        small_start(2)
        g_v.finish()
        for s in attn_sum:
            s.gather()
        small_end(2)
        small_start(3)
    g_o.gather()
    for g in [g_q, g_k, g_v]:
        g.gather()
    if last:
        small_end(3)
        small_out[0:8, :] = acc_small[4, 0:8, :]
        small_out[8:16, :] = acc_small[2, 8:16, :]
        for copy in smalls + moves[0] + moves[1]:
            copy.wait_send()
    for s in attn_sum + grads:
        s.close()


def layer_bwd(layer, collective_id, x1, dy, x, q, k, v, o, gains_a, gains_m, wg_t, wl_t, w_out, w_q, w_k, w_v, w_o, table, mask, small=None):
    seq, width, cols = 512, w_q.shape[1], w_q.shape[2]
    ff = w_out.shape[1]
    rows = 2 * seq
    last = small is not None
    dma = pltpu.SemaphoreType.DMA
    blocks = (2, 2, 2, 128, width)
    stacks = [wg_t, wl_t, w_out, w_q, w_k, w_v, w_o]
    arrays = [x1.reshape(blocks), dy.reshape(blocks), x.reshape(2, seq, width), q, k, v, o.reshape(2, 2, seq, cols)]
    operands = stacks + arrays + [gains_a, gains_m, table, mask] + ([small] if last else [])
    in_specs = any_specs(14) + vmem_specs(5 if last else 4)
    out_shape = [jax.ShapeDtypeStruct((4, 2, 2, 2, 32, width) if last else blocks, BF16), jax.ShapeDtypeStruct((16 if last else 8, width), F32)]
    grads = [(ff // 4, width)] * 3 + [(cols // 4, width)] + [(width // 4, cols)] * 3
    out_shape += [jax.ShapeDtypeStruct((4,) + g, BF16) for g in grads]
    scratch = [pltpu.VMEM(w.shape[1:], BF16) for w in stacks] + [pltpu.VMEM(a.shape if i < 3 else a.shape[1:], BF16) for i, a in enumerate(arrays)] + [dma((7,)), dma((7,))]
    scratch += sum_scratch(0, blocks[3:]) + [pltpu.VMEM(blocks, BF16), pltpu.VMEM((rows, width), BF16)] + [pltpu.VMEM((rows, ff), BF16)] * 3
    scratch += [pltpu.VMEM((seq, seq), F32), pltpu.VMEM((seq, cols), BF16)] + [pltpu.VMEM((2, seq, cols), BF16)] * 3 + [pltpu.VMEM((8, 2 * seq), F32)]
    for g in grads:
        scratch += [pltpu.VMEM((4,) + g, F32), pltpu.VMEM((2,) + g, F32), pltpu.VMEM(g, F32), pltpu.VMEM(g, BF16)]
    scratch += [dma((11, 6)), dma((11, 6)), dma((7,))]
    if last:
        scratch += [pltpu.VMEM((2, 4, 32, width), BF16), pltpu.VMEM((5, 16, width), F32), pltpu.VMEM((4, 16, width), F32), dma((3, 4)), dma((3, 4))]
    return pl.pallas_call(
        functools.partial(layer_bwd_kernel, layer, seq, last),
        out_shape=out_shape, in_specs=in_specs, out_specs=vmem_specs(2) + any_specs(7),
        scratch_shapes=scratch,
        compiler_params=pltpu.CompilerParams(collective_id=collective_id, has_side_effects=True, vmem_limit_bytes=67043328),
        cost_estimate=pl.CostEstimate(flops=20 << 30, bytes_accessed=48 << 20, transcendentals=0),
        name=f"layer_bwd_{layer}",
    )(*operands)


def vmem_specs(n):
    return [pl.BlockSpec(memory_space=pltpu.VMEM)] * n


def solution(mesh):
    seq_spec = P(None, 'cp', None)
    col_spec = P(None, None, 'tp')
    row_spec = P(None, 'tp', None)
    weight_specs = (P(), P(), col_spec, col_spec, col_spec, row_spec, col_spec, col_spec, row_spec)

    def local_program(x_in, d_y, key_mask, rel_bias, g_attn, g_mlp, w_q, w_k, w_v, w_o, w_gate, w_lin, w_out):
        width = x_in.shape[2]
        onehot = bucket_onehot(512)
        table = jnp.sum(jnp.where(onehot[None], rel_bias.T[:, :, None], 0.0), axis=1)
        wg_t, wl_t = jnp.swapaxes(w_gate, 1, 2), jnp.swapaxes(w_lin, 1, 2)
        x0, a0, x1, a1, dy, q, k, v, o, mask = forward(x_in, d_y, key_mask, g_attn, g_mlp, w_q, w_k, w_v, w_o, wg_t, wl_t, w_out, table)

        rest = (g_attn, g_mlp, wg_t, wl_t, w_out, w_q, w_k, w_v, w_o, table, mask)
        dx, small, out1, gate1, lin1, wo1, wq1, wk1, wv1 = layer_bwd(1, 4, a1, dy, x1, q, k, v, o, *rest)
        d_x, small, out0, gate0, lin0, wo0, wq0, wk0, wv0 = layer_bwd(0, 5, a0, dx, x0, q, k, v, o, *rest, small)

        def both(first, second, like, swap=False):
            shape = (like.shape[2], like.shape[1]) if swap else like.shape[1:]
            pair = jnp.stack([first.reshape(shape), second.reshape(shape)])
            return jnp.swapaxes(pair, 1, 2) if swap else pair

        d_bias = jnp.sum(jnp.where(onehot[None], small[8:12][:, None, :], 0.0), axis=2).T
        d_ga = jnp.stack([small[2], small[0]])
        d_gm = jnp.stack([small[3], small[1]])
        return (d_x.reshape(x_in.shape), d_bias, d_ga, d_gm, both(wq0, wq1, w_q), both(wk0, wk1, w_k), both(wv0, wv1, w_v),
                both(wo0, wo1, w_o), both(gate0, gate1, w_gate, True), both(lin0, lin1, w_lin, True), both(out0, out1, w_out))

    return jax.shard_map(local_program, mesh=mesh, in_specs=(seq_spec, seq_spec, P(None, 'cp'), P(None, 'tp')) + weight_specs, out_specs=(seq_spec, P(None, 'tp')) + weight_specs, check_vma=False)
```

```python
import functools
import jax
import jax.numpy as jnp
import numpy as np
from jax import lax
from jax.experimental import pallas as pl
from jax.experimental.pallas import tpu as pltpu
from jax.sharding import PartitionSpec as P

NORM_EPS = 1e-6
MASK_NEG = -1e9
HEAD = 64
F32 = jnp.float32
BF16 = jnp.bfloat16
NT = (((1,), (1,)), ((), ()))
TN = (((0,), (0,)), ((), ()))


def rel_bucket(rel_pos):
    distance = jnp.minimum(jnp.abs(rel_pos), 128)
    distance_sq = distance * distance
    log_part = 8 + sum((distance_sq >= 64 * 2 ** power).astype(jnp.int32) for power in range(1, 8))
    return jnp.where(distance < 8, distance, log_part) + 16 * (rel_pos > 0).astype(jnp.int32)


def bucket_onehot(seq):
    rel = jnp.arange(2 * seq) - seq
    return (rel_bucket(rel)[None, :] == jnp.arange(32)[:, None]) & (jnp.arange(2 * seq) > 0)[None, :]


def dot(a, b, dims=(((1,), (0,)), ((), ()))):
    return lax.dot_general(a, b, dims, preferred_element_type=F32)


def toeplitz(row, seq):
    base = pltpu.roll(row, seq, 1)
    rows = jnp.concatenate([base if i == 0 else pltpu.roll(base, i, 1) for i in range(8)], axis=0)
    size = 8
    while size < seq:
        rows = jnp.concatenate([rows, pltpu.roll(rows, size, 1)], axis=0)
        size *= 2
    return rows[:, :seq]


def diag_sums(mat, seq):
    wide = jnp.concatenate([mat, jnp.zeros_like(mat)], axis=1)
    size = seq
    while size > 1:
        half = size // 2
        wide = wide[:half] + pltpu.roll(wide[half:size], 2 * seq - half, 1)
        size = half
    return pltpu.roll(wide, seq, 1)


def place():
    tp, cp = lax.axis_index('tp'), lax.axis_index('cp')
    z, y = tp // 2, tp % 2
    x, core = cp // 2, cp % 2
    peers = {'z': (1 - z, y, x, core), 'y': (z, 1 - y, x, core), 'x': (z, y, 1 - x, core), 'core': (z, y, x, 1 - core),
             'zy': (1 - z, 1 - y, x, core), 'xc': (z, y, 1 - x, 1 - core)}
    ids = {name: {'tp': p[0] * 2 + p[1], 'cp': p[2] * 2 + p[3]} for name, p in peers.items()}
    return tp, cp, z, y, x, core, ids


def meet(ids, names):
    barrier = pltpu.get_barrier_semaphore()
    for name in names:
        pl.semaphore_signal(barrier, inc=1, device_id=ids[name], device_id_type=pl.DeviceIdType.MESH)
    pl.semaphore_wait(barrier, len(names))


def remote(src, dst, send, recv, target):
    copy = pltpu.make_async_remote_copy(src_ref=src, dst_ref=dst, send_sem=send, recv_sem=recv,
                                        device_id=target, device_id_type=pl.DeviceIdType.MESH)
    copy.start()
    return copy


class Stream:
    def __init__(self, part, near, far, out, send, recv, first, second, a, b, index, pieces=1):
        self.part, self.near, self.far, self.out = part, near, far, out
        self.send, self.recv = send, recv
        self.first, self.second = first, second
        self.own, self.pass_on = index(a, b), index(a, 1 - b)
        self.away_far, self.away = index(1 - a, 1 - b), index(1 - a, b)
        self.pieces = pieces
        self.copies = {}
        self.arrived = False

    def start(self, name, piece, src, dst, target):
        slot = name if name < 2 else 2 + (name - 2) * self.pieces + piece
        self.copies[name, piece] = remote(src, dst, self.send.at[slot], self.recv.at[slot], target)

    def rows(self, ref, piece):
        if self.pieces == 1:
            return ref
        size = ref.shape[0] // self.pieces
        return ref.at[pl.ds(piece * size, size)]

    def send_away(self, slot):
        quarter = self.away_far if slot == 0 else self.away
        self.start(slot, 0, self.part(quarter), self.near.at[slot], self.first)

    def forward(self):
        self.copies[0, 0].wait_recv()
        for piece in range(self.pieces):
            ref = self.rows(self.part(self.pass_on), piece)
            ref[...] += self.rows(self.near.at[0], piece)[...]
            self.start(2, piece, ref, self.rows(self.far, piece), self.second)

    def total(self, piece=0):
        if not self.arrived:
            self.copies[1, 0].wait_recv()
            self.arrived = True
        self.copies[2, piece].wait_recv()
        return self.rows(self.part(self.own), piece)[...] + self.rows(self.near.at[1], piece)[...] + self.rows(self.far, piece)[...]

    def publish(self, piece=0):
        out = self.out(self.own, piece)
        self.start(3, piece, out, out, self.first)
        self.start(4, piece, out, out, self.second)

    def gather(self):
        for piece in range(self.pieces):
            self.copies[4, piece].wait_recv()
            out = self.out(self.pass_on, piece)
            self.start(5, piece, out, out, self.first)

    def close(self):
        for piece in range(self.pieces):
            self.copies[3, piece].wait_recv()
            self.copies[5, piece].wait_recv()
        for copy in self.copies.values():
            copy.wait_send()


def colours(part, near, far, out, send, recv, ids, z, y, pieces=1):
    def make(c, first, second, a, b, index):
        return Stream(lambda q: part.at[q[0], q[1], c], None if near is None else near.at[c], None if far is None else far.at[c],
                      lambda q, piece: out(q, c, piece), send.at[c], recv.at[c], ids[first], ids[second], a, b, index, pieces)
    return [make(0, 'z', 'y', z, y, lambda a, b: (a, b)), make(1, 'y', 'z', y, z, lambda a, b: (b, a))]


class GradStream(Stream):
    def __init__(self, part, near, far, own_ref, out, send, recv, local, ids, x, core):
        super().__init__(lambda q: part.at[q], near, far, lambda q, piece: out.at[q], send, recv,
                         ids['core'], ids['x'], core, x, lambda a, b: b * 2 + a)
        self.own_ref, self.local = own_ref, local

    def send_both(self):
        self.send_away(0)
        self.send_away(1)

    def finish(self):
        self.own_ref[...] = self.total().astype(BF16)
        out = self.out(self.own, 0)
        self.start(4, 0, self.own_ref, out, self.second)
        self.start(3, 0, self.own_ref, out, self.first)
        self.kept = pltpu.make_async_copy(self.own_ref, out, self.local)
        self.kept.start()

    def close(self):
        super().close()
        self.kept.wait()


def grad_into(part, a, b):
    quarter, width = part.shape[1], part.shape[2]
    for lo in range(0, width, 256):
        block = dot(a, b[:, lo:lo + 256], TN)
        for q in range(4):
            part[q, :, lo:lo + 256] = block[q * quarter:(q + 1) * quarter]


def norm_parts(rows):
    xf = rows.astype(F32)
    inv = lax.rsqrt(jnp.mean(xf * xf, axis=-1, keepdims=True) + NORM_EPS)
    return inv, xf * inv


def norm(rows, gain):
    return (norm_parts(rows)[1] * gain).astype(BF16)


def norm_back(d_norm, rows, gain):
    inv, normed = norm_parts(rows)
    d_normed = d_norm * gain
    return inv * (d_normed - normed * jnp.mean(d_normed * normed, axis=-1, keepdims=True)), d_norm * normed


def key_add(mask_ref, b):
    row = jnp.concatenate([mask_ref[j, pl.ds(b, 1), :] for j in range(4)], axis=1)
    return jnp.where(row > 0, 0.0, MASK_NEG).astype(F32)


def exp_scores(q, k, bias, add):
    s = dot(q, k, NT) + bias + add
    e = jnp.exp(s - jnp.max(s, axis=-1, keepdims=True))
    return e, jnp.sum(e, axis=-1, keepdims=True)


def any_specs(n):
    return [pl.BlockSpec(memory_space=pl.ANY)] * n


def gelu_parts(g):
    inner = np.float32(np.sqrt(2 / np.pi)) * (g + 0.044715 * (g * g * g))
    t = jnp.tanh(inner)
    cdf = 0.5 * (1.0 + t)
    slope = cdf + 0.5 * g * (1.0 - t * t) * np.float32(np.sqrt(2 / np.pi)) * (1.0 + 3 * 0.044715 * (g * g))
    return g * cdf, slope


def order(z, y):
    return [(1 - z, 1 - y), (1 - z, y), (z, 1 - y), (z, y)]


def sum_scratch(width, blocks=()):
    return [pltpu.VMEM((2, 2, 2) + blocks, F32), pltpu.VMEM((2, 2) + blocks, F32), pltpu.VMEM((2,) + blocks, F32)]


def forward_kernel(seq, *refs):
    refs = list(refs)
    take = lambda n: [refs.pop(0) for _ in range(n)]
    x_in, d_y, wo_in, wq_in, wk_in, wv_in, wg_in, wl_in, wd_in, mask_in, ga_ref, gm_ref, t_ref = take(13)
    x0_out, a0_out, x1_out, a1_out, dy_out, q_out, k_out, v_out, o_out, mask_ref = take(10)
    x0_ref, a0_ref, x1_ref, a1_ref, dyo_ref, q_ref, k_ref, v_ref, o_ref = take(9)
    wq_ref, wk_ref, wv_ref, wg_ref, wl_ref, wd_ref, wf_ref = take(7)
    bias_ref, of_ref, part, near, far = take(5)
    xsend, xrecv, osend, orecv, send, recv, lsem, ssem = refs
    tp, cp, z, y, x, core, ids = place()
    near_by, far_by = ['core', 'x', 'xc'], ['z', 'y', 'zy']

    def local(src, dst, sem):
        copy = pltpu.make_async_copy(src, dst, sem)
        copy.start()
        return copy

    own_x = local(x_in.at[cp], x0_ref.at[:, cp], lsem.at[0])
    qkv_loads = [local(w, r, lsem.at[1 + i]) for i, (w, r) in enumerate([(wq_in, wq_ref), (wk_in, wk_ref), (wv_in, wv_ref)])]
    own_w = [local(wo_in.at[layer], wf_ref.at[layer, tp], lsem.at[4 + layer]) for layer in range(2)]
    mlp_loads = [local(w.at[0], r, lsem.at[6 + i]) for i, (w, r) in enumerate([(wg_in, wg_ref), (wl_in, wl_ref), (wd_in, wd_ref)])]
    own_dy = local(d_y.at[cp], dyo_ref, lsem.at[9])
    meet(ids, near_by + far_by)
    masks, xs = [], []
    for i, name in enumerate(near_by):
        masks.append(remote(mask_in.at[ids[name]['cp']], mask_ref.at[cp], xsend.at[i], xrecv.at[i], ids[name]))
        xs.append(remote(x_in.at[ids[name]['cp']], x0_ref.at[:, cp], xsend.at[3 + i], xrecv.at[3 + i], ids[name]))
    weights = [remote(wo_in.at[core], wf_ref.at[core, tp], xsend.at[6 + i], xrecv.at[6 + i], ids[name]) for i, name in enumerate(far_by)]
    mask_ref[cp] = mask_in[cp]
    for head in range(t_ref.shape[0]):
        bias_ref[head] = toeplitz(t_ref[head:head + 1, :], seq)

    def project(layer, rows):
        h = norm(rows, ga_ref[layer:layer + 1, :])
        return [dot(h, w[layer]).astype(BF16) for w in (wq_ref, wk_ref, wv_ref)]

    def attention(layer, b):
        add = key_add(mask_ref, b)
        for head in range(t_ref.shape[0]):
            cols = pl.ds(head * HEAD, HEAD)
            e, total = exp_scores(q_ref[layer, b, :, cols], k_ref[layer, b, :, cols], bias_ref[head], add)
            o = (dot(e.astype(BF16), v_ref[layer, b, :, cols]) / total).astype(BF16)
            o_ref[layer, b, 0, :, cols] = o[:seq // 2]
            o_ref[layer, b, 1, :, cols] = o[seq // 2:]

    def ship(layer, name, b, half):
        i = layer * 3 + far_by.index(name)
        return remote(o_ref.at[layer, b, half], of_ref.at[layer, tp], osend.at[i], orecv.at[i], ids[name])

    def project_out(layer, sent, residual, out_ref):
        of_ref[layer, tp] = o_ref[layer, z, y]
        for copy in sent:
            copy.wait_recv()
        streams = colours(None, None, None, lambda q, c, piece: out_ref.at[q[0], q[1], c], send.at[4 * layer:4 * layer + 2], recv.at[4 * layer:4 * layer + 2], ids, z, y)
        for c, s in enumerate(streams):
            rows = pl.ds(c * 128, 128)
            total = sum(dot(of_ref[layer, j, rows, :], wf_ref[layer, j]) for j in range(4))
            out_ref[z, y, c] = (residual(c).astype(F32) + total).astype(BF16)
            s.publish()
        for s in streams:
            s.gather()
        for s in streams:
            s.close()

    for copy in qkv_loads:
        copy.wait()
    for i, name in enumerate(['own'] + near_by):
        if i == 0:
            own_x.wait()
            blk = cp
        else:
            xs[i - 1].wait_recv()
            blk = ids[name]['cp']
        for d_ref, value in zip((q_ref, k_ref, v_ref), project(0, x0_ref[:, blk].reshape(2 * 128, -1))):
            for b in range(2):
                d_ref[0, b, pl.ds(pl.multiple_of(blk * 128, 128), 128), :] = value[b * 128:(b + 1) * 128]
    own_dy.wait()
    saves = [local(x0_ref, x0_out, ssem.at[0]), local(dyo_ref, dy_out.at[:, cp], ssem.at[1])]
    moves = [remote(d_y.at[ids[name]['cp']], dy_out.at[:, cp], xsend.at[12 + i], xrecv.at[12 + i], ids[name]) for i, name in enumerate(near_by)]
    for copy in masks:
        copy.wait_recv()
    attention(0, 1 - z)
    sent = [ship(0, 'zy', 1 - z, 1 - y), ship(0, 'z', 1 - z, y)]
    passed = []
    for i, name in enumerate(far_by):
        weights[i].wait_recv()
        got = wf_ref.at[core, ids[name]['tp']]
        passed.append(remote(got, got, xsend.at[9 + i], xrecv.at[9 + i], ids['core']))
    attention(0, z)
    sent.append(ship(0, 'y', z, 1 - y))
    for copy in own_w:
        copy.wait()
    for copy in passed:
        copy.wait_recv()
    project_out(0, sent, lambda c: x0_ref[z, y * 2 + c], a0_ref)
    saves.append(local(a0_ref, a0_out, ssem.at[2]))

    for copy in mlp_loads:
        copy.wait()
    zy, yz = streams = colours(part, near, far, lambda q, c, piece: x1_ref.at[q[0], q[1], c, pl.ds(piece * 64, 64)], send.at[2:4], recv.at[2:4], ids, z, y, 2)

    def mlp_quarter(q):
        h2 = norm(a0_ref[q].reshape(256, -1), gm_ref[0:1, :])
        gated = (gelu_parts(dot(h2, wg_ref[...], NT))[0] * dot(h2, wl_ref[...], NT)).astype(BF16)
        part[q] = dot(gated, wd_ref[...]).reshape(part.shape[2:])

    quarters = order(z, y)
    mlp_quarter(quarters[0])
    zy.send_away(0)
    yz.send_away(0)
    mlp_quarter(quarters[1])
    zy.send_away(1)
    mlp_quarter(quarters[2])
    yz.send_away(1)
    mlp_quarter(quarters[3])
    for s in streams:
        s.forward()
    for piece in range(2):
        rows = pl.ds(piece * 64, 64)
        for c, s in enumerate(streams):
            x1_ref[z, y, c, rows, :] = (a0_ref[z, y, c, rows, :].astype(F32) + s.total(piece)).astype(BF16)
            s.publish(piece)
    for s in streams:
        s.gather()
    for s in streams:
        s.close()
    saves.append(local(x1_ref, x1_out, ssem.at[3]))

    late = []
    for step in range(2):
        b = 1 - z if step == 0 else z
        for half in range(2):
            rows = pl.ds(half * 256, 256)
            for d_ref, value in zip((q_ref, k_ref, v_ref), project(1, x1_ref[b, half].reshape(256, -1))):
                d_ref[1, b, rows, :] = value
        attention(1, b)
        if step == 0:
            late += [ship(1, 'zy', b, 1 - y), ship(1, 'z', b, y)]
        else:
            late.append(ship(1, 'y', b, 1 - y))
    saves += [local(src, dst, ssem.at[4 + i]) for i, (src, dst) in enumerate([(q_ref, q_out), (k_ref, k_out), (v_ref, v_out), (o_ref, o_out)])]
    project_out(1, late, lambda c: x1_ref[z, y, c], a1_ref)
    saves.append(local(a1_ref, a1_out, ssem.at[8]))
    for copy in masks + xs + weights + passed + sent + late:
        copy.wait_send()
    for copy in moves + saves:
        copy.wait()


def forward(x_in, d_y, key_mask, gains_a, gains_m, w_q, w_k, w_v, w_o, wg_t, wl_t, w_out, table):
    batch, blk, width = x_in.shape
    seq, cols = 4 * blk, w_q.shape[2]
    dma = pltpu.SemaphoreType.DMA
    blocks = (2, 2, 2, blk, width)
    arrived = (2, 4, blk, width)
    heads = (2, 2, seq, cols)
    halves = (2, 2, 2, seq // 2, cols)
    hbm = [arrived, blocks, blocks, blocks, arrived, heads, heads, heads, halves]
    operands = [x_in.reshape(4, 2, blk, width), d_y.reshape(4, 2, blk, width), w_o, w_q, w_k, w_v, wg_t, wl_t, w_out,
                key_mask.reshape(4, 2, blk), gains_a, gains_m, table]
    scratch = [pltpu.VMEM(h, BF16) for h in hbm[:4] + [(2, blk, width)] + hbm[5:]]
    scratch += [pltpu.VMEM(w.shape, BF16) for w in (w_q, w_k, w_v)] + [pltpu.VMEM(w.shape[1:], BF16) for w in (wg_t, wl_t, w_out)]
    scratch += [pltpu.VMEM((2, 4) + w_o.shape[1:], BF16), pltpu.VMEM((table.shape[0], seq, seq), F32), pltpu.VMEM((2, 4, 2 * blk, cols), BF16)]
    scratch += sum_scratch(0, blocks[3:])
    scratch += [dma((15,)), dma((15,)), dma((6,)), dma((6,)), dma((6, 10)), dma((6, 10)), dma((10,)), dma((9,))]
    return pl.pallas_call(
        functools.partial(forward_kernel, seq),
        out_shape=[jax.ShapeDtypeStruct(h, BF16) for h in hbm] + [jax.ShapeDtypeStruct((4, 2, blk), jnp.int32)],
        in_specs=any_specs(9) + vmem_specs(4), out_specs=any_specs(9) + vmem_specs(1),
        scratch_shapes=scratch,
        compiler_params=pltpu.CompilerParams(collective_id=0, has_side_effects=True, vmem_limit_bytes=62 << 20),
        cost_estimate=pl.CostEstimate(flops=15 << 30, bytes_accessed=48 << 20, transcendentals=0),
        name="forward",
    )(*operands)


def backward_kernel(seq, *refs):
    refs = list(refs)
    take = lambda n: [refs.pop(0) for _ in range(n)]
    stacks = take(7)
    x1_all, dy_in, x_all, heads_all = take(2), refs.pop(0), take(2), take(4)
    ga_ref, gm_ref, t_ref, mask_ref = take(4)
    dx_ref, small_out = take(2)
    grad_out = {1: take(7), 0: take(7)}
    weights, holds = take(7), take(7)
    lsem, part, near, far, dm_ref, h_ref, gated_ref, dgate_ref, dlin_ref = take(9)
    bias_ref, do_ref, dq_ref, dk_ref, dv_ref, dt_ref = take(6)
    grad_scratch = [take(4) for _ in range(7)]
    send, recv, gsend, grecv, kept, own_ref, acc_small, got_small, msend, mrecv, csend, crecv = refs
    wg_ref, wl_ref, wd_ref, wq_ref, wk_ref, wv_ref, wo_ref = weights
    x1_ref, dy_ref, x_ref, q_ref, k_ref, v_ref, o_ref = holds
    tp, cp, z, y, x, core, ids = place()
    heads = t_ref.shape[0]
    width = x_ref.shape[-1]
    quarters = order(z, y)
    p_out, p_gate, p_lin, p_o, p_q, p_k, p_v = [g[0] for g in grad_scratch]

    def fetch(layer, attention):
        if attention:
            pairs = [(x_all[layer], x_ref)] + [(h.at[layer], r) for h, r in zip(heads_all, (q_ref, k_ref, v_ref, o_ref))]
            pairs += [(w.at[layer], r) for w, r in zip(stacks[3:], weights[3:])]
        else:
            pairs = [(x1_all[layer], x1_ref)] + ([(dy_in, dy_ref)] if layer == 1 else []) + [(w.at[layer], r) for w, r in zip(stacks[:3], weights[:3])]
        copies = [pltpu.make_async_copy(src, dst, lsem.at[int(attention), layer, i]) for i, (src, dst) in enumerate(pairs)]
        for copy in copies:
            copy.start()
        return copies

    def mlp_quarter(q, gain):
        h2 = norm(x1_ref[q].reshape(256, -1), gain)
        rows = pl.ds(pl.multiple_of((q[0] * 2 + q[1]) * 256, 256), 256)
        h_ref[rows, :] = h2
        value, slope = gelu_parts(dot(h2, wg_ref[...], NT))
        lin = dot(h2, wl_ref[...], NT)
        gated_ref[rows, :] = (value * lin).astype(BF16)
        d_gated = dot(dy_ref[q].reshape(256, -1), wd_ref[...], NT)
        d_lin = (d_gated * value).astype(BF16)
        d_gate = (d_gated * lin * slope).astype(BF16)
        dlin_ref[rows, :] = d_lin
        dgate_ref[rows, :] = d_gate
        part[q] = (dot(d_gate, wg_ref[...]) + dot(d_lin, wl_ref[...])).reshape(part.shape[2:])

    def attend(b, first, hook):
        add = key_add(mask_ref, b)
        do_ref[...] = dot(dm_ref[b].reshape(seq, width), wo_ref[...], NT).astype(BF16)
        for head in range(heads):
            bias_ref[...] = toeplitz(t_ref[head:head + 1, :], seq)
            cols = pl.ds(head * HEAD, HEAD)
            q, k, v, do = q_ref[b, :, cols], k_ref[b, :, cols], v_ref[b, :, cols], do_ref[:, cols]
            e, total = exp_scores(q, k, bias_ref[...], add)
            p = e * (1.0 / total)
            row_dot = jnp.sum(do.astype(F32) * o_ref[b, :, cols].astype(F32), axis=-1, keepdims=True)
            ds = p * (dot(do, v, NT) - row_dot)
            sums = diag_sums(ds, seq)
            dt_ref[head:head + 1, :] = sums if first else dt_ref[head:head + 1, :] + sums
            dsl = ds.astype(BF16)
            dq_ref[b, :, cols] = dot(dsl, k).astype(BF16)
            dk_ref[b, :, cols] = dot(dsl, q, TN).astype(BF16)
            dv_ref[b, :, cols] = dot(p.astype(BF16), do, TN).astype(BF16)
            if head == 0:
                hook()

    loads = {(1, False): fetch(1, False), (1, True): fetch(1, True)}
    meet(ids, ['z', 'y', 'x', 'core', 'xc'])
    pending = []
    for layer in (1, 0):
        last = layer == 0
        deep = 32 if last else 128
        across = 128 // deep
        half = deep // 2
        g_out, g_gate, g_lin, g_o, g_q, g_k, g_v = grads = [
            GradStream(*grad_scratch[i], grad_out[layer][i], gsend.at[layer, i], grecv.at[layer, i], kept.at[layer, i], ids, x, core) for i in range(7)]
        zy, yz = mlp_sum = colours(part, near, far, lambda q, c, piece: dm_ref.at[q[0], q[1], c, pl.ds(piece * 64, 64)],
                                   send.at[layer, 0:2], recv.at[layer, 0:2], ids, z, y, 2)
        for copy in loads[layer, False]:
            copy.wait()
        gain, gain_a = gm_ref[layer:layer + 1, :], ga_ref[layer:layer + 1, :]
        mlp_quarter(quarters[0], gain)
        zy.send_away(0)
        yz.send_away(0)
        mlp_quarter(quarters[1], gain)
        zy.send_away(1)
        mlp_quarter(quarters[2], gain)
        yz.send_away(1)
        mlp_quarter(quarters[3], gain)
        grad_into(p_out, gated_ref[...], dy_ref[...].reshape(h_ref.shape))
        g_out.send_both()
        grad_into(p_gate, dgate_ref[...], h_ref)
        g_gate.send_both()
        g_out.forward()
        for s in mlp_sum:
            s.forward()
        for g in pending:
            g.gather()
        grad_into(p_lin, dlin_ref[...], h_ref)
        g_lin.send_both()
        g_gate.forward()
        for copy in loads[layer, True]:
            copy.wait()
        for b in range(2):
            h_ref[b * seq:(b + 1) * seq, :] = norm(x_ref[b], gain_a)
        g_lin.forward()
        for g in pending:
            g.close()
        g_out.finish()
        dg_m = 0.0
        for piece in range(2):
            rows = pl.ds(piece * 64, 64)
            for c, s in enumerate(mlp_sum):
                d_x, dg = norm_back(s.total(piece), x1_ref[z, y, c, rows, :], gain)
                dm_ref[z, y, c, rows, :] = (d_x + dy_ref[z, y, c, rows, :].astype(F32)).astype(BF16)
                s.publish(piece)
                dg_m = dg_m + jnp.sum(dg, axis=0, keepdims=True)
        g_gate.finish()
        for s in mlp_sum:
            s.gather()
        for s in mlp_sum:
            s.close()
        if not last:
            loads[0, False] = fetch(0, False)

        if last:
            def region(q, c, piece):
                return dx_ref.at[:, q[0], q[1], c, pl.ds(piece * 16, 16)]
        else:
            def region(q, c, piece):
                return dy_ref.at[q[0], q[1], c, pl.ds(piece * 64, 64)]
        zy, yz = attn_sum = colours(part, near, far, region, send.at[layer, 2:4], recv.at[layer, 2:4], ids, z, y, 2)

        def pick(ref, offset, size, q):
            pieces = [ref[q[0], pl.ds(pl.multiple_of(j * 4 * deep + q[1] * 2 * deep + offset, half), size), :] for j in range(across)]
            return pieces[0] if across == 1 else jnp.concatenate(pieces, axis=0)

        def attn_quarter(q):
            total = sum(dot(pick(d, 0, 2 * deep, q), w[...], NT) for d, w in [(dq_ref, wq_ref), (dk_ref, wk_ref), (dv_ref, wv_ref)])
            total = total.reshape(across, 2, 2, half, width)
            for c in range(2):
                for piece in range(2):
                    part[q[0], q[1], c, pl.ds(piece * 64, 64), :] = total[:, c, piece].reshape(64, width)

        attend(1 - z, not last, lambda: None)
        attn_quarter(quarters[0])
        zy.send_away(0)
        yz.send_away(0)
        attn_quarter(quarters[1])
        zy.send_away(1)
        grad_into(p_o, o_ref[...].reshape(2 * seq, -1), dm_ref[...].reshape(2 * seq, width))
        g_o.send_both()
        g_lin.finish()
        g_out.gather()
        attend(z, False, g_o.forward)
        attn_quarter(quarters[2])
        yz.send_away(1)
        attn_quarter(quarters[3])
        for g, p, d in [(g_q, p_q, dq_ref), (g_k, p_k, dk_ref), (g_v, p_v, dv_ref)]:
            grad_into(p, h_ref[...], d[...].reshape(2 * seq, -1))
            g.send_both()
        for s in attn_sum:
            s.forward()
        for g in [g_q, g_k, g_v]:
            g.forward()
        g_gate.gather()
        g_lin.gather()
        g_o.finish()
        dg_a = 0.0
        moves = {}
        for piece in range(2):
            for c, s in enumerate(attn_sum):
                rows = pl.ds(piece * half, half)
                d_x, dg = norm_back(s.total(piece), pick(x_ref, c * deep + piece * half, half, (z, y)), gain_a)
                dg_a = dg_a + jnp.sum(dg, axis=0, keepdims=True)
                if last:
                    at = pl.ds(pl.multiple_of(y * 2 * deep + c * deep + piece * half, half), half)
                    res = jnp.concatenate([dm_ref[z, j // 2, j % 2, at, :] for j in range(4)], axis=0)
                else:
                    res = dm_ref[z, y, c, rows, :]
                d_x = (d_x + res.astype(F32)).astype(BF16)
                if last:
                    own_ref[c, piece] = d_x.reshape(across, half, width)
                    dx_ref[cp, z, y, c, rows, :] = own_ref[c, piece, cp]
                    moves[c, piece] = [remote(own_ref.at[c, piece, ids[name]['cp']], dx_ref.at[cp, z, y, c, rows], msend.at[c, piece, i], mrecv.at[c, piece, i], ids[name])
                                       for i, name in enumerate(['x', 'xc', 'core'])]
                else:
                    dy_ref[z, y, c, rows, :] = d_x
                    s.publish(piece)
        acc_small[0, 2 - 2 * layer:3 - 2 * layer, :] = dg_a
        acc_small[0, 3 - 2 * layer:4 - 2 * layer, :] = dg_m
        if not last:
            loads[0, True] = fetch(0, True)
            for g in [g_q, g_k, g_v]:
                g.finish()
            for s in attn_sum:
                s.gather()
            for s in attn_sum + [g_out, g_gate, g_lin]:
                s.close()
            pending = [g_o, g_q, g_k, g_v]

    acc_small[0, 4:8, :] = jnp.zeros((4, width), F32)
    acc_small[0, 8:12, :] = dt_ref[0:4, :]
    acc_small[0, 12:16, :] = jnp.zeros((4, width), F32)
    smalls = []

    def small_start(i):
        rows = pl.ds(0, 16 if i < 2 else 8)
        smalls.append(remote(acc_small.at[i, rows], got_small.at[i, rows], csend.at[i], crecv.at[i], ids[['x', 'core', 'y', 'z'][i]]))

    def small_end(i):
        rows = pl.ds(0, 16 if i < 2 else 8)
        smalls[i].wait_recv()
        acc_small[i + 1, rows, :] = acc_small[i, rows, :] + got_small[i, rows, :]

    small_start(0)
    for piece in range(2):
        for c, s in enumerate(attn_sum):
            for copy in moves[c, piece]:
                copy.wait_recv()
            s.publish(piece)
    g_q.finish()
    small_end(0)
    small_start(1)
    g_k.finish()
    small_end(1)
    small_start(2)
    g_v.finish()
    for s in attn_sum:
        s.gather()
    small_end(2)
    small_start(3)
    for g in [g_o, g_q, g_k, g_v]:
        g.gather()
    small_end(3)
    small_out[0:8, :] = acc_small[4, 0:8, :]
    small_out[8:16, :] = acc_small[2, 8:16, :]
    for copy in smalls + sum(moves.values(), []):
        copy.wait_send()
    for s in attn_sum + grads:
        s.close()


def backward(x1s, dy, xs, heads, gains_a, gains_m, wg_t, wl_t, w_out, w_q, w_k, w_v, w_o, table, mask):
    seq, width, cols = 512, w_q.shape[1], w_q.shape[2]
    ff = w_out.shape[1]
    rows = 2 * seq
    dma = pltpu.SemaphoreType.DMA
    blocks = (2, 2, 2, 128, width)
    flat = (2, seq, width)
    stacks = [wg_t, wl_t, w_out, w_q, w_k, w_v, w_o]
    operands = stacks + [a.reshape(blocks) for a in x1s] + [dy.reshape(blocks)] + [a.reshape(flat) for a in xs]
    operands += [h.reshape(2, 2, seq, cols) for h in heads] + [gains_a, gains_m, table, mask]
    grads = [(ff // 4, width)] * 3 + [(cols // 4, width)] + [(width // 4, cols)] * 3
    out_shape = [jax.ShapeDtypeStruct((4, 2, 2, 2, 32, width), BF16), jax.ShapeDtypeStruct((16, width), F32)]
    out_shape += [jax.ShapeDtypeStruct((4,) + g, BF16) for g in grads] * 2
    scratch = [pltpu.VMEM(w.shape[1:], BF16) for w in stacks]
    scratch += [pltpu.VMEM(blocks, BF16)] * 2 + [pltpu.VMEM(flat, BF16)] + [pltpu.VMEM((2, seq, cols), BF16)] * 4 + [dma((2, 2, 9))]
    scratch += sum_scratch(0, blocks[3:]) + [pltpu.VMEM(blocks, BF16), pltpu.VMEM((rows, width), BF16)] + [pltpu.VMEM((rows, ff), BF16)] * 3
    scratch += [pltpu.VMEM((seq, seq), F32), pltpu.VMEM((seq, cols), BF16)] + [pltpu.VMEM((2, seq, cols), BF16)] * 3 + [pltpu.VMEM((8, 2 * seq), F32)]
    for g in grads:
        scratch += [pltpu.VMEM((4,) + g, F32), pltpu.VMEM((2,) + g, F32), pltpu.VMEM(g, F32), pltpu.VMEM(g, BF16)]
    scratch += [dma((2, 4, 10)), dma((2, 4, 10)), dma((2, 7, 6)), dma((2, 7, 6)), dma((2, 7))]
    scratch += [pltpu.VMEM((2, 2, 4, 16, width), BF16), pltpu.VMEM((5, 16, width), F32), pltpu.VMEM((4, 16, width), F32)]
    scratch += [dma((2, 2, 3)), dma((2, 2, 3)), dma((4,)), dma((4,))]
    return pl.pallas_call(
        functools.partial(backward_kernel, seq),
        out_shape=out_shape, in_specs=any_specs(16) + vmem_specs(4), out_specs=vmem_specs(2) + any_specs(14),
        scratch_shapes=scratch,
        compiler_params=pltpu.CompilerParams(collective_id=1, has_side_effects=True, vmem_limit_bytes=67043328),
        cost_estimate=pl.CostEstimate(flops=40 << 30, bytes_accessed=96 << 20, transcendentals=0),
        name="backward",
    )(*operands)


def vmem_specs(n):
    return [pl.BlockSpec(memory_space=pltpu.VMEM)] * n


def solution(mesh):
    seq_spec = P(None, 'cp', None)
    col_spec = P(None, None, 'tp')
    row_spec = P(None, 'tp', None)
    weight_specs = (P(), P(), col_spec, col_spec, col_spec, row_spec, col_spec, col_spec, row_spec)

    def local_program(x_in, d_y, key_mask, rel_bias, g_attn, g_mlp, w_q, w_k, w_v, w_o, w_gate, w_lin, w_out):
        width = x_in.shape[2]
        onehot = bucket_onehot(512)
        table = jnp.sum(jnp.where(onehot[None], rel_bias.T[:, :, None], 0.0), axis=1)
        wg_t, wl_t = jnp.swapaxes(w_gate, 1, 2), jnp.swapaxes(w_lin, 1, 2)
        x0, a0, x1, a1, dy, q, k, v, o, mask = forward(x_in, d_y, key_mask, g_attn, g_mlp, w_q, w_k, w_v, w_o, wg_t, wl_t, w_out, table)

        outs = backward((a0, a1), dy, (x0, x1), (q, k, v, o), g_attn, g_mlp, wg_t, wl_t, w_out, w_q, w_k, w_v, w_o, table, mask)
        d_x, small = outs[:2]
        out1, gate1, lin1, wo1, wq1, wk1, wv1, out0, gate0, lin0, wo0, wq0, wk0, wv0 = outs[2:]

        def both(first, second, like, swap=False):
            shape = (like.shape[2], like.shape[1]) if swap else like.shape[1:]
            pair = jnp.stack([first.reshape(shape), second.reshape(shape)])
            return jnp.swapaxes(pair, 1, 2) if swap else pair

        d_bias = jnp.sum(jnp.where(onehot[None], small[8:12][:, None, :], 0.0), axis=2).T
        d_ga = jnp.stack([small[2], small[0]])
        d_gm = jnp.stack([small[3], small[1]])
        return (d_x.reshape(x_in.shape), d_bias, d_ga, d_gm, both(wq0, wq1, w_q), both(wk0, wk1, w_k), both(wv0, wv1, w_v),
                both(wo0, wo1, w_o), both(gate0, gate1, w_gate, True), both(lin0, lin1, w_lin, True), both(out0, out1, w_out))

    return jax.shard_map(local_program, mesh=mesh, in_specs=(seq_spec, seq_spec, P(None, 'cp'), P(None, 'tp')) + weight_specs, out_specs=(seq_spec, P(None, 'tp')) + weight_specs, check_vma=False)
```

```python
import functools
import jax
import jax.numpy as jnp
import numpy as np
from jax import lax
from jax.experimental import pallas as pl
from jax.experimental.pallas import tpu as pltpu
from jax.sharding import PartitionSpec as P

NORM_EPS = 1e-6
MASK_NEG = -1e9
HEAD = 64
F32 = jnp.float32
BF16 = jnp.bfloat16
NT = (((1,), (1,)), ((), ()))
TN = (((0,), (0,)), ((), ()))


def rel_bucket(rel_pos):
    distance = jnp.minimum(jnp.abs(rel_pos), 128)
    distance_sq = distance * distance
    log_part = 8 + sum((distance_sq >= 64 * 2 ** power).astype(jnp.int32) for power in range(1, 8))
    return jnp.where(distance < 8, distance, log_part) + 16 * (rel_pos > 0).astype(jnp.int32)


def bucket_onehot(seq):
    rel = jnp.arange(2 * seq) - seq
    return (rel_bucket(rel)[None, :] == jnp.arange(32)[:, None]) & (jnp.arange(2 * seq) > 0)[None, :]


def dot(a, b, dims=(((1,), (0,)), ((), ()))):
    return lax.dot_general(a, b, dims, preferred_element_type=F32)


def toeplitz(row, seq):
    base = pltpu.roll(row, seq, 1)
    rows = jnp.concatenate([base if i == 0 else pltpu.roll(base, i, 1) for i in range(8)], axis=0)
    size = 8
    while size < seq:
        rows = jnp.concatenate([rows, pltpu.roll(rows, size, 1)], axis=0)
        size *= 2
    return rows[:, :seq]


def diag_sums(mat, seq):
    wide = jnp.concatenate([mat, jnp.zeros_like(mat)], axis=1)
    size = seq
    while size > 1:
        half = size // 2
        wide = wide[:half] + pltpu.roll(wide[half:size], 2 * seq - half, 1)
        size = half
    return pltpu.roll(wide, seq, 1)


def place():
    tp, cp = lax.axis_index('tp'), lax.axis_index('cp')
    z, y = tp // 2, tp % 2
    x, core = cp // 2, cp % 2
    peers = {'z': (1 - z, y, x, core), 'y': (z, 1 - y, x, core), 'x': (z, y, 1 - x, core), 'core': (z, y, x, 1 - core),
             'zy': (1 - z, 1 - y, x, core), 'xc': (z, y, 1 - x, 1 - core)}
    ids = {name: {'tp': p[0] * 2 + p[1], 'cp': p[2] * 2 + p[3]} for name, p in peers.items()}
    return tp, cp, z, y, x, core, ids


def meet(ids, names):
    barrier = pltpu.get_barrier_semaphore()
    for name in names:
        pl.semaphore_signal(barrier, inc=1, device_id=ids[name], device_id_type=pl.DeviceIdType.MESH)
    pl.semaphore_wait(barrier, len(names))


def remote(src, dst, send, recv, target):
    copy = pltpu.make_async_remote_copy(src_ref=src, dst_ref=dst, send_sem=send, recv_sem=recv,
                                        device_id=target, device_id_type=pl.DeviceIdType.MESH)
    copy.start()
    return copy


class Stream:
    def __init__(self, part, near, far, out, send, recv, first, second, a, b, index, pieces=1):
        self.part, self.near, self.far, self.out = part, near, far, out
        self.send, self.recv = send, recv
        self.first, self.second = first, second
        self.own, self.pass_on = index(a, b), index(a, 1 - b)
        self.away_far, self.away = index(1 - a, 1 - b), index(1 - a, b)
        self.pieces = pieces
        self.copies = {}
        self.arrived = False

    def start(self, name, piece, src, dst, target):
        slot = name if name < 2 else 2 + (name - 2) * self.pieces + piece
        self.copies[name, piece] = remote(src, dst, self.send.at[slot], self.recv.at[slot], target)

    def rows(self, ref, piece):
        if self.pieces == 1:
            return ref
        size = ref.shape[0] // self.pieces
        return ref.at[pl.ds(piece * size, size)]

    def send_away(self, slot):
        quarter = self.away_far if slot == 0 else self.away
        self.start(slot, 0, self.part(quarter), self.near.at[slot], self.first)

    def forward(self):
        self.copies[0, 0].wait_recv()
        for piece in range(self.pieces):
            ref = self.rows(self.part(self.pass_on), piece)
            ref[...] += self.rows(self.near.at[0], piece)[...]
            self.start(2, piece, ref, self.rows(self.far, piece), self.second)

    def total(self, piece=0):
        if not self.arrived:
            self.copies[1, 0].wait_recv()
            self.arrived = True
        self.copies[2, piece].wait_recv()
        return self.rows(self.part(self.own), piece)[...] + self.rows(self.near.at[1], piece)[...] + self.rows(self.far, piece)[...]

    def publish(self, piece=0):
        out = self.out(self.own, piece)
        self.start(3, piece, out, out, self.first)
        self.start(4, piece, out, out, self.second)

    def gather(self):
        for piece in range(self.pieces):
            self.copies[4, piece].wait_recv()
            out = self.out(self.pass_on, piece)
            self.start(5, piece, out, out, self.first)

    def close(self):
        for piece in range(self.pieces):
            self.copies[3, piece].wait_recv()
            self.copies[5, piece].wait_recv()
        for copy in self.copies.values():
            copy.wait_send()


def colours(part, near, far, out, send, recv, ids, z, y, pieces=1):
    def make(c, first, second, a, b, index):
        return Stream(lambda q: part.at[q[0], q[1], c], None if near is None else near.at[c], None if far is None else far.at[c],
                      lambda q, piece: out(q, c, piece), send.at[c], recv.at[c], ids[first], ids[second], a, b, index, pieces)
    return [make(0, 'z', 'y', z, y, lambda a, b: (a, b)), make(1, 'y', 'z', y, z, lambda a, b: (b, a))]


class GradStream(Stream):
    def __init__(self, part, near, far, own_ref, out, send, recv, local, ids, x, core):
        super().__init__(lambda q: part.at[q], near, far, lambda q, piece: out.at[q], send, recv,
                         ids['core'], ids['x'], core, x, lambda a, b: b * 2 + a)
        self.own_ref, self.local = own_ref, local

    def send_both(self):
        self.send_away(0)
        self.send_away(1)

    def finish(self):
        self.own_ref[...] = self.total().astype(BF16)
        out = self.out(self.own, 0)
        self.start(4, 0, self.own_ref, out, self.second)
        self.start(3, 0, self.own_ref, out, self.first)
        self.kept = pltpu.make_async_copy(self.own_ref, out, self.local)
        self.kept.start()

    def close(self):
        super().close()
        self.kept.wait()


def grad_into(part, a, b):
    quarter, width = part.shape[1], part.shape[2]
    for lo in range(0, width, 256):
        block = dot(a, b[:, lo:lo + 256], TN)
        for q in range(4):
            part[q, :, lo:lo + 256] = block[q * quarter:(q + 1) * quarter]


def norm_parts(rows):
    xf = rows.astype(F32)
    inv = lax.rsqrt(jnp.mean(xf * xf, axis=-1, keepdims=True) + NORM_EPS)
    return inv, xf * inv


def norm(rows, gain):
    return (norm_parts(rows)[1] * gain).astype(BF16)


def norm_back(d_norm, rows, gain):
    inv, normed = norm_parts(rows)
    d_normed = d_norm * gain
    return inv * (d_normed - normed * jnp.mean(d_normed * normed, axis=-1, keepdims=True)), d_norm * normed


def key_add(mask_ref, b):
    row = jnp.concatenate([mask_ref[j, pl.ds(b, 1), :] for j in range(4)], axis=1)
    return jnp.where(row > 0, 0.0, MASK_NEG).astype(F32)


def exp_scores(q, k, bias, add):
    s = dot(q, k, NT) + bias + add
    e = jnp.exp(s - jnp.max(s, axis=-1, keepdims=True))
    return e, jnp.sum(e, axis=-1, keepdims=True)


def any_specs(n):
    return [pl.BlockSpec(memory_space=pl.ANY)] * n


def gelu_parts(g):
    inner = np.float32(np.sqrt(2 / np.pi)) * (g + 0.044715 * (g * g * g))
    t = jnp.tanh(inner)
    cdf = 0.5 * (1.0 + t)
    slope = cdf + 0.5 * g * (1.0 - t * t) * np.float32(np.sqrt(2 / np.pi)) * (1.0 + 3 * 0.044715 * (g * g))
    return g * cdf, slope


def order(z, y):
    return [(1 - z, 1 - y), (1 - z, y), (z, 1 - y), (z, y)]


def sum_scratch(width, blocks=()):
    return [pltpu.VMEM((2, 2, 2) + blocks, F32), pltpu.VMEM((2, 2) + blocks, F32), pltpu.VMEM((2,) + blocks, F32)]


def forward_kernel(seq, *refs):
    refs = list(refs)
    take = lambda n: [refs.pop(0) for _ in range(n)]
    x_in, d_y, wo_in, wq_in, wk_in, wv_in, wg_in, wl_in, wd_in, mask_in, ga_ref, gm_ref, rb_ref = take(13)
    x0_out, a0_out, x1_out, a1_out, dy_out, q_out, k_out, v_out, o_out, mask_ref, t_ref = take(11)
    x0_ref, a0_ref, x1_ref, a1_ref, dyo_ref, q_ref, k_ref, v_ref, o_ref = take(9)
    wq_ref, wk_ref, wv_ref, wg_ref, wl_ref, wd_ref, wf_ref = take(7)
    bias_ref, of_ref, part, near, far = take(5)
    xsend, xrecv, osend, orecv, send, recv, lsem, ssem = refs
    tp, cp, z, y, x, core, ids = place()
    near_by, far_by = ['core', 'x', 'xc'], ['z', 'y', 'zy']

    def local(src, dst, sem):
        copy = pltpu.make_async_copy(src, dst, sem)
        copy.start()
        return copy

    own_x = local(x_in.at[cp], x0_ref.at[:, cp], lsem.at[0])
    qkv_loads = [local(w, r, lsem.at[1 + i]) for i, (w, r) in enumerate([(wq_in, wq_ref), (wk_in, wk_ref), (wv_in, wv_ref)])]
    own_w = [local(wo_in.at[layer], wf_ref.at[layer, tp], lsem.at[4 + layer]) for layer in range(2)]
    mlp_loads = [local(w.at[0], r, lsem.at[6 + i]) for i, (w, r) in enumerate([(wg_in, wg_ref), (wl_in, wl_ref), (wd_in, wd_ref)])]
    own_dy = local(d_y.at[cp], dyo_ref, lsem.at[9])
    meet(ids, near_by + far_by)
    masks, xs = [], []
    for i, name in enumerate(near_by):
        masks.append(remote(mask_in.at[ids[name]['cp']], mask_ref.at[cp], xsend.at[i], xrecv.at[i], ids[name]))
        xs.append(remote(x_in.at[ids[name]['cp']], x0_ref.at[:, cp], xsend.at[3 + i], xrecv.at[3 + i], ids[name]))
    weights = [remote(wo_in.at[core], wf_ref.at[core, tp], xsend.at[6 + i], xrecv.at[6 + i], ids[name]) for i, name in enumerate(far_by)]
    mask_ref[cp] = mask_in[cp]
    place_row = lax.broadcasted_iota(jnp.int32, (1, 2 * seq), 1)
    bucket = rel_bucket(place_row - seq)
    for head in range(t_ref.shape[0]):
        row = jnp.zeros((1, 2 * seq), F32)
        for j in range(32):
            row = jnp.where(bucket == j, rb_ref[j:j + 1, head:head + 1], row)
        t_ref[head:head + 1, :] = row
    for head in range(t_ref.shape[0]):
        bias_ref[head] = toeplitz(t_ref[head:head + 1, :], seq)

    def project(layer, rows):
        h = norm(rows, ga_ref[layer:layer + 1, :])
        return [dot(h, w[layer]).astype(BF16) for w in (wq_ref, wk_ref, wv_ref)]

    def attention(layer, b):
        add = key_add(mask_ref, b)
        for head in range(t_ref.shape[0]):
            cols = pl.ds(head * HEAD, HEAD)
            e, total = exp_scores(q_ref[layer, b, :, cols], k_ref[layer, b, :, cols], bias_ref[head], add)
            o = (dot(e.astype(BF16), v_ref[layer, b, :, cols]) / total).astype(BF16)
            o_ref[layer, b, 0, :, cols] = o[:seq // 2]
            o_ref[layer, b, 1, :, cols] = o[seq // 2:]

    def ship(layer, name, b, half):
        i = layer * 3 + far_by.index(name)
        return remote(o_ref.at[layer, b, half], of_ref.at[layer, tp], osend.at[i], orecv.at[i], ids[name])

    def project_out(layer, sent, residual, out_ref):
        of_ref[layer, tp] = o_ref[layer, z, y]
        for copy in sent:
            copy.wait_recv()
        streams = colours(None, None, None, lambda q, c, piece: out_ref.at[q[0], q[1], c], send.at[4 * layer:4 * layer + 2], recv.at[4 * layer:4 * layer + 2], ids, z, y)
        for c, s in enumerate(streams):
            rows = pl.ds(c * 128, 128)
            total = sum(dot(of_ref[layer, j, rows, :], wf_ref[layer, j]) for j in range(4))
            out_ref[z, y, c] = (residual(c).astype(F32) + total).astype(BF16)
            s.publish()
        for s in streams:
            s.gather()
        for s in streams:
            s.close()

    for copy in qkv_loads:
        copy.wait()
    for i, name in enumerate(['own'] + near_by):
        if i == 0:
            own_x.wait()
            blk = cp
        else:
            xs[i - 1].wait_recv()
            blk = ids[name]['cp']
        for d_ref, value in zip((q_ref, k_ref, v_ref), project(0, x0_ref[:, blk].reshape(2 * 128, -1))):
            for b in range(2):
                d_ref[0, b, pl.ds(pl.multiple_of(blk * 128, 128), 128), :] = value[b * 128:(b + 1) * 128]
    own_dy.wait()
    saves = [local(x0_ref, x0_out, ssem.at[0]), local(dyo_ref, dy_out.at[:, cp], ssem.at[1])]
    moves = [remote(d_y.at[ids[name]['cp']], dy_out.at[:, cp], xsend.at[12 + i], xrecv.at[12 + i], ids[name]) for i, name in enumerate(near_by)]
    for copy in masks:
        copy.wait_recv()
    attention(0, 1 - z)
    sent = [ship(0, 'zy', 1 - z, 1 - y), ship(0, 'z', 1 - z, y)]
    passed = []
    for i, name in enumerate(far_by):
        weights[i].wait_recv()
        got = wf_ref.at[core, ids[name]['tp']]
        passed.append(remote(got, got, xsend.at[9 + i], xrecv.at[9 + i], ids['core']))
    attention(0, z)
    sent.append(ship(0, 'y', z, 1 - y))
    for copy in own_w:
        copy.wait()
    for copy in passed:
        copy.wait_recv()
    project_out(0, sent, lambda c: x0_ref[z, y * 2 + c], a0_ref)
    saves.append(local(a0_ref, a0_out, ssem.at[2]))

    for copy in mlp_loads:
        copy.wait()
    zy, yz = streams = colours(part, near, far, lambda q, c, piece: x1_ref.at[q[0], q[1], c, pl.ds(piece * 64, 64)], send.at[2:4], recv.at[2:4], ids, z, y, 2)

    def mlp_quarter(q):
        h2 = norm(a0_ref[q].reshape(256, -1), gm_ref[0:1, :])
        gated = (gelu_parts(dot(h2, wg_ref[...], NT))[0] * dot(h2, wl_ref[...], NT)).astype(BF16)
        part[q] = dot(gated, wd_ref[...]).reshape(part.shape[2:])

    quarters = order(z, y)
    mlp_quarter(quarters[0])
    zy.send_away(0)
    yz.send_away(0)
    mlp_quarter(quarters[1])
    zy.send_away(1)
    mlp_quarter(quarters[2])
    yz.send_away(1)
    mlp_quarter(quarters[3])
    for s in streams:
        s.forward()
    for piece in range(2):
        rows = pl.ds(piece * 64, 64)
        for c, s in enumerate(streams):
            x1_ref[z, y, c, rows, :] = (a0_ref[z, y, c, rows, :].astype(F32) + s.total(piece)).astype(BF16)
            s.publish(piece)
    for s in streams:
        s.gather()
    for s in streams:
        s.close()
    saves.append(local(x1_ref, x1_out, ssem.at[3]))

    late = []
    for step in range(2):
        b = 1 - z if step == 0 else z
        for half in range(2):
            rows = pl.ds(half * 256, 256)
            for d_ref, value in zip((q_ref, k_ref, v_ref), project(1, x1_ref[b, half].reshape(256, -1))):
                d_ref[1, b, rows, :] = value
        attention(1, b)
        if step == 0:
            late += [ship(1, 'zy', b, 1 - y), ship(1, 'z', b, y)]
        else:
            late.append(ship(1, 'y', b, 1 - y))
    saves += [local(src, dst, ssem.at[4 + i]) for i, (src, dst) in enumerate([(q_ref, q_out), (k_ref, k_out), (v_ref, v_out), (o_ref, o_out)])]
    project_out(1, late, lambda c: x1_ref[z, y, c], a1_ref)
    saves.append(local(a1_ref, a1_out, ssem.at[8]))
    for copy in masks + xs + weights + passed + sent + late:
        copy.wait_send()
    for copy in moves + saves:
        copy.wait()


def forward(x_in, d_y, key_mask, gains_a, gains_m, w_q, w_k, w_v, w_o, wg_t, wl_t, w_out, rel_bias):
    batch, blk, width = x_in.shape
    seq, cols = 4 * blk, w_q.shape[2]
    dma = pltpu.SemaphoreType.DMA
    blocks = (2, 2, 2, blk, width)
    arrived = (2, 4, blk, width)
    heads = (2, 2, seq, cols)
    halves = (2, 2, 2, seq // 2, cols)
    hbm = [arrived, blocks, blocks, blocks, arrived, heads, heads, heads, halves]
    operands = [x_in.reshape(4, 2, blk, width), d_y.reshape(4, 2, blk, width), w_o, w_q, w_k, w_v, wg_t, wl_t, w_out,
                key_mask.reshape(4, 2, blk), gains_a, gains_m, rel_bias]
    scratch = [pltpu.VMEM(h, BF16) for h in hbm[:4] + [(2, blk, width)] + hbm[5:]]
    scratch += [pltpu.VMEM(w.shape, BF16) for w in (w_q, w_k, w_v)] + [pltpu.VMEM(w.shape[1:], BF16) for w in (wg_t, wl_t, w_out)]
    scratch += [pltpu.VMEM((2, 4) + w_o.shape[1:], BF16), pltpu.VMEM((rel_bias.shape[1], seq, seq), F32), pltpu.VMEM((2, 4, 2 * blk, cols), BF16)]
    scratch += sum_scratch(0, blocks[3:])
    scratch += [dma((15,)), dma((15,)), dma((6,)), dma((6,)), dma((6, 10)), dma((6, 10)), dma((10,)), dma((9,))]
    return pl.pallas_call(
        functools.partial(forward_kernel, seq),
        out_shape=[jax.ShapeDtypeStruct(h, BF16) for h in hbm] + [jax.ShapeDtypeStruct((4, 2, blk), jnp.int32), jax.ShapeDtypeStruct((rel_bias.shape[1], 2 * seq), F32)],
        in_specs=any_specs(9) + vmem_specs(4), out_specs=any_specs(9) + vmem_specs(2),
        scratch_shapes=scratch,
        compiler_params=pltpu.CompilerParams(collective_id=0, has_side_effects=True, vmem_limit_bytes=62 << 20),
        cost_estimate=pl.CostEstimate(flops=15 << 30, bytes_accessed=48 << 20, transcendentals=0),
        name="forward",
    )(*operands)


def backward_kernel(seq, *refs):
    refs = list(refs)
    take = lambda n: [refs.pop(0) for _ in range(n)]
    stacks = take(7)
    x1_all, dy_in, x_all, heads_all = take(2), refs.pop(0), take(2), take(4)
    ga_ref, gm_ref, t_ref, mask_ref = take(4)
    dx_ref, small_out = take(2)
    grad_out = take(7)
    weights, holds = take(7), take(7)
    lsem, part, near, far, dm_ref, h_ref, gated_ref, dgate_ref, dlin_ref = take(9)
    bias_ref, dt_ref = take(2)
    dq_ref, dk_ref = dgate_ref.at[:, :, 0:256], dgate_ref.at[:, :, 256:512]
    dv_ref, do_ref = dlin_ref.at[:, :, 0:256], dlin_ref.at[0, :, 256:512]
    grad_scratch = [take(4) for _ in range(7)]
    send, recv, gsend, grecv, kept, own_ref, acc_small, got_small, msend, mrecv, csend, crecv = refs
    wg_ref, wl_ref, wd_ref, wq_ref, wk_ref, wv_ref, wo_ref = weights
    x1_ref, dy_ref, x_ref, q_ref, k_ref, v_ref, o_ref = holds
    tp, cp, z, y, x, core, ids = place()
    heads = t_ref.shape[0]
    width = x_ref.shape[-1]
    quarters = order(z, y)
    p_out, p_gate, p_lin, p_o, p_q, p_k, p_v = [g[0] for g in grad_scratch]

    def fetch(layer, attention):
        if attention:
            pairs = [(x_all[layer], x_ref)] + [(h.at[layer], r) for h, r in zip(heads_all, (q_ref, k_ref, v_ref, o_ref))]
            pairs += [(w.at[layer], r) for w, r in zip(stacks[3:], weights[3:])]
        else:
            pairs = [(x1_all[layer], x1_ref)] + ([(dy_in, dy_ref)] if layer == 1 else []) + [(w.at[layer], r) for w, r in zip(stacks[:3], weights[:3])]
        copies = [pltpu.make_async_copy(src, dst, lsem.at[int(attention), layer, i]) for i, (src, dst) in enumerate(pairs)]
        for copy in copies:
            copy.start()
        return copies

    def mlp_quarter(q, gain, write_gated):
        h2 = norm(x1_ref[q].reshape(256, -1), gain)
        rows = pl.ds(pl.multiple_of((q[0] * 2 + q[1]) * 256, 256), 256)
        h_ref[rows, :] = h2
        value, slope = gelu_parts(dot(h2, wg_ref[...], NT))
        lin = dot(h2, wl_ref[...], NT)
        if write_gated:
            gated_ref[rows, :] = (value * lin).astype(BF16)
        d_gated = dot(dy_ref[q].reshape(256, -1), wd_ref[...], NT)
        d_lin = (d_gated * value).astype(BF16)
        d_gate = (d_gated * lin * slope).astype(BF16)
        in_batch = pl.ds(pl.multiple_of(q[1] * 256, 256), 256)
        dlin_ref[q[0], in_batch, :] = d_lin
        dgate_ref[q[0], in_batch, :] = d_gate
        part[q] = (dot(d_gate, wg_ref[...]) + dot(d_lin, wl_ref[...])).reshape(part.shape[2:])

    def attend(b, first, hook):
        add = key_add(mask_ref, b)
        do_ref[...] = dot(dm_ref[b].reshape(seq, width), wo_ref[...], NT).astype(BF16)
        for head in range(heads):
            cols = pl.ds(head * HEAD, HEAD)
            q, k, v, do = q_ref[b, :, cols], k_ref[b, :, cols], v_ref[b, :, cols], do_ref[:, cols]
            e, total = exp_scores(q, k, bias_ref[head], add)
            p = e * (1.0 / total)
            row_dot = jnp.sum(do.astype(F32) * o_ref[b, :, cols].astype(F32), axis=-1, keepdims=True)
            ds = p * (dot(do, v, NT) - row_dot)
            sums = diag_sums(ds, seq)
            dt_ref[head:head + 1, :] = sums if first else dt_ref[head:head + 1, :] + sums
            dsl = ds.astype(BF16)
            dq_ref[b, :, cols] = dot(dsl, k).astype(BF16)
            dk_ref[b, :, cols] = dot(dsl, q, TN).astype(BF16)
            dv_ref[b, :, cols] = dot(p.astype(BF16), do, TN).astype(BF16)
            if head == 0:
                hook()

    loads = {(1, False): fetch(1, False), (1, True): fetch(1, True)}
    meet(ids, ['z', 'y', 'x', 'core', 'xc'])
    pending = []
    for layer in (1, 0):
        last = layer == 0
        deep = 32 if last else 128
        across = 128 // deep
        half = deep // 2
        g_out, g_gate, g_lin, g_o, g_q, g_k, g_v = grads = [
            GradStream(*grad_scratch[i], grad_out[i].at[layer], gsend.at[layer, i], grecv.at[layer, i], kept.at[layer, i], ids, x, core) for i in range(7)]
        zy, yz = mlp_sum = colours(part, near, far, lambda q, c, piece: dm_ref.at[q[0], q[1], c, pl.ds(piece * 64, 64)],
                                   send.at[layer, 0:2], recv.at[layer, 0:2], ids, z, y, 2)
        if not last:
            for copy in loads[layer, False]:
                copy.wait()
        gain, gain_a = gm_ref[layer:layer + 1, :], ga_ref[layer:layer + 1, :]
        mlp_quarter(quarters[0], gain, not last)
        zy.send_away(0)
        yz.send_away(0)
        if last:
            for g in pending[:1]:
                g.gather()
            grad_into(p_out, gated_ref[...], dy_ref[...].reshape(h_ref.shape))
            g_out.send_both()
        mlp_quarter(quarters[1], gain, not last)
        zy.send_away(1)
        mlp_quarter(quarters[2], gain, not last)
        yz.send_away(1)
        if last:
            g_out.forward()
        mlp_quarter(quarters[3], gain, not last)
        if not last:
            grad_into(p_out, gated_ref[...], dy_ref[...].reshape(h_ref.shape))
            g_out.send_both()
        grad_into(p_gate, dgate_ref[...].reshape(2 * seq, -1), h_ref)
        g_gate.send_both()
        if not last:
            g_out.forward()
        for s in mlp_sum:
            s.forward()
        for g in pending[1:]:
            g.gather()
        grad_into(p_lin, dlin_ref[...].reshape(2 * seq, -1), h_ref)
        g_lin.send_both()
        g_gate.forward()
        if not last:
            for head in range(heads):
                bias_ref[head] = toeplitz(t_ref[head:head + 1, :], seq)
        for copy in loads[layer, True]:
            copy.wait()
        for b in range(2):
            h_ref[b * seq:(b + 1) * seq, :] = norm(x_ref[b], gain_a)
        g_lin.forward()
        for g in pending:
            g.close()
        g_out.finish()
        dg_m = 0.0
        for piece in range(2):
            rows = pl.ds(piece * 64, 64)
            for c, s in enumerate(mlp_sum):
                d_x, dg = norm_back(s.total(piece), x1_ref[z, y, c, rows, :], gain)
                dm_ref[z, y, c, rows, :] = (d_x + dy_ref[z, y, c, rows, :].astype(F32)).astype(BF16)
                s.publish(piece)
                dg_m = dg_m + jnp.sum(dg, axis=0, keepdims=True)
        g_gate.finish()
        for s in mlp_sum:
            s.gather()
        for s in mlp_sum:
            s.close()
        if not last:
            loads[0, False] = fetch(0, False)

        if last:
            def region(q, c, piece):
                return dx_ref.at[:, q[0], q[1], c, pl.ds(piece * 16, 16)]
        else:
            def region(q, c, piece):
                return dy_ref.at[q[0], q[1], c, pl.ds(piece * 64, 64)]
        zy, yz = attn_sum = colours(part, near, far, region, send.at[layer, 2:4], recv.at[layer, 2:4], ids, z, y, 2)

        def pick(ref, offset, size, q):
            pieces = [ref[q[0], pl.ds(pl.multiple_of(j * 4 * deep + q[1] * 2 * deep + offset, half), size), :] for j in range(across)]
            return pieces[0] if across == 1 else jnp.concatenate(pieces, axis=0)

        def attn_quarter(q):
            total = sum(dot(pick(d, 0, 2 * deep, q), w[...], NT) for d, w in [(dq_ref, wq_ref), (dk_ref, wk_ref), (dv_ref, wv_ref)])
            total = total.reshape(across, 2, 2, half, width)
            for c in range(2):
                for piece in range(2):
                    part[q[0], q[1], c, pl.ds(piece * 64, 64), :] = total[:, c, piece].reshape(64, width)

        attend(1 - z, not last, lambda: None)
        attn_quarter(quarters[0])
        zy.send_away(0)
        yz.send_away(0)
        attn_quarter(quarters[1])
        zy.send_away(1)
        grad_into(p_o, o_ref[...].reshape(2 * seq, -1), dm_ref[...].reshape(2 * seq, width))
        g_o.send_both()
        g_lin.finish()
        g_out.gather()
        attend(z, False, g_o.forward)
        attn_quarter(quarters[2])
        yz.send_away(1)
        attn_quarter(quarters[3])
        for g, p, d in [(g_q, p_q, dq_ref), (g_k, p_k, dk_ref), (g_v, p_v, dv_ref)]:
            grad_into(p, h_ref[...], d[...].reshape(2 * seq, -1))
            g.send_both()
        for s in attn_sum:
            s.forward()
        for g in [g_q, g_k, g_v]:
            g.forward()
        if not last:
            for copy in loads[0, False]:
                copy.wait()
            for i in range(4):
                h2 = norm(x1_ref[i // 2, i % 2].reshape(256, -1), gm_ref[0:1, :])
                gated_ref[i * 256:(i + 1) * 256, :] = (gelu_parts(dot(h2, wg_ref[...], NT))[0] * dot(h2, wl_ref[...], NT)).astype(BF16)
        g_gate.gather()
        g_lin.gather()
        g_o.finish()
        dg_a = 0.0
        moves = {}
        for piece in range(2):
            for c, s in enumerate(attn_sum):
                rows = pl.ds(piece * half, half)
                d_x, dg = norm_back(s.total(piece), pick(x_ref, c * deep + piece * half, half, (z, y)), gain_a)
                dg_a = dg_a + jnp.sum(dg, axis=0, keepdims=True)
                if last:
                    at = pl.ds(pl.multiple_of(y * 2 * deep + c * deep + piece * half, half), half)
                    res = jnp.concatenate([dm_ref[z, j // 2, j % 2, at, :] for j in range(4)], axis=0)
                else:
                    res = dm_ref[z, y, c, rows, :]
                d_x = (d_x + res.astype(F32)).astype(BF16)
                if last:
                    own_ref[c, piece] = d_x.reshape(across, half, width)
                    dx_ref[cp, z, y, c, rows, :] = own_ref[c, piece, cp]
                    moves[c, piece] = [remote(own_ref.at[c, piece, ids[name]['cp']], dx_ref.at[cp, z, y, c, rows], msend.at[c, piece, i], mrecv.at[c, piece, i], ids[name])
                                       for i, name in enumerate(['x', 'xc', 'core'])]
                else:
                    dy_ref[z, y, c, rows, :] = d_x
                    s.publish(piece)
        acc_small[0, 2 - 2 * layer:3 - 2 * layer, :] = dg_a
        acc_small[0, 3 - 2 * layer:4 - 2 * layer, :] = dg_m
        if not last:
            loads[0, True] = fetch(0, True)
            for g in [g_q, g_k, g_v]:
                g.finish()
            for s in attn_sum:
                s.gather()
            for s in attn_sum + [g_out, g_gate, g_lin]:
                s.close()
            pending = [g_o, g_q, g_k, g_v]

    acc_small[0, 4:8, :] = jnp.zeros((4, width), F32)
    acc_small[0, 8:12, :] = dt_ref[0:4, :]
    acc_small[0, 12:16, :] = jnp.zeros((4, width), F32)
    smalls = []

    def small_start(i):
        rows = pl.ds(0, 16 if i < 2 else 8)
        smalls.append(remote(acc_small.at[i, rows], got_small.at[i, rows], csend.at[i], crecv.at[i], ids[['x', 'core', 'y', 'z'][i]]))

    def small_end(i):
        rows = pl.ds(0, 16 if i < 2 else 8)
        smalls[i].wait_recv()
        acc_small[i + 1, rows, :] = acc_small[i, rows, :] + got_small[i, rows, :]

    small_start(0)
    for piece in range(2):
        for c, s in enumerate(attn_sum):
            for copy in moves[c, piece]:
                copy.wait_recv()
            s.publish(piece)
    g_q.finish()
    small_end(0)
    small_start(1)
    g_k.finish()
    small_end(1)
    small_start(2)
    g_v.finish()
    for s in attn_sum:
        s.gather()
    small_end(2)
    small_start(3)
    for g in [g_o, g_q, g_k, g_v]:
        g.gather()
    small_end(3)
    small_out[0:8, :] = acc_small[4, 0:8, :]
    small_out[8:16, :] = acc_small[2, 8:16, :]
    for copy in smalls + sum(moves.values(), []):
        copy.wait_send()
    for s in attn_sum + grads:
        s.close()


def backward(x1s, dy, xs, heads, gains_a, gains_m, wg_t, wl_t, w_out, w_q, w_k, w_v, w_o, table, mask):
    seq, width, cols = 512, w_q.shape[1], w_q.shape[2]
    ff = w_out.shape[1]
    rows = 2 * seq
    dma = pltpu.SemaphoreType.DMA
    blocks = (2, 2, 2, 128, width)
    flat = (2, seq, width)
    stacks = [wg_t, wl_t, w_out, w_q, w_k, w_v, w_o]
    operands = stacks + [a.reshape(blocks) for a in x1s] + [dy.reshape(blocks)] + [a.reshape(flat) for a in xs]
    operands += [h.reshape(2, 2, seq, cols) for h in heads] + [gains_a, gains_m, table, mask]
    grads = [(ff // 4, width)] * 3 + [(cols // 4, width)] + [(width // 4, cols)] * 3
    out_shape = [jax.ShapeDtypeStruct((4, 2, 2, 2, 32, width), BF16), jax.ShapeDtypeStruct((16, width), F32)]
    out_shape += [jax.ShapeDtypeStruct((2, 4) + g, BF16) for g in grads]
    scratch = [pltpu.VMEM(w.shape[1:], BF16) for w in stacks]
    scratch += [pltpu.VMEM(blocks, BF16)] * 2 + [pltpu.VMEM(flat, BF16)] + [pltpu.VMEM((2, seq, cols), BF16)] * 4 + [dma((2, 2, 9))]
    scratch += sum_scratch(0, blocks[3:]) + [pltpu.VMEM(blocks, BF16), pltpu.VMEM((rows, width), BF16), pltpu.VMEM((rows, ff), BF16)] + [pltpu.VMEM((2, seq, ff), BF16)] * 2
    scratch += [pltpu.VMEM((table.shape[0], seq, seq), F32), pltpu.VMEM((8, 2 * seq), F32)]
    for g in grads:
        scratch += [pltpu.VMEM((4,) + g, F32), pltpu.VMEM((2,) + g, F32), pltpu.VMEM(g, F32), pltpu.VMEM(g, BF16)]
    scratch += [dma((2, 4, 10)), dma((2, 4, 10)), dma((2, 7, 6)), dma((2, 7, 6)), dma((2, 7))]
    scratch += [pltpu.VMEM((2, 2, 4, 16, width), BF16), pltpu.VMEM((5, 16, width), F32), pltpu.VMEM((4, 16, width), F32)]
    scratch += [dma((2, 2, 3)), dma((2, 2, 3)), dma((4,)), dma((4,))]
    return pl.pallas_call(
        functools.partial(backward_kernel, seq),
        out_shape=out_shape, in_specs=any_specs(16) + vmem_specs(4), out_specs=vmem_specs(2) + any_specs(7),
        scratch_shapes=scratch,
        compiler_params=pltpu.CompilerParams(collective_id=1, has_side_effects=True, vmem_limit_bytes=67043328),
        cost_estimate=pl.CostEstimate(flops=40 << 30, bytes_accessed=96 << 20, transcendentals=0),
        name="backward",
    )(*operands)


def vmem_specs(n):
    return [pl.BlockSpec(memory_space=pltpu.VMEM)] * n


def solution(mesh):
    seq_spec = P(None, 'cp', None)
    col_spec = P(None, None, 'tp')
    row_spec = P(None, 'tp', None)
    weight_specs = (P(), P(), col_spec, col_spec, col_spec, row_spec, col_spec, col_spec, row_spec)

    def local_program(x_in, d_y, key_mask, rel_bias, g_attn, g_mlp, w_q, w_k, w_v, w_o, w_gate, w_lin, w_out):
        width = x_in.shape[2]
        onehot = bucket_onehot(512)
        wg_t, wl_t = jnp.swapaxes(w_gate, 1, 2), jnp.swapaxes(w_lin, 1, 2)
        x0, a0, x1, a1, dy, q, k, v, o, mask, table = forward(x_in, d_y, key_mask, g_attn, g_mlp, w_q, w_k, w_v, w_o, wg_t, wl_t, w_out, rel_bias)

        outs = backward((a0, a1), dy, (x0, x1), (q, k, v, o), g_attn, g_mlp, wg_t, wl_t, w_out, w_q, w_k, w_v, w_o, table, mask)
        d_x, small = outs[:2]
        d_out, d_gate, d_lin, d_wo, d_wq, d_wk, d_wv = [g.reshape(2, -1, g.shape[-1]) for g in outs[2:]]
        d_gate, d_lin = jnp.swapaxes(d_gate, 1, 2), jnp.swapaxes(d_lin, 1, 2)

        d_bias = jnp.sum(jnp.where(onehot[None], small[8:12][:, None, :], 0.0), axis=2).T
        d_ga = jnp.stack([small[2], small[0]])
        d_gm = jnp.stack([small[3], small[1]])
        return d_x.reshape(x_in.shape), d_bias, d_ga, d_gm, d_wq, d_wk, d_wv, d_wo, d_gate, d_lin, d_out

    return jax.shard_map(local_program, mesh=mesh, in_specs=(seq_spec, seq_spec, P(None, 'cp'), P(None, 'tp')) + weight_specs, out_specs=(seq_spec, P(None, 'tp')) + weight_specs, check_vma=False)
```

```python
import functools
import jax
import jax.numpy as jnp
import numpy as np
from jax import lax
from jax.experimental import pallas as pl
from jax.experimental.pallas import tpu as pltpu
from jax.sharding import PartitionSpec as P

NORM_EPS = 1e-6
MASK_NEG = -1e9
HEAD = 64
F32 = jnp.float32
BF16 = jnp.bfloat16
NT = (((1,), (1,)), ((), ()))
TN = (((0,), (0,)), ((), ()))


def rel_bucket(rel_pos):
    distance = jnp.minimum(jnp.abs(rel_pos), 128)
    distance_sq = distance * distance
    log_part = 8 + sum((distance_sq >= 64 * 2 ** power).astype(jnp.int32) for power in range(1, 8))
    return jnp.where(distance < 8, distance, log_part) + 16 * (rel_pos > 0).astype(jnp.int32)


def dot(a, b, dims=(((1,), (0,)), ((), ()))):
    return lax.dot_general(a, b, dims, preferred_element_type=F32)


def toeplitz(row, seq):
    base = pltpu.roll(row, seq, 1)
    rows = jnp.concatenate([base if i == 0 else pltpu.roll(base, i, 1) for i in range(8)], axis=0)
    size = 8
    while size < seq:
        rows = jnp.concatenate([rows, pltpu.roll(rows, size, 1)], axis=0)
        size *= 2
    return rows[:, :seq]


def diag_sums(mat, seq):
    wide = jnp.concatenate([mat, jnp.zeros_like(mat)], axis=1)
    size = seq
    while size > 1:
        half = size // 2
        wide = wide[:half] + pltpu.roll(wide[half:size], 2 * seq - half, 1)
        size = half
    return pltpu.roll(wide, seq, 1)


def place():
    tp, cp = lax.axis_index('tp'), lax.axis_index('cp')
    z, y = tp // 2, tp % 2
    x, core = cp // 2, cp % 2
    peers = {'z': (1 - z, y, x, core), 'y': (z, 1 - y, x, core), 'x': (z, y, 1 - x, core), 'core': (z, y, x, 1 - core),
             'zy': (1 - z, 1 - y, x, core), 'xc': (z, y, 1 - x, 1 - core)}
    ids = {name: {'tp': p[0] * 2 + p[1], 'cp': p[2] * 2 + p[3]} for name, p in peers.items()}
    return tp, cp, z, y, x, core, ids


def meet(ids, names):
    barrier = pltpu.get_barrier_semaphore()
    for name in names:
        pl.semaphore_signal(barrier, inc=1, device_id=ids[name], device_id_type=pl.DeviceIdType.MESH)
    pl.semaphore_wait(barrier, len(names))


def remote(src, dst, send, recv, target):
    copy = pltpu.make_async_remote_copy(src_ref=src, dst_ref=dst, send_sem=send, recv_sem=recv,
                                        device_id=target, device_id_type=pl.DeviceIdType.MESH)
    copy.start()
    return copy


class Stream:
    def __init__(self, part, near, far, out, send, recv, first, second, a, b, index, pieces=1):
        self.part, self.near, self.far, self.out = part, near, far, out
        self.send, self.recv = send, recv
        self.first, self.second = first, second
        self.own, self.pass_on = index(a, b), index(a, 1 - b)
        self.away_far, self.away = index(1 - a, 1 - b), index(1 - a, b)
        self.pieces = pieces
        self.copies = {}
        self.arrived = False

    def start(self, name, piece, src, dst, target):
        slot = name if name < 2 else 2 + (name - 2) * self.pieces + piece
        self.copies[name, piece] = remote(src, dst, self.send.at[slot], self.recv.at[slot], target)

    def rows(self, ref, piece):
        if self.pieces == 1:
            return ref
        size = ref.shape[0] // self.pieces
        return ref.at[pl.ds(piece * size, size)]

    def send_away(self, slot):
        quarter = self.away_far if slot == 0 else self.away
        self.start(slot, 0, self.part(quarter), self.near.at[slot], self.first)

    def forward(self):
        self.copies[0, 0].wait_recv()
        for piece in range(self.pieces):
            ref = self.rows(self.part(self.pass_on), piece)
            ref[...] += self.rows(self.near.at[0], piece)[...]
            self.start(2, piece, ref, self.rows(self.far, piece), self.second)

    def total(self, piece=0):
        if not self.arrived:
            self.copies[1, 0].wait_recv()
            self.arrived = True
        self.copies[2, piece].wait_recv()
        return self.rows(self.part(self.own), piece)[...] + self.rows(self.near.at[1], piece)[...] + self.rows(self.far, piece)[...]

    def publish(self, piece=0):
        out = self.out(self.own, piece)
        self.start(3, piece, out, out, self.first)
        self.start(4, piece, out, out, self.second)

    def gather(self):
        for piece in range(self.pieces):
            self.copies[4, piece].wait_recv()
            out = self.out(self.pass_on, piece)
            self.start(5, piece, out, out, self.first)

    def close(self):
        for piece in range(self.pieces):
            self.copies[3, piece].wait_recv()
            self.copies[5, piece].wait_recv()
        for copy in self.copies.values():
            copy.wait_send()


def colours(part, near, far, out, send, recv, ids, z, y, pieces=1):
    def make(c, first, second, a, b, index):
        return Stream(lambda q: part.at[q[0], q[1], c], None if near is None else near.at[c], None if far is None else far.at[c],
                      lambda q, piece: out(q, c, piece), send.at[c], recv.at[c], ids[first], ids[second], a, b, index, pieces)
    return [make(0, 'z', 'y', z, y, lambda a, b: (a, b)), make(1, 'y', 'z', y, z, lambda a, b: (b, a))]


class GradStream(Stream):
    def __init__(self, part, near, far, own_ref, out, send, recv, local, ids, x, core):
        super().__init__(lambda q: part.at[q], near, far, lambda q, piece: out.at[q], send, recv,
                         ids['core'], ids['x'], core, x, lambda a, b: b * 2 + a)
        self.own_ref, self.local = own_ref, local

    def send_both(self):
        self.send_away(0)
        self.send_away(1)

    def finish(self):
        self.own_ref[...] = self.total().astype(BF16)
        out = self.out(self.own, 0)
        self.start(4, 0, self.own_ref, out, self.second)
        self.start(3, 0, self.own_ref, out, self.first)
        self.kept = pltpu.make_async_copy(self.own_ref, out, self.local)
        self.kept.start()

    def close(self):
        super().close()
        self.kept.wait()


def grad_into(part, a, b):
    quarter, width = part.shape[1], part.shape[2]
    for lo in range(0, width, 256):
        block = dot(a, b[:, lo:lo + 256], TN)
        for q in range(4):
            part[q, :, lo:lo + 256] = block[q * quarter:(q + 1) * quarter]


def norm_parts(rows):
    xf = rows.astype(F32)
    inv = lax.rsqrt(jnp.mean(xf * xf, axis=-1, keepdims=True) + NORM_EPS)
    return inv, xf * inv


def norm(rows, gain):
    return (norm_parts(rows)[1] * gain).astype(BF16)


def norm_back(d_norm, rows, gain):
    inv, normed = norm_parts(rows)
    d_normed = d_norm * gain
    return inv * (d_normed - normed * jnp.mean(d_normed * normed, axis=-1, keepdims=True)), d_norm * normed


def key_add(mask_ref, b):
    row = jnp.concatenate([mask_ref[j, pl.ds(b, 1), :] for j in range(4)], axis=1)
    return jnp.where(row > 0, 0.0, MASK_NEG).astype(F32)


def exp_scores(q, k, bias, add):
    s = dot(q, k, NT) + bias + add
    e = jnp.exp(s - jnp.max(s, axis=-1, keepdims=True))
    return e, jnp.sum(e, axis=-1, keepdims=True)


def any_specs(n):
    return [pl.BlockSpec(memory_space=pl.ANY)] * n


def gelu_parts(g):
    inner = np.float32(np.sqrt(2 / np.pi)) * (g + 0.044715 * (g * g * g))
    t = jnp.tanh(inner)
    cdf = 0.5 * (1.0 + t)
    slope = cdf + 0.5 * g * (1.0 - t * t) * np.float32(np.sqrt(2 / np.pi)) * (1.0 + 3 * 0.044715 * (g * g))
    return g * cdf, slope


def order(z, y):
    return [(1 - z, 1 - y), (1 - z, y), (z, 1 - y), (z, y)]


def sum_scratch(width, blocks=()):
    return [pltpu.VMEM((2, 2, 2) + blocks, F32), pltpu.VMEM((2, 2) + blocks, F32), pltpu.VMEM((2,) + blocks, F32)]


def forward_kernel(seq, *refs):
    refs = list(refs)
    take = lambda n: [refs.pop(0) for _ in range(n)]
    x_in, d_y, wo_in, wq_in, wk_in, wv_in, wg_in, wl_in, wd_in, mask_in, ga_ref, gm_ref, rb_ref = take(13)
    x0_out, a0_out, x1_out, a1_out, dy_out, q_out, k_out, v_out, o_out, mask_ref, t_ref = take(11)
    x0_ref, a0_ref, x1_ref, a1_ref, dyo_ref, q_ref, k_ref, v_ref, o_ref = take(9)
    wq_ref, wk_ref, wv_ref, wg_ref, wl_ref, wd_ref, wf_ref = take(7)
    bias_ref, of_ref, part, near, far = take(5)
    xsend, xrecv, osend, orecv, send, recv, lsem, ssem = refs
    tp, cp, z, y, x, core, ids = place()
    near_by, far_by = ['core', 'x', 'xc'], ['z', 'y', 'zy']

    def local(src, dst, sem):
        copy = pltpu.make_async_copy(src, dst, sem)
        copy.start()
        return copy

    own_x = local(x_in.at[cp], x0_ref.at[:, cp], lsem.at[0])
    qkv_loads = [local(w, r, lsem.at[1 + i]) for i, (w, r) in enumerate([(wq_in, wq_ref), (wk_in, wk_ref), (wv_in, wv_ref)])]
    own_w = [local(wo_in.at[layer], wf_ref.at[layer, tp], lsem.at[4 + layer]) for layer in range(2)]
    mlp_loads = [local(w.at[0], r, lsem.at[6 + i]) for i, (w, r) in enumerate([(wg_in, wg_ref), (wl_in, wl_ref), (wd_in, wd_ref)])]
    own_dy = local(d_y.at[cp], dyo_ref, lsem.at[9])
    meet(ids, near_by + far_by)
    masks, xs = [], []
    for i, name in enumerate(near_by):
        masks.append(remote(mask_in.at[ids[name]['cp']], mask_ref.at[cp], xsend.at[i], xrecv.at[i], ids[name]))
        xs.append(remote(x_in.at[ids[name]['cp']], x0_ref.at[:, cp], xsend.at[3 + i], xrecv.at[3 + i], ids[name]))
    weights = [remote(wo_in.at[core], wf_ref.at[core, tp], xsend.at[6 + i], xrecv.at[6 + i], ids[name]) for i, name in enumerate(far_by)]
    mask_ref[cp] = mask_in[cp]
    place_row = lax.broadcasted_iota(jnp.int32, (1, 2 * seq), 1)
    bucket = rel_bucket(place_row - seq)
    for head in range(t_ref.shape[0]):
        row = jnp.zeros((1, 2 * seq), F32)
        for j in range(32):
            row = jnp.where(bucket == j, rb_ref[head:head + 1, j:j + 1], row)
        t_ref[head:head + 1, :] = row
    for head in range(t_ref.shape[0]):
        bias_ref[head] = toeplitz(t_ref[head:head + 1, :], seq)

    def project(layer, rows):
        h = norm(rows, ga_ref[layer:layer + 1, :])
        return [dot(h, w[layer]).astype(BF16) for w in (wq_ref, wk_ref, wv_ref)]

    def attention(layer, b):
        add = key_add(mask_ref, b)
        for head in range(t_ref.shape[0]):
            cols = pl.ds(head * HEAD, HEAD)
            e, total = exp_scores(q_ref[layer, b, :, cols], k_ref[layer, b, :, cols], bias_ref[head], add)
            o = (dot(e.astype(BF16), v_ref[layer, b, :, cols]) / total).astype(BF16)
            o_ref[layer, b, 0, :, cols] = o[:seq // 2]
            o_ref[layer, b, 1, :, cols] = o[seq // 2:]

    def ship(layer, name, b, half):
        i = layer * 3 + far_by.index(name)
        return remote(o_ref.at[layer, b, half], of_ref.at[layer, tp], osend.at[i], orecv.at[i], ids[name])

    def project_out(layer, sent, residual, out_ref):
        of_ref[layer, tp] = o_ref[layer, z, y]
        for copy in sent:
            copy.wait_recv()
        streams = colours(None, None, None, lambda q, c, piece: out_ref.at[q[0], q[1], c], send.at[4 * layer:4 * layer + 2], recv.at[4 * layer:4 * layer + 2], ids, z, y)
        for c, s in enumerate(streams):
            rows = pl.ds(c * 128, 128)
            total = sum(dot(of_ref[layer, j, rows, :], wf_ref[layer, j]) for j in range(4))
            out_ref[z, y, c] = (residual(c).astype(F32) + total).astype(BF16)
            s.publish()
        for s in streams:
            s.gather()
        for s in streams:
            s.close()

    for copy in qkv_loads:
        copy.wait()
    for i, name in enumerate(['own'] + near_by):
        if i == 0:
            own_x.wait()
            blk = cp
        else:
            xs[i - 1].wait_recv()
            blk = ids[name]['cp']
        for d_ref, value in zip((q_ref, k_ref, v_ref), project(0, x0_ref[:, blk].reshape(2 * 128, -1))):
            for b in range(2):
                d_ref[0, b, pl.ds(pl.multiple_of(blk * 128, 128), 128), :] = value[b * 128:(b + 1) * 128]
    own_dy.wait()
    saves = [local(x0_ref, x0_out, ssem.at[0]), local(dyo_ref, dy_out.at[:, cp], ssem.at[1])]
    moves = [remote(d_y.at[ids[name]['cp']], dy_out.at[:, cp], xsend.at[12 + i], xrecv.at[12 + i], ids[name]) for i, name in enumerate(near_by)]
    for copy in masks:
        copy.wait_recv()
    attention(0, 1 - z)
    sent = [ship(0, 'zy', 1 - z, 1 - y), ship(0, 'z', 1 - z, y)]
    passed = []
    for i, name in enumerate(far_by):
        weights[i].wait_recv()
        got = wf_ref.at[core, ids[name]['tp']]
        passed.append(remote(got, got, xsend.at[9 + i], xrecv.at[9 + i], ids['core']))
    attention(0, z)
    sent.append(ship(0, 'y', z, 1 - y))
    for copy in own_w:
        copy.wait()
    for copy in passed:
        copy.wait_recv()
    project_out(0, sent, lambda c: x0_ref[z, y * 2 + c], a0_ref)
    saves.append(local(a0_ref, a0_out, ssem.at[2]))

    for copy in mlp_loads:
        copy.wait()
    zy, yz = streams = colours(part, near, far, lambda q, c, piece: x1_ref.at[q[0], q[1], c, pl.ds(piece * 64, 64)], send.at[2:4], recv.at[2:4], ids, z, y, 2)

    def mlp_quarter(q):
        h2 = norm(a0_ref[q].reshape(256, -1), gm_ref[0:1, :])
        gated = (gelu_parts(dot(h2, wg_ref[...], NT))[0] * dot(h2, wl_ref[...], NT)).astype(BF16)
        part[q] = dot(gated, wd_ref[...]).reshape(part.shape[2:])

    quarters = order(z, y)
    mlp_quarter(quarters[0])
    zy.send_away(0)
    yz.send_away(0)
    mlp_quarter(quarters[1])
    zy.send_away(1)
    mlp_quarter(quarters[2])
    yz.send_away(1)
    mlp_quarter(quarters[3])
    for s in streams:
        s.forward()
    for piece in range(2):
        rows = pl.ds(piece * 64, 64)
        for c, s in enumerate(streams):
            x1_ref[z, y, c, rows, :] = (a0_ref[z, y, c, rows, :].astype(F32) + s.total(piece)).astype(BF16)
            s.publish(piece)
    for s in streams:
        s.gather()
    for s in streams:
        s.close()
    saves.append(local(x1_ref, x1_out, ssem.at[3]))

    late = []
    for step in range(2):
        b = 1 - z if step == 0 else z
        for half in range(2):
            rows = pl.ds(half * 256, 256)
            for d_ref, value in zip((q_ref, k_ref, v_ref), project(1, x1_ref[b, half].reshape(256, -1))):
                d_ref[1, b, rows, :] = value
        attention(1, b)
        if step == 0:
            late += [ship(1, 'zy', b, 1 - y), ship(1, 'z', b, y)]
        else:
            late.append(ship(1, 'y', b, 1 - y))
    saves += [local(src, dst, ssem.at[4 + i]) for i, (src, dst) in enumerate([(q_ref, q_out), (k_ref, k_out), (v_ref, v_out), (o_ref, o_out)])]
    project_out(1, late, lambda c: x1_ref[z, y, c], a1_ref)
    saves.append(local(a1_ref, a1_out, ssem.at[8]))
    for copy in masks + xs + weights + passed + sent + late:
        copy.wait_send()
    for copy in moves + saves:
        copy.wait()


def forward(x_in, d_y, key_mask, gains_a, gains_m, w_q, w_k, w_v, w_o, wg_t, wl_t, w_out, bias_rows):
    batch, blk, width = x_in.shape
    seq, cols = 4 * blk, w_q.shape[2]
    dma = pltpu.SemaphoreType.DMA
    blocks = (2, 2, 2, blk, width)
    arrived = (2, 4, blk, width)
    heads = (2, 2, seq, cols)
    halves = (2, 2, 2, seq // 2, cols)
    hbm = [arrived, blocks, blocks, blocks, arrived, heads, heads, heads, halves]
    operands = [x_in.reshape(4, 2, blk, width), d_y.reshape(4, 2, blk, width), w_o, w_q, w_k, w_v, wg_t, wl_t, w_out,
                key_mask.reshape(4, 2, blk), gains_a, gains_m, bias_rows]
    scratch = [pltpu.VMEM(h, BF16) for h in hbm[:4] + [(2, blk, width)] + hbm[5:]]
    scratch += [pltpu.VMEM(w.shape, BF16) for w in (w_q, w_k, w_v)] + [pltpu.VMEM(w.shape[1:], BF16) for w in (wg_t, wl_t, w_out)]
    scratch += [pltpu.VMEM((2, 4) + w_o.shape[1:], BF16), pltpu.VMEM((bias_rows.shape[0], seq, seq), F32), pltpu.VMEM((2, 4, 2 * blk, cols), BF16)]
    scratch += sum_scratch(0, blocks[3:])
    scratch += [dma((15,)), dma((15,)), dma((6,)), dma((6,)), dma((6, 10)), dma((6, 10)), dma((10,)), dma((9,))]
    return pl.pallas_call(
        functools.partial(forward_kernel, seq),
        out_shape=[jax.ShapeDtypeStruct(h, BF16) for h in hbm] + [jax.ShapeDtypeStruct((4, 2, blk), jnp.int32), jax.ShapeDtypeStruct((bias_rows.shape[0], 2 * seq), F32)],
        in_specs=any_specs(9) + vmem_specs(4), out_specs=any_specs(9) + vmem_specs(2),
        scratch_shapes=scratch,
        compiler_params=pltpu.CompilerParams(collective_id=0, has_side_effects=True, vmem_limit_bytes=62 << 20),
        cost_estimate=pl.CostEstimate(flops=15 << 30, bytes_accessed=48 << 20, transcendentals=0),
        name="forward",
    )(*operands)


def backward_kernel(seq, *refs):
    refs = list(refs)
    take = lambda n: [refs.pop(0) for _ in range(n)]
    stacks = take(7)
    x1_all, dy_in, x_all, heads_all = take(2), refs.pop(0), take(2), take(4)
    ga_ref, gm_ref, t_ref, mask_ref = take(4)
    dx_ref, small_out = take(2)
    grad_out = take(7)
    weights, holds = take(7), take(7)
    lsem, part, near, far, dm_ref, h_ref, gated_ref, dgate_ref, dlin_ref = take(9)
    bias_ref, dt_ref = take(2)
    dq_ref, dk_ref = dgate_ref.at[:, :, 0:256], dgate_ref.at[:, :, 256:512]
    dv_ref, do_ref = dlin_ref.at[:, :, 0:256], dlin_ref.at[0, :, 256:512]
    grad_scratch = [take(4) for _ in range(7)]
    send, recv, gsend, grecv, kept, own_ref, acc_small, got_small, msend, mrecv, csend, crecv = refs
    wg_ref, wl_ref, wd_ref, wq_ref, wk_ref, wv_ref, wo_ref = weights
    x1_ref, dy_ref, x_ref, q_ref, k_ref, v_ref, o_ref = holds
    tp, cp, z, y, x, core, ids = place()
    heads = t_ref.shape[0]
    width = x_ref.shape[-1]
    quarters = order(z, y)
    p_out, p_gate, p_lin, p_o, p_q, p_k, p_v = [g[0] for g in grad_scratch]

    def fetch(layer, attention):
        if attention:
            pairs = [(x_all[layer], x_ref)] + [(h.at[layer], r) for h, r in zip(heads_all, (q_ref, k_ref, v_ref, o_ref))]
            pairs += [(w.at[layer], r) for w, r in zip(stacks[3:], weights[3:])]
        else:
            pairs = [(x1_all[layer], x1_ref)] + ([(dy_in, dy_ref)] if layer == 1 else []) + [(w.at[layer], r) for w, r in zip(stacks[:3], weights[:3])]
        copies = [pltpu.make_async_copy(src, dst, lsem.at[int(attention), layer, i]) for i, (src, dst) in enumerate(pairs)]
        for copy in copies:
            copy.start()
        return copies

    def mlp_quarter(q, gain, write_gated):
        h2 = norm(x1_ref[q].reshape(256, -1), gain)
        rows = pl.ds(pl.multiple_of((q[0] * 2 + q[1]) * 256, 256), 256)
        h_ref[rows, :] = h2
        value, slope = gelu_parts(dot(h2, wg_ref[...], NT))
        lin = dot(h2, wl_ref[...], NT)
        if write_gated:
            gated_ref[rows, :] = (value * lin).astype(BF16)
        d_gated = dot(dy_ref[q].reshape(256, -1), wd_ref[...], NT)
        d_lin = (d_gated * value).astype(BF16)
        d_gate = (d_gated * lin * slope).astype(BF16)
        in_batch = pl.ds(pl.multiple_of(q[1] * 256, 256), 256)
        dlin_ref[q[0], in_batch, :] = d_lin
        dgate_ref[q[0], in_batch, :] = d_gate
        part[q] = (dot(d_gate, wg_ref[...]) + dot(d_lin, wl_ref[...])).reshape(part.shape[2:])

    def attend(b, ready, fresh, hook):
        add = key_add(mask_ref, b)
        do_ref[...] = dot(dm_ref[b].reshape(seq, width), wo_ref[...], NT).astype(BF16)
        for head in range(heads):
            cols = pl.ds(head * HEAD, HEAD)
            q, k, v, do = q_ref[b, :, cols], k_ref[b, :, cols], v_ref[b, :, cols], do_ref[:, cols]
            if ready:
                p = bias_ref[head]
            else:
                bias_ref[head] = toeplitz(t_ref[head:head + 1, :], seq)
                e, total = exp_scores(q, k, bias_ref[head], add)
                p = e * (1.0 / total)
            row_dot = jnp.sum(do.astype(F32) * o_ref[b, :, cols].astype(F32), axis=-1, keepdims=True)
            ds = p * (dot(do, v, NT) - row_dot)
            sums = diag_sums(ds, seq)
            dt_ref[head:head + 1, :] = sums if fresh else dt_ref[head:head + 1, :] + sums
            dsl = ds.astype(BF16)
            dq_ref[b, :, cols] = dot(dsl, k).astype(BF16)
            dk_ref[b, :, cols] = dot(dsl, q, TN).astype(BF16)
            dv_ref[b, :, cols] = dot(p.astype(BF16), do, TN).astype(BF16)
            if head == 0:
                hook()

    loads = {(1, False): fetch(1, False), (1, True): fetch(1, True)}
    meet(ids, ['z', 'y', 'x', 'core', 'xc'])
    pending = []
    for layer in (1, 0):
        last = layer == 0
        deep = 32 if last else 128
        across = 128 // deep
        half = deep // 2
        g_out, g_gate, g_lin, g_o, g_q, g_k, g_v = grads = [
            GradStream(*grad_scratch[i], grad_out[i].at[layer], gsend.at[layer, i], grecv.at[layer, i], kept.at[layer, i], ids, x, core) for i in range(7)]
        zy, yz = mlp_sum = colours(part, near, far, lambda q, c, piece: dm_ref.at[q[0], q[1], c, pl.ds(piece * 64, 64)],
                                   send.at[layer, 0:2], recv.at[layer, 0:2], ids, z, y, 2)
        if not last:
            for copy in loads[layer, False]:
                copy.wait()
        gain, gain_a = gm_ref[layer:layer + 1, :], ga_ref[layer:layer + 1, :]
        mlp_quarter(quarters[0], gain, not last)
        zy.send_away(0)
        yz.send_away(0)
        if last:
            for g in pending[:1]:
                g.gather()
            grad_into(p_out, gated_ref[...], dy_ref[...].reshape(h_ref.shape))
            g_out.send_both()
        mlp_quarter(quarters[1], gain, not last)
        zy.send_away(1)
        mlp_quarter(quarters[2], gain, not last)
        yz.send_away(1)
        if last:
            g_out.forward()
        mlp_quarter(quarters[3], gain, not last)
        if not last:
            grad_into(p_out, gated_ref[...], dy_ref[...].reshape(h_ref.shape))
            g_out.send_both()
        grad_into(p_gate, dgate_ref[...].reshape(2 * seq, -1), h_ref)
        g_gate.send_both()
        if not last:
            g_out.forward()
        for s in mlp_sum:
            s.forward()
        for g in pending[1:]:
            g.gather()
        grad_into(p_lin, dlin_ref[...].reshape(2 * seq, -1), h_ref)
        g_lin.send_both()
        g_gate.forward()
        for copy in loads[layer, True]:
            copy.wait()
        for b in range(2):
            h_ref[b * seq:(b + 1) * seq, :] = norm(x_ref[b], gain_a)
        g_lin.forward()
        add = key_add(mask_ref, 1 - z)
        for head in range(heads):
            cols = pl.ds(head * HEAD, HEAD)
            bias_ref[head] = toeplitz(t_ref[head:head + 1, :], seq)
            e, total = exp_scores(q_ref[1 - z, :, cols], k_ref[1 - z, :, cols], bias_ref[head], add)
            bias_ref[head] = e * (1.0 / total)
        for g in pending:
            g.close()
        g_out.finish()
        dg_m = 0.0
        for piece in range(2):
            rows = pl.ds(piece * 64, 64)
            for c, s in enumerate(mlp_sum):
                d_x, dg = norm_back(s.total(piece), x1_ref[z, y, c, rows, :], gain)
                dm_ref[z, y, c, rows, :] = (d_x + dy_ref[z, y, c, rows, :].astype(F32)).astype(BF16)
                s.publish(piece)
                dg_m = dg_m + jnp.sum(dg, axis=0, keepdims=True)
        g_gate.finish()
        for s in mlp_sum:
            s.gather()
        for s in mlp_sum:
            s.close()
        if not last:
            loads[0, False] = fetch(0, False)

        if last:
            def region(q, c, piece):
                return dx_ref.at[:, q[0], q[1], c, pl.ds(piece * 16, 16)]
        else:
            def region(q, c, piece):
                return dy_ref.at[q[0], q[1], c, pl.ds(piece * 64, 64)]
        zy, yz = attn_sum = colours(part, near, far, region, send.at[layer, 2:4], recv.at[layer, 2:4], ids, z, y, 2)

        def pick(ref, offset, size, q):
            pieces = [ref[q[0], pl.ds(pl.multiple_of(j * 4 * deep + q[1] * 2 * deep + offset, half), size), :] for j in range(across)]
            return pieces[0] if across == 1 else jnp.concatenate(pieces, axis=0)

        def attn_quarter(q):
            total = sum(dot(pick(d, 0, 2 * deep, q), w[...], NT) for d, w in [(dq_ref, wq_ref), (dk_ref, wk_ref), (dv_ref, wv_ref)])
            total = total.reshape(across, 2, 2, half, width)
            for c in range(2):
                for piece in range(2):
                    part[q[0], q[1], c, pl.ds(piece * 64, 64), :] = total[:, c, piece].reshape(64, width)

        attend(1 - z, True, not last, lambda: None)
        attn_quarter(quarters[0])
        zy.send_away(0)
        yz.send_away(0)
        attn_quarter(quarters[1])
        zy.send_away(1)
        grad_into(p_o, o_ref[...].reshape(2 * seq, -1), dm_ref[...].reshape(2 * seq, width))
        g_o.send_both()
        g_lin.finish()
        g_out.gather()
        attend(z, False, False, g_o.forward)
        attn_quarter(quarters[2])
        yz.send_away(1)
        attn_quarter(quarters[3])
        for g, p, d in [(g_q, p_q, dq_ref), (g_k, p_k, dk_ref), (g_v, p_v, dv_ref)]:
            grad_into(p, h_ref[...], d[...].reshape(2 * seq, -1))
            g.send_both()
        for s in attn_sum:
            s.forward()
        for g in [g_q, g_k, g_v]:
            g.forward()
        if not last:
            for copy in loads[0, False]:
                copy.wait()
            for i in range(4):
                h2 = norm(x1_ref[i // 2, i % 2].reshape(256, -1), gm_ref[0:1, :])
                gated_ref[i * 256:(i + 1) * 256, :] = (gelu_parts(dot(h2, wg_ref[...], NT))[0] * dot(h2, wl_ref[...], NT)).astype(BF16)
        g_gate.gather()
        g_lin.gather()
        g_o.finish()
        dg_a = 0.0
        moves = {}
        for piece in range(2):
            for c, s in enumerate(attn_sum):
                rows = pl.ds(piece * half, half)
                d_x, dg = norm_back(s.total(piece), pick(x_ref, c * deep + piece * half, half, (z, y)), gain_a)
                dg_a = dg_a + jnp.sum(dg, axis=0, keepdims=True)
                if last:
                    at = pl.ds(pl.multiple_of(y * 2 * deep + c * deep + piece * half, half), half)
                    res = jnp.concatenate([dm_ref[z, j // 2, j % 2, at, :] for j in range(4)], axis=0)
                else:
                    res = dm_ref[z, y, c, rows, :]
                d_x = (d_x + res.astype(F32)).astype(BF16)
                if last:
                    own_ref[c, piece] = d_x.reshape(across, half, width)
                    dx_ref[cp, z, y, c, rows, :] = own_ref[c, piece, cp]
                    moves[c, piece] = [remote(own_ref.at[c, piece, ids[name]['cp']], dx_ref.at[cp, z, y, c, rows], msend.at[c, piece, i], mrecv.at[c, piece, i], ids[name])
                                       for i, name in enumerate(['x', 'xc', 'core'])]
                else:
                    dy_ref[z, y, c, rows, :] = d_x
                    s.publish(piece)
        acc_small[0, 2 - 2 * layer:3 - 2 * layer, :] = dg_a
        acc_small[0, 3 - 2 * layer:4 - 2 * layer, :] = dg_m
        if not last:
            loads[0, True] = fetch(0, True)
            for g in [g_q, g_k, g_v]:
                g.finish()
            for s in attn_sum:
                s.gather()
            for s in attn_sum + [g_out, g_gate, g_lin]:
                s.close()
            pending = [g_o, g_q, g_k, g_v]

    acc_small[0, 4:8, :] = jnp.zeros((4, width), F32)
    acc_small[0, 8:12, :] = dt_ref[0:4, :]
    acc_small[0, 12:16, :] = jnp.zeros((4, width), F32)
    smalls = []

    def small_start(i):
        rows = pl.ds(0, 16 if i < 2 else 8)
        smalls.append(remote(acc_small.at[i, rows], got_small.at[i, rows], csend.at[i], crecv.at[i], ids[['x', 'core', 'y', 'z'][i]]))

    def small_end(i):
        rows = pl.ds(0, 16 if i < 2 else 8)
        smalls[i].wait_recv()
        acc_small[i + 1, rows, :] = acc_small[i, rows, :] + got_small[i, rows, :]

    small_start(0)
    for piece in range(2):
        for c, s in enumerate(attn_sum):
            for copy in moves[c, piece]:
                copy.wait_recv()
            s.publish(piece)
    g_q.finish()
    small_end(0)
    small_start(1)
    g_k.finish()
    small_end(1)
    small_start(2)
    g_v.finish()
    for s in attn_sum:
        s.gather()
    small_end(2)
    small_start(3)
    for g in [g_o, g_q, g_k, g_v]:
        g.gather()
    small_end(3)
    small_out[0:8, :] = acc_small[4, 0:8, :]
    small_out[8:16, :] = acc_small[2, 8:16, :]
    for copy in smalls + sum(moves.values(), []):
        copy.wait_send()
    for s in attn_sum + grads:
        s.close()


def backward(x1s, dy, xs, heads, gains_a, gains_m, wg_t, wl_t, w_out, w_q, w_k, w_v, w_o, table, mask):
    seq, width, cols = 512, w_q.shape[1], w_q.shape[2]
    ff = w_out.shape[1]
    rows = 2 * seq
    dma = pltpu.SemaphoreType.DMA
    blocks = (2, 2, 2, 128, width)
    flat = (2, seq, width)
    stacks = [wg_t, wl_t, w_out, w_q, w_k, w_v, w_o]
    operands = stacks + [a.reshape(blocks) for a in x1s] + [dy.reshape(blocks)] + [a.reshape(flat) for a in xs]
    operands += [h.reshape(2, 2, seq, cols) for h in heads] + [gains_a, gains_m, table, mask]
    grads = [(ff // 4, width)] * 3 + [(cols // 4, width)] + [(width // 4, cols)] * 3
    out_shape = [jax.ShapeDtypeStruct((4, 2, 2, 2, 32, width), BF16), jax.ShapeDtypeStruct((16, width), F32)]
    out_shape += [jax.ShapeDtypeStruct((2, 4) + g, BF16) for g in grads]
    scratch = [pltpu.VMEM(w.shape[1:], BF16) for w in stacks]
    scratch += [pltpu.VMEM(blocks, BF16)] * 2 + [pltpu.VMEM(flat, BF16)] + [pltpu.VMEM((2, seq, cols), BF16)] * 4 + [dma((2, 2, 9))]
    scratch += sum_scratch(0, blocks[3:]) + [pltpu.VMEM(blocks, BF16), pltpu.VMEM((rows, width), BF16), pltpu.VMEM((rows, ff), BF16)] + [pltpu.VMEM((2, seq, ff), BF16)] * 2
    scratch += [pltpu.VMEM((table.shape[0], seq, seq), F32), pltpu.VMEM((8, 2 * seq), F32)]
    for g in grads:
        scratch += [pltpu.VMEM((4,) + g, F32), pltpu.VMEM((2,) + g, F32), pltpu.VMEM(g, F32), pltpu.VMEM(g, BF16)]
    scratch += [dma((2, 4, 10)), dma((2, 4, 10)), dma((2, 7, 6)), dma((2, 7, 6)), dma((2, 7))]
    scratch += [pltpu.VMEM((2, 2, 4, 16, width), BF16), pltpu.VMEM((5, 16, width), F32), pltpu.VMEM((4, 16, width), F32)]
    scratch += [dma((2, 2, 3)), dma((2, 2, 3)), dma((4,)), dma((4,))]
    return pl.pallas_call(
        functools.partial(backward_kernel, seq),
        out_shape=out_shape, in_specs=any_specs(16) + vmem_specs(4), out_specs=vmem_specs(2) + any_specs(7),
        scratch_shapes=scratch,
        compiler_params=pltpu.CompilerParams(collective_id=1, has_side_effects=True, vmem_limit_bytes=67043328),
        cost_estimate=pl.CostEstimate(flops=40 << 30, bytes_accessed=96 << 20, transcendentals=0),
        name="backward",
    )(*operands)


def finish_kernel(seq, *refs):
    refs = list(refs)
    n = (len(refs) - 6) // 3
    small_ref, ins = refs[0], refs[1:1 + n]
    outs, (ga_ref, gm_ref, bias_ref) = refs[1 + n:1 + 2 * n], refs[1 + 2 * n:4 + 2 * n]
    bufs, (rsem, wsem) = refs[4 + 2 * n:4 + 3 * n], refs[4 + 3 * n:6 + 3 * n]
    reads, writes = [], []
    for i in range(n):
        for h in range(2):
            reads.append(pltpu.make_async_copy(ins[i].at[h], bufs[i].at[h], rsem.at[i, h]))
            writes.append(pltpu.make_async_copy(bufs[i].at[h], outs[i].at[h], wsem.at[i, h]))
    for copy in reads:
        copy.start()
    ga_ref[0:1, :], ga_ref[1:2, :] = small_ref[2:3, :], small_ref[0:1, :]
    gm_ref[0:1, :], gm_ref[1:2, :] = small_ref[3:4, :], small_ref[1:2, :]
    shape = (32, 2 * seq)
    column = lax.broadcasted_iota(jnp.int32, shape, 1)
    hit = (rel_bucket(column - seq) == lax.broadcasted_iota(jnp.int32, shape, 0)) & (column > 0)
    bias_ref[...] = lax.dot_general(small_ref[8:16, :], jnp.where(hit, 1.0, 0.0).astype(F32), NT, precision=lax.Precision.HIGHEST, preferred_element_type=F32)
    for read, write in zip(reads, writes):
        read.wait()
        write.start()
    for copy in writes:
        copy.wait()


def finish(small, arrays):
    dma = pltpu.SemaphoreType.DMA
    n = len(arrays)
    shapes = [jax.ShapeDtypeStruct(a.shape, a.dtype) for a in arrays]
    outs = pl.pallas_call(
        functools.partial(finish_kernel, 512),
        out_shape=shapes + [jax.ShapeDtypeStruct((2, small.shape[1]), F32)] * 2 + [jax.ShapeDtypeStruct((8, 32), F32)],
        in_specs=vmem_specs(1) + any_specs(n), out_specs=any_specs(n) + vmem_specs(3),
        scratch_shapes=[pltpu.VMEM(a.shape, a.dtype) for a in arrays] + [dma((n, 2)), dma((n, 2))],
        compiler_params=pltpu.CompilerParams(vmem_limit_bytes=67043328),
        cost_estimate=pl.CostEstimate(flops=1 << 20, bytes_accessed=32 << 20, transcendentals=0),
        name="finish",
    )(small, *arrays)
    return outs[:n], outs[n], outs[n + 1], outs[n + 2][:4]


def vmem_specs(n):
    return [pl.BlockSpec(memory_space=pltpu.VMEM)] * n


def solution(mesh):
    seq_spec = P(None, 'cp', None)
    col_spec = P(None, None, 'tp')
    row_spec = P(None, 'tp', None)
    weight_specs = (P(), P(), col_spec, col_spec, col_spec, row_spec, col_spec, col_spec, row_spec)

    def local_program(x_in, d_y, key_mask, rel_bias, g_attn, g_mlp, w_q, w_k, w_v, w_o, w_gate, w_lin, w_out):
        width = x_in.shape[2]
        wg_t, wl_t = jnp.swapaxes(w_gate, 1, 2), jnp.swapaxes(w_lin, 1, 2)
        x0, a0, x1, a1, dy, q, k, v, o, mask, table = forward(x_in, d_y, key_mask, g_attn, g_mlp, w_q, w_k, w_v, w_o, wg_t, wl_t, w_out, rel_bias.T)

        outs = backward((a0, a1), dy, (x0, x1), (q, k, v, o), g_attn, g_mlp, wg_t, wl_t, w_out, w_q, w_k, w_v, w_o, table, mask)
        arrays = [outs[0].reshape((2, -1) + outs[0].shape[1:])] + list(outs[2:])
        moved, d_ga, d_gm, d_bias = finish(outs[1], arrays)
        d_x = moved[0]
        d_out, d_gate, d_lin, d_wo, d_wq, d_wk, d_wv = [g.reshape(2, -1, g.shape[-1]) for g in moved[1:]]
        d_gate, d_lin = jnp.swapaxes(d_gate, 1, 2), jnp.swapaxes(d_lin, 1, 2)
        d_bias = d_bias.T

        return d_x.reshape(x_in.shape), d_bias, d_ga, d_gm, d_wq, d_wk, d_wv, d_wo, d_gate, d_lin, d_out

    return jax.shard_map(local_program, mesh=mesh, in_specs=(seq_spec, seq_spec, P(None, 'cp'), P(None, 'tp')) + weight_specs, out_specs=(seq_spec, P(None, 'tp')) + weight_specs, check_vma=False)
```

```python
import functools
import jax
import jax.numpy as jnp
import numpy as np
from jax import lax
from jax.experimental import pallas as pl
from jax.experimental.pallas import tpu as pltpu
from jax.sharding import PartitionSpec as P

NORM_EPS = 1e-6
MASK_NEG = -1e9
HEAD = 64
PAIR, FOUR, BLOCK, ROWS, PIECE = 2, 4, 128, 256, 64
THREE, GRADS, EIGHT, SMALLS, MIB = 3, 7, 8, 16, 20
F32 = jnp.float32
BF16 = jnp.bfloat16
NT = (((1,), (1,)), ((), ()))
TN = (((0,), (0,)), ((), ()))


def rel_bucket(rel_pos):
    distance = jnp.minimum(jnp.abs(rel_pos), 128)
    distance_sq = distance * distance
    log_part = 8 + sum((distance_sq >= 64 * 2 ** power).astype(jnp.int32) for power in range(1, 8))
    return jnp.where(distance < 8, distance, log_part) + 16 * (rel_pos > 0).astype(jnp.int32)


def dot(a, b, dims=(((1,), (0,)), ((), ()))):
    return lax.dot_general(a, b, dims, preferred_element_type=F32)


def toeplitz(row, seq):
    base = pltpu.roll(row, seq, 1)
    rows = jnp.concatenate([base if i == 0 else pltpu.roll(base, i, 1) for i in range(8)], axis=0)
    size = 8
    while size < seq:
        rows = jnp.concatenate([rows, pltpu.roll(rows, size, 1)], axis=0)
        size *= 2
    return rows[:, :seq]


def diag_sums(mat, seq):
    wide = jnp.concatenate([mat, jnp.zeros_like(mat)], axis=1)
    size = seq
    while size > 1:
        half = size // 2
        wide = wide[:half] + pltpu.roll(wide[half:size], 2 * seq - half, 1)
        size = half
    return pltpu.roll(wide, seq, 1)


def place():
    tp, cp = lax.axis_index('tp'), lax.axis_index('cp')
    z, y = tp // PAIR, tp % PAIR
    x, core = cp // PAIR, cp % PAIR
    peers = {'z': (1 - z, y, x, core), 'y': (z, 1 - y, x, core), 'x': (z, y, 1 - x, core), 'core': (z, y, x, 1 - core),
             'zy': (1 - z, 1 - y, x, core), 'xc': (z, y, 1 - x, 1 - core)}
    ids = {name: {'tp': p[0] * PAIR + p[1], 'cp': p[PAIR] * PAIR + p[THREE]} for name, p in peers.items()}
    return tp, cp, z, y, x, core, ids


def meet(ids, names):
    barrier = pltpu.get_barrier_semaphore()
    for name in names:
        pl.semaphore_signal(barrier, inc=1, device_id=ids[name], device_id_type=pl.DeviceIdType.MESH)
    pl.semaphore_wait(barrier, len(names))


def remote(src, dst, send, recv, target):
    copy = pltpu.make_async_remote_copy(src_ref=src, dst_ref=dst, send_sem=send, recv_sem=recv,
                                        device_id=target, device_id_type=pl.DeviceIdType.MESH)
    copy.start()
    return copy


class Stream:
    def __init__(self, part, near, far, out, send, recv, first, second, a, b, index, pieces=1):
        self.part, self.near, self.far, self.out = part, near, far, out
        self.send, self.recv = send, recv
        self.first, self.second = first, second
        self.own, self.pass_on = index(a, b), index(a, 1 - b)
        self.away_far, self.away = index(1 - a, 1 - b), index(1 - a, b)
        self.pieces = pieces
        self.copies = {}
        self.arrived = False

    def start(self, name, piece, src, dst, target):
        slot = name if name < 2 else 2 + (name - 2) * self.pieces + piece
        self.copies[name, piece] = remote(src, dst, self.send.at[slot], self.recv.at[slot], target)

    def rows(self, ref, piece):
        if self.pieces == 1:
            return ref
        size = ref.shape[0] // self.pieces
        return ref.at[pl.ds(piece * size, size)]

    def send_away(self, slot):
        quarter = self.away_far if slot == 0 else self.away
        self.start(slot, 0, self.part(quarter), self.near.at[slot], self.first)

    def forward(self):
        self.copies[0, 0].wait_recv()
        for piece in range(self.pieces):
            ref = self.rows(self.part(self.pass_on), piece)
            ref[...] += self.rows(self.near.at[0], piece)[...]
            self.start(2, piece, ref, self.rows(self.far, piece), self.second)

    def total(self, piece=0):
        if not self.arrived:
            self.copies[1, 0].wait_recv()
            self.arrived = True
        self.copies[2, piece].wait_recv()
        return self.rows(self.part(self.own), piece)[...] + self.rows(self.near.at[1], piece)[...] + self.rows(self.far, piece)[...]

    def publish(self, piece=0):
        out = self.out(self.own, piece)
        self.start(3, piece, out, out, self.first)
        self.start(4, piece, out, out, self.second)

    def gather(self):
        for piece in range(self.pieces):
            self.copies[4, piece].wait_recv()
            out = self.out(self.pass_on, piece)
            self.start(5, piece, out, out, self.first)

    def close(self):
        for piece in range(self.pieces):
            self.copies[3, piece].wait_recv()
            self.copies[5, piece].wait_recv()
        for copy in self.copies.values():
            copy.wait_send()


def colours(part, near, far, out, send, recv, ids, z, y, pieces=1):
    def make(c, first, second, a, b, index):
        return Stream(lambda q: part.at[q[0], q[1], c], None if near is None else near.at[c], None if far is None else far.at[c],
                      lambda q, piece: out(q, c, piece), send.at[c], recv.at[c], ids[first], ids[second], a, b, index, pieces)
    return [make(0, 'z', 'y', z, y, lambda a, b: (a, b)), make(1, 'y', 'z', y, z, lambda a, b: (b, a))]


class GradStream(Stream):
    def __init__(self, part, near, far, own_ref, out, send, recv, local, ids, x, core):
        super().__init__(lambda q: part.at[q], near, far, lambda q, piece: out.at[q], send, recv,
                         ids['core'], ids['x'], core, x, lambda a, b: b * 2 + a)
        self.own_ref, self.local = own_ref, local

    def send_both(self):
        self.send_away(0)
        self.send_away(1)

    def finish(self):
        self.own_ref[...] = self.total().astype(BF16)
        out = self.out(self.own, 0)
        self.start(4, 0, self.own_ref, out, self.second)
        self.start(3, 0, self.own_ref, out, self.first)
        self.kept = pltpu.make_async_copy(self.own_ref, out, self.local)
        self.kept.start()

    def close(self):
        super().close()
        self.kept.wait()


def grad_into(part, a, b):
    quarter, width = part.shape[1], part.shape[2]
    for lo in range(0, width, 256):
        block = dot(a, b[:, lo:lo + 256], TN)
        for q in range(4):
            part[q, :, lo:lo + 256] = block[q * quarter:(q + 1) * quarter]


def norm_parts(rows):
    xf = rows.astype(F32)
    inv = lax.rsqrt(jnp.mean(xf * xf, axis=-1, keepdims=True) + NORM_EPS)
    return inv, xf * inv


def norm(rows, gain):
    return (norm_parts(rows)[1] * gain).astype(BF16)


def norm_back(d_norm, rows, gain):
    inv, normed = norm_parts(rows)
    d_normed = d_norm * gain
    return inv * (d_normed - normed * jnp.mean(d_normed * normed, axis=-1, keepdims=True)), d_norm * normed


def key_add(mask_ref, b):
    row = jnp.concatenate([mask_ref[j, pl.ds(b, 1), :] for j in range(4)], axis=1)
    return jnp.where(row > 0, 0.0, MASK_NEG).astype(F32)


def exp_scores(q, k, bias, add):
    s = dot(q, k, NT) + bias + add
    e = jnp.exp(s - jnp.max(s, axis=-1, keepdims=True))
    return e, jnp.sum(e, axis=-1, keepdims=True)


def any_specs(n):
    return [pl.BlockSpec(memory_space=pl.ANY)] * n


def gelu_parts(g):
    inner = np.float32(np.sqrt(2 / np.pi)) * (g + 0.044715 * (g * g * g))
    t = jnp.tanh(inner)
    cdf = 0.5 * (1.0 + t)
    slope = cdf + 0.5 * g * (1.0 - t * t) * np.float32(np.sqrt(2 / np.pi)) * (1.0 + 3 * 0.044715 * (g * g))
    return g * cdf, slope


def order(z, y):
    return [(1 - z, 1 - y), (1 - z, y), (z, 1 - y), (z, y)]


def sum_scratch(width, blocks=()):
    return [pltpu.VMEM((2, 2, 2) + blocks, F32), pltpu.VMEM((2, 2) + blocks, F32), pltpu.VMEM((2,) + blocks, F32)]


def forward_kernel(seq, *refs):
    refs = list(refs)
    take = lambda n: [refs.pop(0) for _ in range(n)]
    x_in, d_y, wo_in, wq_in, wk_in, wv_in, wg_in, wl_in, wd_in, mask_in, ga_ref, gm_ref, rb_ref = take(13)
    x0_out, a0_out, x1_out, a1_out, dy_out, q_out, k_out, v_out, o_out, mask_ref, t_ref = take(11)
    x0_ref, a0_ref, x1_ref, a1_ref, dyo_ref, q_ref, k_ref, v_ref, o_ref = take(9)
    wq_ref, wk_ref, wv_ref, wg_ref, wl_ref, wd_ref, wf_ref = take(GRADS)
    bias_ref, of_ref, part, near, far = take(5)
    xsend, xrecv, osend, orecv, send, recv, lsem, ssem = refs
    tp, cp, z, y, x, core, ids = place()
    near_by, far_by = ['core', 'x', 'xc'], ['z', 'y', 'zy']

    def local(src, dst, sem):
        copy = pltpu.make_async_copy(src, dst, sem)
        copy.start()
        return copy

    own_x = local(x_in.at[cp], x0_ref.at[:, cp], lsem.at[0])
    qkv_loads = [local(w, r, lsem.at[1 + i]) for i, (w, r) in enumerate([(wq_in, wq_ref), (wk_in, wk_ref), (wv_in, wv_ref)])]
    own_w = [local(wo_in.at[layer], wf_ref.at[layer, tp], lsem.at[FOUR + layer]) for layer in range(PAIR)]
    mlp_loads = [local(w.at[0], r, lsem.at[6 + i]) for i, (w, r) in enumerate([(wg_in, wg_ref), (wl_in, wl_ref), (wd_in, wd_ref)])]
    own_dy = local(d_y.at[cp], dyo_ref, lsem.at[9])
    meet(ids, near_by + far_by)
    masks, xs = [], []
    for i, name in enumerate(near_by):
        masks.append(remote(mask_in.at[ids[name]['cp']], mask_ref.at[cp], xsend.at[i], xrecv.at[i], ids[name]))
        xs.append(remote(x_in.at[ids[name]['cp']], x0_ref.at[:, cp], xsend.at[THREE + i], xrecv.at[THREE + i], ids[name]))
    weights = [remote(wo_in.at[core], wf_ref.at[core, tp], xsend.at[6 + i], xrecv.at[6 + i], ids[name]) for i, name in enumerate(far_by)]
    mask_ref[cp] = mask_in[cp]
    place_row = lax.broadcasted_iota(jnp.int32, (1, PAIR * seq), 1)
    bucket = rel_bucket(place_row - seq)
    for head in range(t_ref.shape[0]):
        row = jnp.zeros((1, PAIR * seq), F32)
        for j in range(32):
            row = jnp.where(bucket == j, rb_ref[head:head + 1, j:j + 1], row)
        t_ref[head:head + 1, :] = row
    for head in range(t_ref.shape[0]):
        bias_ref[head] = toeplitz(t_ref[head:head + 1, :], seq)

    def project(layer, rows):
        h = norm(rows, ga_ref[layer:layer + 1, :])
        return [dot(h, w[layer]).astype(BF16) for w in (wq_ref, wk_ref, wv_ref)]

    def attention(layer, b):
        add = key_add(mask_ref, b)
        for head in range(t_ref.shape[0]):
            cols = pl.ds(head * HEAD, HEAD)
            e, total = exp_scores(q_ref[layer, b, :, cols], k_ref[layer, b, :, cols], bias_ref[head], add)
            o = (dot(e.astype(BF16), v_ref[layer, b, :, cols]) / total).astype(BF16)
            o_ref[layer, b, 0, :, cols] = o[:seq // PAIR]
            o_ref[layer, b, 1, :, cols] = o[seq // PAIR:]

    def ship(layer, name, b, half):
        i = layer * THREE + far_by.index(name)
        return remote(o_ref.at[layer, b, half], of_ref.at[layer, tp], osend.at[i], orecv.at[i], ids[name])

    def project_out(layer, sent, residual, out_ref):
        of_ref[layer, tp] = o_ref[layer, z, y]
        for copy in sent:
            copy.wait_recv()
        streams = colours(None, None, None, lambda q, c, piece: out_ref.at[q[0], q[1], c], send.at[FOUR * layer:FOUR * layer + PAIR], recv.at[FOUR * layer:FOUR * layer + PAIR], ids, z, y)
        for c, s in enumerate(streams):
            rows = pl.ds(c * BLOCK, BLOCK)
            total = sum(dot(of_ref[layer, j, rows, :], wf_ref[layer, j]) for j in range(FOUR))
            out_ref[z, y, c] = (residual(c).astype(F32) + total).astype(BF16)
            s.publish()
        for s in streams:
            s.gather()
        for s in streams:
            s.close()

    for copy in qkv_loads:
        copy.wait()
    for i, name in enumerate(['own'] + near_by):
        if i == 0:
            own_x.wait()
            blk = cp
        else:
            xs[i - 1].wait_recv()
            blk = ids[name]['cp']
        for d_ref, value in zip((q_ref, k_ref, v_ref), project(0, x0_ref[:, blk].reshape(PAIR * BLOCK, -1))):
            for b in range(PAIR):
                d_ref[0, b, pl.ds(pl.multiple_of(blk * BLOCK, BLOCK), BLOCK), :] = value[b * BLOCK:(b + 1) * BLOCK]
    own_dy.wait()
    saves = [local(x0_ref, x0_out, ssem.at[0]), local(dyo_ref, dy_out.at[:, cp], ssem.at[1])]
    moves = [remote(d_y.at[ids[name]['cp']], dy_out.at[:, cp], xsend.at[12 + i], xrecv.at[12 + i], ids[name]) for i, name in enumerate(near_by)]
    for copy in masks:
        copy.wait_recv()
    attention(0, 1 - z)
    sent = [ship(0, 'zy', 1 - z, 1 - y), ship(0, 'z', 1 - z, y)]
    passed = []
    for i, name in enumerate(far_by):
        weights[i].wait_recv()
        got = wf_ref.at[core, ids[name]['tp']]
        passed.append(remote(got, got, xsend.at[9 + i], xrecv.at[9 + i], ids['core']))
    attention(0, z)
    sent.append(ship(0, 'y', z, 1 - y))
    for copy in own_w:
        copy.wait()
    for copy in passed:
        copy.wait_recv()
    project_out(0, sent, lambda c: x0_ref[z, y * PAIR + c], a0_ref)
    saves.append(local(a0_ref, a0_out, ssem.at[PAIR]))

    for copy in mlp_loads:
        copy.wait()
    zy, yz = streams = colours(part, near, far, lambda q, c, piece: x1_ref.at[q[0], q[1], c, pl.ds(piece * PIECE, PIECE)], send.at[PAIR:FOUR], recv.at[PAIR:FOUR], ids, z, y, PAIR)

    def mlp_quarter(q):
        h2 = norm(a0_ref[q].reshape(ROWS, -1), gm_ref[0:1, :])
        gated = (gelu_parts(dot(h2, wg_ref[...], NT))[0] * dot(h2, wl_ref[...], NT)).astype(BF16)
        part[q] = dot(gated, wd_ref[...]).reshape(part.shape[PAIR:])

    quarters = order(z, y)
    mlp_quarter(quarters[0])
    zy.send_away(0)
    yz.send_away(0)
    mlp_quarter(quarters[1])
    zy.send_away(1)
    mlp_quarter(quarters[PAIR])
    yz.send_away(1)
    mlp_quarter(quarters[THREE])
    for s in streams:
        s.forward()
    for piece in range(PAIR):
        rows = pl.ds(piece * PIECE, PIECE)
        for c, s in enumerate(streams):
            x1_ref[z, y, c, rows, :] = (a0_ref[z, y, c, rows, :].astype(F32) + s.total(piece)).astype(BF16)
            s.publish(piece)
    for s in streams:
        s.gather()
    for s in streams:
        s.close()
    saves.append(local(x1_ref, x1_out, ssem.at[THREE]))

    late = []
    for step in range(PAIR):
        b = 1 - z if step == 0 else z
        for half in range(PAIR):
            rows = pl.ds(half * ROWS, ROWS)
            for d_ref, value in zip((q_ref, k_ref, v_ref), project(1, x1_ref[b, half].reshape(ROWS, -1))):
                d_ref[1, b, rows, :] = value
        attention(1, b)
        if step == 0:
            late += [ship(1, 'zy', b, 1 - y), ship(1, 'z', b, y)]
        else:
            late.append(ship(1, 'y', b, 1 - y))
    saves += [local(src, dst, ssem.at[FOUR + i]) for i, (src, dst) in enumerate([(q_ref, q_out), (k_ref, k_out), (v_ref, v_out), (o_ref, o_out)])]
    project_out(1, late, lambda c: x1_ref[z, y, c], a1_ref)
    saves.append(local(a1_ref, a1_out, ssem.at[EIGHT]))
    for copy in masks + xs + weights + passed + sent + late:
        copy.wait_send()
    for copy in moves + saves:
        copy.wait()


def forward(x_in, d_y, key_mask, gains_a, gains_m, w_q, w_k, w_v, w_o, wg_t, wl_t, w_out, bias_rows):
    batch, blk, width = x_in.shape
    seq, cols = FOUR * blk, w_q.shape[PAIR]
    dma = pltpu.SemaphoreType.DMA
    blocks = (PAIR, PAIR, PAIR, blk, width)
    arrived = (PAIR, FOUR, blk, width)
    heads = (PAIR, PAIR, seq, cols)
    halves = (PAIR, PAIR, PAIR, seq // PAIR, cols)
    hbm = [arrived, blocks, blocks, blocks, arrived, heads, heads, heads, halves]
    operands = [x_in.reshape(FOUR, PAIR, blk, width), d_y.reshape(FOUR, PAIR, blk, width), w_o, w_q, w_k, w_v, wg_t, wl_t, w_out,
                key_mask.reshape(FOUR, PAIR, blk), gains_a, gains_m, bias_rows]
    scratch = [pltpu.VMEM(h, BF16) for h in hbm[:FOUR] + [(PAIR, blk, width)] + hbm[5:]]
    scratch += [pltpu.VMEM(w.shape, BF16) for w in (w_q, w_k, w_v)] + [pltpu.VMEM(w.shape[1:], BF16) for w in (wg_t, wl_t, w_out)]
    scratch += [pltpu.VMEM((PAIR, FOUR) + w_o.shape[1:], BF16), pltpu.VMEM((bias_rows.shape[0], seq, seq), F32), pltpu.VMEM((PAIR, FOUR, PAIR * blk, cols), BF16)]
    scratch += sum_scratch(0, blocks[THREE:])
    scratch += [dma((15,)), dma((15,)), dma((6,)), dma((6,)), dma((6, 10)), dma((6, 10)), dma((10,)), dma((9,))]
    return pl.pallas_call(
        functools.partial(forward_kernel, seq),
        out_shape=[jax.ShapeDtypeStruct(h, BF16) for h in hbm] + [jax.ShapeDtypeStruct((FOUR, PAIR, blk), jnp.int32), jax.ShapeDtypeStruct((bias_rows.shape[0], PAIR * seq), F32)],
        in_specs=any_specs(9) + vmem_specs(FOUR), out_specs=any_specs(9) + vmem_specs(PAIR),
        scratch_shapes=scratch,
        compiler_params=pltpu.CompilerParams(collective_id=0, has_side_effects=True, vmem_limit_bytes=62 << MIB),
        cost_estimate=pl.CostEstimate(flops=15 << 30, bytes_accessed=48 << MIB, transcendentals=0),
        name="forward",
    )(*operands)


def backward_kernel(seq, *refs):
    refs = list(refs)
    take = lambda n: [refs.pop(0) for _ in range(n)]
    stacks = take(GRADS)
    x1_all, dy_in, x_all, heads_all = take(PAIR), refs.pop(0), take(PAIR), take(FOUR)
    ga_ref, gm_ref, t_ref, mask_ref = take(FOUR)
    dx_ref, small_out = take(PAIR)
    grad_out = take(GRADS)
    weights, holds = take(GRADS), take(GRADS)
    lsem, part, near, far, dm_ref, h_ref, gated_ref, dgate_ref, dlin_ref = take(9)
    bias_ref, dt_ref = take(PAIR)
    dq_ref, dk_ref = dgate_ref.at[:, :, 0:ROWS], dgate_ref.at[:, :, ROWS:512]
    dv_ref, do_ref = dlin_ref.at[:, :, 0:ROWS], dlin_ref.at[0, :, ROWS:512]
    grad_scratch = [take(FOUR) for _ in range(GRADS)]
    send, recv, gsend, grecv, kept, own_ref, acc_small, got_small, msend, mrecv, csend, crecv = refs
    wg_ref, wl_ref, wd_ref, wq_ref, wk_ref, wv_ref, wo_ref = weights
    x1_ref, dy_ref, x_ref, q_ref, k_ref, v_ref, o_ref = holds
    tp, cp, z, y, x, core, ids = place()
    heads = t_ref.shape[0]
    width = x_ref.shape[-1]
    quarters = order(z, y)
    p_out, p_gate, p_lin, p_o, p_q, p_k, p_v = [g[0] for g in grad_scratch]

    def fetch(layer, attention):
        if attention:
            pairs = [(x_all[layer], x_ref)] + [(h.at[layer], r) for h, r in zip(heads_all, (q_ref, k_ref, v_ref, o_ref))]
            pairs += [(w.at[layer], r) for w, r in zip(stacks[THREE:], weights[THREE:])]
        else:
            pairs = [(x1_all[layer], x1_ref)] + ([(dy_in, dy_ref)] if layer == 1 else []) + [(w.at[layer], r) for w, r in zip(stacks[:THREE], weights[:THREE])]
        copies = [pltpu.make_async_copy(src, dst, lsem.at[int(attention), layer, i]) for i, (src, dst) in enumerate(pairs)]
        for copy in copies:
            copy.start()
        return copies

    def mlp_quarter(q, gain, write_gated):
        h2 = norm(x1_ref[q].reshape(ROWS, -1), gain)
        rows = pl.ds(pl.multiple_of((q[0] * PAIR + q[1]) * ROWS, ROWS), ROWS)
        h_ref[rows, :] = h2
        value, slope = gelu_parts(dot(h2, wg_ref[...], NT))
        lin = dot(h2, wl_ref[...], NT)
        if write_gated:
            gated_ref[rows, :] = (value * lin).astype(BF16)
        d_gated = dot(dy_ref[q].reshape(ROWS, -1), wd_ref[...], NT)
        d_lin = (d_gated * value).astype(BF16)
        d_gate = (d_gated * lin * slope).astype(BF16)
        in_batch = pl.ds(pl.multiple_of(q[1] * ROWS, ROWS), ROWS)
        dlin_ref[q[0], in_batch, :] = d_lin
        dgate_ref[q[0], in_batch, :] = d_gate
        part[q] = (dot(d_gate, wg_ref[...]) + dot(d_lin, wl_ref[...])).reshape(part.shape[PAIR:])

    def attend(b, ready, fresh, hook):
        add = key_add(mask_ref, b)
        do_ref[...] = dot(dm_ref[b].reshape(seq, width), wo_ref[...], NT).astype(BF16)
        for head in range(heads):
            cols = pl.ds(head * HEAD, HEAD)
            q, k, v, do = q_ref[b, :, cols], k_ref[b, :, cols], v_ref[b, :, cols], do_ref[:, cols]
            if ready:
                p = bias_ref[head]
            else:
                bias_ref[head] = toeplitz(t_ref[head:head + 1, :], seq)
                e, total = exp_scores(q, k, bias_ref[head], add)
                p = e * (1.0 / total)
            row_dot = jnp.sum(do.astype(F32) * o_ref[b, :, cols].astype(F32), axis=-1, keepdims=True)
            ds = p * (dot(do, v, NT) - row_dot)
            sums = diag_sums(ds, seq)
            dt_ref[head:head + 1, :] = sums if fresh else dt_ref[head:head + 1, :] + sums
            dsl = ds.astype(BF16)
            dq_ref[b, :, cols] = dot(dsl, k).astype(BF16)
            dk_ref[b, :, cols] = dot(dsl, q, TN).astype(BF16)
            dv_ref[b, :, cols] = dot(p.astype(BF16), do, TN).astype(BF16)
            if head == 0:
                hook()

    loads = {(1, False): fetch(1, False), (1, True): fetch(1, True)}
    meet(ids, ['z', 'y', 'x', 'core', 'xc'])
    pending = []
    for layer in (1, 0):
        last = layer == 0
        deep = 32 if last else BLOCK
        across = BLOCK // deep
        half = deep // PAIR
        g_out, g_gate, g_lin, g_o, g_q, g_k, g_v = grads = [
            GradStream(*grad_scratch[i], grad_out[i].at[layer], gsend.at[layer, i], grecv.at[layer, i], kept.at[layer, i], ids, x, core) for i in range(GRADS)]
        zy, yz = mlp_sum = colours(part, near, far, lambda q, c, piece: dm_ref.at[q[0], q[1], c, pl.ds(piece * PIECE, PIECE)],
                                   send.at[layer, 0:PAIR], recv.at[layer, 0:PAIR], ids, z, y, PAIR)
        if not last:
            for copy in loads[layer, False]:
                copy.wait()
        gain, gain_a = gm_ref[layer:layer + 1, :], ga_ref[layer:layer + 1, :]
        mlp_quarter(quarters[0], gain, not last)
        zy.send_away(0)
        yz.send_away(0)
        if last:
            for g in pending[:1]:
                g.gather()
            grad_into(p_out, gated_ref[...], dy_ref[...].reshape(h_ref.shape))
            g_out.send_both()
        mlp_quarter(quarters[1], gain, not last)
        zy.send_away(1)
        mlp_quarter(quarters[PAIR], gain, not last)
        yz.send_away(1)
        if last:
            g_out.forward()
        mlp_quarter(quarters[THREE], gain, not last)
        if not last:
            grad_into(p_out, gated_ref[...], dy_ref[...].reshape(h_ref.shape))
            g_out.send_both()
        grad_into(p_gate, dgate_ref[...].reshape(PAIR * seq, -1), h_ref)
        g_gate.send_both()
        if not last:
            g_out.forward()
        for s in mlp_sum:
            s.forward()
        for g in pending[1:]:
            g.gather()
        grad_into(p_lin, dlin_ref[...].reshape(PAIR * seq, -1), h_ref)
        g_lin.send_both()
        g_gate.forward()
        for copy in loads[layer, True]:
            copy.wait()
        for b in range(PAIR):
            h_ref[b * seq:(b + 1) * seq, :] = norm(x_ref[b], gain_a)
        g_lin.forward()
        add = key_add(mask_ref, 1 - z)
        for head in range(heads):
            cols = pl.ds(head * HEAD, HEAD)
            bias_ref[head] = toeplitz(t_ref[head:head + 1, :], seq)
            e, total = exp_scores(q_ref[1 - z, :, cols], k_ref[1 - z, :, cols], bias_ref[head], add)
            bias_ref[head] = e * (1.0 / total)
        for g in pending:
            g.close()
        g_out.finish()
        dg_m = 0.0
        for piece in range(PAIR):
            rows = pl.ds(piece * PIECE, PIECE)
            for c, s in enumerate(mlp_sum):
                d_x, dg = norm_back(s.total(piece), x1_ref[z, y, c, rows, :], gain)
                dm_ref[z, y, c, rows, :] = (d_x + dy_ref[z, y, c, rows, :].astype(F32)).astype(BF16)
                s.publish(piece)
                dg_m = dg_m + jnp.sum(dg, axis=0, keepdims=True)
        g_gate.finish()
        for s in mlp_sum:
            s.gather()
        for s in mlp_sum:
            s.close()
        if not last:
            loads[0, False] = fetch(0, False)

        if last:
            def region(q, c, piece):
                return dx_ref.at[:, q[0], q[1], c, pl.ds(piece * SMALLS, SMALLS)]
        else:
            def region(q, c, piece):
                return dy_ref.at[q[0], q[1], c, pl.ds(piece * PIECE, PIECE)]
        zy, yz = attn_sum = colours(part, near, far, region, send.at[layer, PAIR:FOUR], recv.at[layer, PAIR:FOUR], ids, z, y, PAIR)

        def pick(ref, offset, size, q):
            pieces = [ref[q[0], pl.ds(pl.multiple_of(j * FOUR * deep + q[1] * PAIR * deep + offset, half), size), :] for j in range(across)]
            return pieces[0] if across == 1 else jnp.concatenate(pieces, axis=0)

        def attn_quarter(q):
            total = sum(dot(pick(d, 0, PAIR * deep, q), w[...], NT) for d, w in [(dq_ref, wq_ref), (dk_ref, wk_ref), (dv_ref, wv_ref)])
            total = total.reshape(across, PAIR, PAIR, half, width)
            for c in range(PAIR):
                for piece in range(PAIR):
                    part[q[0], q[1], c, pl.ds(piece * PIECE, PIECE), :] = total[:, c, piece].reshape(PIECE, width)

        attend(1 - z, True, not last, lambda: None)
        attn_quarter(quarters[0])
        zy.send_away(0)
        yz.send_away(0)
        attn_quarter(quarters[1])
        zy.send_away(1)
        grad_into(p_o, o_ref[...].reshape(PAIR * seq, -1), dm_ref[...].reshape(PAIR * seq, width))
        g_o.send_both()
        g_lin.finish()
        g_out.gather()
        attend(z, False, False, g_o.forward)
        attn_quarter(quarters[PAIR])
        yz.send_away(1)
        attn_quarter(quarters[THREE])
        for g, p, d in [(g_q, p_q, dq_ref), (g_k, p_k, dk_ref), (g_v, p_v, dv_ref)]:
            grad_into(p, h_ref[...], d[...].reshape(PAIR * seq, -1))
            g.send_both()
        for s in attn_sum:
            s.forward()
        for g in [g_q, g_k, g_v]:
            g.forward()
        if not last:
            for copy in loads[0, False]:
                copy.wait()
            for i in range(FOUR):
                h2 = norm(x1_ref[i // PAIR, i % PAIR].reshape(ROWS, -1), gm_ref[0:1, :])
                gated_ref[i * ROWS:(i + 1) * ROWS, :] = (gelu_parts(dot(h2, wg_ref[...], NT))[0] * dot(h2, wl_ref[...], NT)).astype(BF16)
        g_gate.gather()
        g_lin.gather()
        g_o.finish()
        dg_a = 0.0
        moves = {}
        for piece in range(PAIR):
            for c, s in enumerate(attn_sum):
                rows = pl.ds(piece * half, half)
                d_x, dg = norm_back(s.total(piece), pick(x_ref, c * deep + piece * half, half, (z, y)), gain_a)
                dg_a = dg_a + jnp.sum(dg, axis=0, keepdims=True)
                if last:
                    at = pl.ds(pl.multiple_of(y * PAIR * deep + c * deep + piece * half, half), half)
                    res = jnp.concatenate([dm_ref[z, j // PAIR, j % PAIR, at, :] for j in range(FOUR)], axis=0)
                else:
                    res = dm_ref[z, y, c, rows, :]
                d_x = (d_x + res.astype(F32)).astype(BF16)
                if last:
                    own_ref[c, piece] = d_x.reshape(across, half, width)
                    dx_ref[cp, z, y, c, rows, :] = own_ref[c, piece, cp]
                    moves[c, piece] = [remote(own_ref.at[c, piece, ids[name]['cp']], dx_ref.at[cp, z, y, c, rows], msend.at[c, piece, i], mrecv.at[c, piece, i], ids[name])
                                       for i, name in enumerate(['x', 'xc', 'core'])]
                else:
                    dy_ref[z, y, c, rows, :] = d_x
                    s.publish(piece)
        acc_small[0, PAIR - PAIR * layer:THREE - PAIR * layer, :] = dg_a
        acc_small[0, THREE - PAIR * layer:FOUR - PAIR * layer, :] = dg_m
        if not last:
            loads[0, True] = fetch(0, True)
            for g in [g_q, g_k, g_v]:
                g.finish()
            for s in attn_sum:
                s.gather()
            for s in attn_sum + [g_out, g_gate, g_lin]:
                s.close()
            pending = [g_o, g_q, g_k, g_v]

    acc_small[0, FOUR:EIGHT, :] = jnp.zeros((FOUR, width), F32)
    acc_small[0, EIGHT:12, :] = dt_ref[0:FOUR, :]
    acc_small[0, 12:SMALLS, :] = jnp.zeros((FOUR, width), F32)
    smalls = []

    def small_start(i):
        rows = pl.ds(0, SMALLS if i < PAIR else EIGHT)
        smalls.append(remote(acc_small.at[i, rows], got_small.at[i, rows], csend.at[i], crecv.at[i], ids[['x', 'core', 'y', 'z'][i]]))

    def small_end(i):
        rows = pl.ds(0, SMALLS if i < PAIR else EIGHT)
        smalls[i].wait_recv()
        acc_small[i + 1, rows, :] = acc_small[i, rows, :] + got_small[i, rows, :]

    small_start(0)
    for piece in range(PAIR):
        for c, s in enumerate(attn_sum):
            for copy in moves[c, piece]:
                copy.wait_recv()
            s.publish(piece)
    g_q.finish()
    small_end(0)
    small_start(1)
    g_k.finish()
    small_end(1)
    small_start(PAIR)
    g_v.finish()
    for s in attn_sum:
        s.gather()
    small_end(PAIR)
    small_start(THREE)
    for g in [g_o, g_q, g_k, g_v]:
        g.gather()
    small_end(THREE)
    small_out[0:EIGHT, :] = acc_small[FOUR, 0:EIGHT, :]
    small_out[EIGHT:SMALLS, :] = acc_small[PAIR, EIGHT:SMALLS, :]
    for copy in smalls + sum(moves.values(), []):
        copy.wait_send()
    for s in attn_sum + grads:
        s.close()


def backward(x1s, dy, xs, heads, gains_a, gains_m, wg_t, wl_t, w_out, w_q, w_k, w_v, w_o, table, mask):
    seq, width, cols = 512, w_q.shape[1], w_q.shape[PAIR]
    ff = w_out.shape[1]
    rows = PAIR * seq
    dma = pltpu.SemaphoreType.DMA
    blocks = (PAIR, PAIR, PAIR, BLOCK, width)
    flat = (PAIR, seq, width)
    stacks = [wg_t, wl_t, w_out, w_q, w_k, w_v, w_o]
    operands = stacks + [a.reshape(blocks) for a in x1s] + [dy.reshape(blocks)] + [a.reshape(flat) for a in xs]
    operands += [h.reshape(PAIR, PAIR, seq, cols) for h in heads] + [gains_a, gains_m, table, mask]
    grads = [(ff // FOUR, width)] * THREE + [(cols // FOUR, width)] + [(width // FOUR, cols)] * THREE
    out_shape = [jax.ShapeDtypeStruct((FOUR, PAIR, PAIR, PAIR, 32, width), BF16), jax.ShapeDtypeStruct((SMALLS, width), F32)]
    out_shape += [jax.ShapeDtypeStruct((PAIR, FOUR) + g, BF16) for g in grads]
    scratch = [pltpu.VMEM(w.shape[1:], BF16) for w in stacks]
    scratch += [pltpu.VMEM(blocks, BF16)] * PAIR + [pltpu.VMEM(flat, BF16)] + [pltpu.VMEM((PAIR, seq, cols), BF16)] * FOUR + [dma((PAIR, PAIR, 9))]
    scratch += sum_scratch(0, blocks[THREE:]) + [pltpu.VMEM(blocks, BF16), pltpu.VMEM((rows, width), BF16), pltpu.VMEM((rows, ff), BF16)] + [pltpu.VMEM((PAIR, seq, ff), BF16)] * PAIR
    scratch += [pltpu.VMEM((table.shape[0], seq, seq), F32), pltpu.VMEM((EIGHT, PAIR * seq), F32)]
    for g in grads:
        scratch += [pltpu.VMEM((FOUR,) + g, F32), pltpu.VMEM((PAIR,) + g, F32), pltpu.VMEM(g, F32), pltpu.VMEM(g, BF16)]
    scratch += [dma((PAIR, FOUR, 10)), dma((PAIR, FOUR, 10)), dma((PAIR, GRADS, 6)), dma((PAIR, GRADS, 6)), dma((PAIR, GRADS))]
    scratch += [pltpu.VMEM((PAIR, PAIR, FOUR, SMALLS, width), BF16), pltpu.VMEM((5, SMALLS, width), F32), pltpu.VMEM((FOUR, SMALLS, width), F32)]
    scratch += [dma((PAIR, PAIR, THREE)), dma((PAIR, PAIR, THREE)), dma((FOUR,)), dma((FOUR,))]
    return pl.pallas_call(
        functools.partial(backward_kernel, seq),
        out_shape=out_shape, in_specs=any_specs(SMALLS) + vmem_specs(FOUR), out_specs=vmem_specs(PAIR) + any_specs(GRADS),
        scratch_shapes=scratch,
        compiler_params=pltpu.CompilerParams(collective_id=1, has_side_effects=True, vmem_limit_bytes=67043328),
        cost_estimate=pl.CostEstimate(flops=40 << 30, bytes_accessed=96 << MIB, transcendentals=0),
        name="backward",
    )(*operands)


def finish_kernel(seq, *refs):
    refs = list(refs)
    n = (len(refs) - 6) // THREE
    small_ref, ins = refs[0], refs[1:1 + n]
    outs, (ga_ref, gm_ref, bias_ref) = refs[1 + n:1 + PAIR * n], refs[1 + PAIR * n:FOUR + PAIR * n]
    bufs, (rsem, wsem) = refs[FOUR + PAIR * n:FOUR + THREE * n], refs[FOUR + THREE * n:6 + THREE * n]
    reads, writes = [], []
    for i in range(n):
        for h in range(PAIR):
            reads.append(pltpu.make_async_copy(ins[i].at[h], bufs[i].at[h], rsem.at[i, h]))
            writes.append(pltpu.make_async_copy(bufs[i].at[h], outs[i].at[h], wsem.at[i, h]))
    for copy in reads:
        copy.start()
    ga_ref[0:1, :], ga_ref[1:PAIR, :] = small_ref[PAIR:THREE, :], small_ref[0:1, :]
    gm_ref[0:1, :], gm_ref[1:PAIR, :] = small_ref[THREE:FOUR, :], small_ref[1:PAIR, :]
    shape = (32, PAIR * seq)
    column = lax.broadcasted_iota(jnp.int32, shape, 1)
    hit = (rel_bucket(column - seq) == lax.broadcasted_iota(jnp.int32, shape, 0)) & (column > 0)
    bias_ref[...] = lax.dot_general(small_ref[EIGHT:12, :], jnp.where(hit, 1.0, 0.0).astype(F32), NT, precision=lax.Precision.HIGHEST, preferred_element_type=F32)
    for read, write in zip(reads, writes):
        read.wait()
        write.start()
    for copy in writes:
        copy.wait()


def finish(small, arrays):
    dma = pltpu.SemaphoreType.DMA
    n = len(arrays)
    shapes = [jax.ShapeDtypeStruct(a.shape, a.dtype) for a in arrays]
    outs = pl.pallas_call(
        functools.partial(finish_kernel, 512),
        out_shape=shapes + [jax.ShapeDtypeStruct((PAIR, small.shape[1]), F32)] * PAIR + [jax.ShapeDtypeStruct((FOUR, 32), F32)],
        in_specs=vmem_specs(1) + any_specs(n), out_specs=any_specs(n) + vmem_specs(THREE),
        scratch_shapes=[pltpu.VMEM(a.shape, a.dtype) for a in arrays] + [dma((n, PAIR)), dma((n, PAIR))],
        compiler_params=pltpu.CompilerParams(vmem_limit_bytes=67043328),
        cost_estimate=pl.CostEstimate(flops=1 << MIB, bytes_accessed=32 << MIB, transcendentals=0),
        name="finish",
    )(small, *arrays)
    return outs[:n], *outs[n:]


def vmem_specs(n):
    return [pl.BlockSpec(memory_space=pltpu.VMEM)] * n


def solution(mesh):
    seq_spec = P(None, 'cp', None)
    col_spec = P(None, None, 'tp')
    row_spec = P(None, 'tp', None)
    weight_specs = (P(), P(), col_spec, col_spec, col_spec, row_spec, col_spec, col_spec, row_spec)

    def local_program(x_in, d_y, key_mask, rel_bias, g_attn, g_mlp, w_q, w_k, w_v, w_o, w_gate, w_lin, w_out):
        width = x_in.shape[2]
        wg_t, wl_t = jnp.swapaxes(w_gate, 1, 2), jnp.swapaxes(w_lin, 1, 2)
        x0, a0, x1, a1, dy, q, k, v, o, mask, table = forward(x_in, d_y, key_mask, g_attn, g_mlp, w_q, w_k, w_v, w_o, wg_t, wl_t, w_out, rel_bias.T)

        outs = backward((a0, a1), dy, (x0, x1), (q, k, v, o), g_attn, g_mlp, wg_t, wl_t, w_out, w_q, w_k, w_v, w_o, table, mask)
        arrays = [outs[0].reshape((2, -1) + outs[0].shape[1:])] + list(outs[2:])
        moved, d_ga, d_gm, d_bias = finish(outs[1], arrays)
        d_x = moved[0]
        d_out, d_gate, d_lin, d_wo, d_wq, d_wk, d_wv = [g.reshape(2, -1, g.shape[-1]) for g in moved[1:]]
        d_gate, d_lin = jnp.swapaxes(d_gate, 1, 2), jnp.swapaxes(d_lin, 1, 2)
        d_bias = d_bias.T

        return d_x.reshape(x_in.shape), d_bias, d_ga, d_gm, d_wq, d_wk, d_wv, d_wo, d_gate, d_lin, d_out

    return jax.shard_map(local_program, mesh=mesh, in_specs=(seq_spec, seq_spec, P(None, 'cp'), P(None, 'tp')) + weight_specs, out_specs=(seq_spec, P(None, 'tp')) + weight_specs, check_vma=False)
```

```python
import functools
import jax
import jax.numpy as jnp
import numpy as np
from jax import lax
from jax.experimental import pallas as pl
from jax.experimental.pallas import tpu as pltpu
from jax.sharding import PartitionSpec as P

NORM_EPS = 1e-6
MASK_NEG = -1e9
HEAD = 64
PAIR, FOUR, BLOCK, ROWS, PIECE = 2, 4, 128, 256, 64
THREE, GRADS, EIGHT, SMALLS, MIB = 3, 7, 8, 16, 20
F32 = jnp.float32
BF16 = jnp.bfloat16
NT = (((1,), (1,)), ((), ()))
TN = (((0,), (0,)), ((), ()))


def rel_bucket(rel_pos):
    distance = jnp.minimum(jnp.abs(rel_pos), 128)
    distance_sq = distance * distance
    log_part = 8 + sum((distance_sq >= 64 * 2 ** power).astype(jnp.int32) for power in range(1, 8))
    return jnp.where(distance < 8, distance, log_part) + 16 * (rel_pos > 0).astype(jnp.int32)


def dot(a, b, dims=(((1,), (0,)), ((), ()))):
    return lax.dot_general(a, b, dims, preferred_element_type=F32)


def toeplitz(row, seq):
    base = pltpu.roll(row, seq, 1)
    rows = jnp.concatenate([base if i == 0 else pltpu.roll(base, i, 1) for i in range(8)], axis=0)
    size = 8
    while size < seq:
        rows = jnp.concatenate([rows, pltpu.roll(rows, size, 1)], axis=0)
        size *= 2
    return rows[:, :seq]


def diag_sums(mat, seq):
    wide = jnp.concatenate([mat, jnp.zeros_like(mat)], axis=1)
    size = seq
    while size > 1:
        half = size // 2
        wide = wide[:half] + pltpu.roll(wide[half:size], 2 * seq - half, 1)
        size = half
    return pltpu.roll(wide, seq, 1)


def place():
    tp, cp = lax.axis_index('tp'), lax.axis_index('cp')
    z, y = tp // PAIR, tp % PAIR
    x, core = cp // PAIR, cp % PAIR
    peers = {'z': (1 - z, y, x, core), 'y': (z, 1 - y, x, core), 'x': (z, y, 1 - x, core), 'core': (z, y, x, 1 - core),
             'zy': (1 - z, 1 - y, x, core), 'xc': (z, y, 1 - x, 1 - core)}
    ids = {name: {'tp': p[0] * PAIR + p[1], 'cp': p[PAIR] * PAIR + p[THREE]} for name, p in peers.items()}
    return tp, cp, z, y, x, core, ids


def meet(ids, names):
    barrier = pltpu.get_barrier_semaphore()
    for name in names:
        pl.semaphore_signal(barrier, inc=1, device_id=ids[name], device_id_type=pl.DeviceIdType.MESH)
    pl.semaphore_wait(barrier, len(names))


def remote(src, dst, send, recv, target):
    copy = pltpu.make_async_remote_copy(src_ref=src, dst_ref=dst, send_sem=send, recv_sem=recv,
                                        device_id=target, device_id_type=pl.DeviceIdType.MESH)
    copy.start()
    return copy


class Stream:
    def __init__(self, part, near, far, out, send, recv, first, second, a, b, index, pieces=1):
        self.part, self.near, self.far, self.out = part, near, far, out
        self.send, self.recv = send, recv
        self.first, self.second = first, second
        self.own, self.pass_on = index(a, b), index(a, 1 - b)
        self.away_far, self.away = index(1 - a, 1 - b), index(1 - a, b)
        self.pieces = pieces
        self.copies = {}
        self.arrived = False

    def start(self, name, piece, src, dst, target):
        slot = name if name < 2 else 2 + (name - 2) * self.pieces + piece
        self.copies[name, piece] = remote(src, dst, self.send.at[slot], self.recv.at[slot], target)

    def rows(self, ref, piece):
        if self.pieces == 1:
            return ref
        size = ref.shape[0] // self.pieces
        return ref.at[pl.ds(piece * size, size)]

    def send_away(self, slot):
        quarter = self.away_far if slot == 0 else self.away
        self.start(slot, 0, self.part(quarter), self.near.at[slot], self.first)

    def forward(self):
        self.copies[0, 0].wait_recv()
        for piece in range(self.pieces):
            ref = self.rows(self.part(self.pass_on), piece)
            ref[...] += self.rows(self.near.at[0], piece)[...]
            self.start(2, piece, ref, self.rows(self.far, piece), self.second)

    def total(self, piece=0):
        if not self.arrived:
            self.copies[1, 0].wait_recv()
            self.arrived = True
        self.copies[2, piece].wait_recv()
        return self.rows(self.part(self.own), piece)[...] + self.rows(self.near.at[1], piece)[...] + self.rows(self.far, piece)[...]

    def publish(self, piece=0):
        out = self.out(self.own, piece)
        self.start(3, piece, out, out, self.first)
        self.start(4, piece, out, out, self.second)

    def gather(self):
        for piece in range(self.pieces):
            self.copies[4, piece].wait_recv()
            out = self.out(self.pass_on, piece)
            self.start(5, piece, out, out, self.first)

    def close(self):
        for piece in range(self.pieces):
            self.copies[3, piece].wait_recv()
            self.copies[5, piece].wait_recv()
        for copy in self.copies.values():
            copy.wait_send()


def colours(part, near, far, out, send, recv, ids, z, y, pieces=1):
    def make(c, first, second, a, b, index):
        return Stream(lambda q: part.at[q[0], q[1], c], None if near is None else near.at[c], None if far is None else far.at[c],
                      lambda q, piece: out(q, c, piece), send.at[c], recv.at[c], ids[first], ids[second], a, b, index, pieces)
    return [make(0, 'z', 'y', z, y, lambda a, b: (a, b)), make(1, 'y', 'z', y, z, lambda a, b: (b, a))]


class GradStream(Stream):
    def __init__(self, part, near, far, own_ref, out, send, recv, local, ids, x, core):
        super().__init__(lambda q: part.at[q], near, far, lambda q, piece: out.at[q], send, recv,
                         ids['core'], ids['x'], core, x, lambda a, b: b * 2 + a)
        self.own_ref, self.local = own_ref, local

    def send_both(self):
        self.send_away(0)
        self.send_away(1)

    def finish(self):
        self.own_ref[...] = self.total().astype(BF16)
        out = self.out(self.own, 0)
        self.start(4, 0, self.own_ref, out, self.second)
        self.start(3, 0, self.own_ref, out, self.first)
        self.kept = pltpu.make_async_copy(self.own_ref, out, self.local)
        self.kept.start()

    def close(self):
        super().close()
        self.kept.wait()


def grad_into(part, a, b):
    quarter, width = part.shape[1], part.shape[2]
    for lo in range(0, width, 256):
        block = dot(a, b[:, lo:lo + 256], TN)
        for q in range(4):
            part[q, :, lo:lo + 256] = block[q * quarter:(q + 1) * quarter]


def norm_parts(rows):
    xf = rows.astype(F32)
    inv = lax.rsqrt(jnp.mean(xf * xf, axis=-1, keepdims=True) + NORM_EPS)
    return inv, xf * inv


def norm(rows, gain):
    return (norm_parts(rows)[1] * gain).astype(BF16)


def norm_back(d_norm, rows, gain):
    inv, normed = norm_parts(rows)
    d_normed = d_norm * gain
    return inv * (d_normed - normed * jnp.mean(d_normed * normed, axis=-1, keepdims=True)), d_norm * normed


def key_add(mask_ref, b):
    row = jnp.concatenate([mask_ref[j, pl.ds(b, 1), :] for j in range(4)], axis=1)
    return jnp.where(row > 0, 0.0, MASK_NEG).astype(F32)


def exp_scores(q, k, bias, add):
    s = dot(q, k, NT) + bias + add
    e = jnp.exp(s - jnp.max(s, axis=-1, keepdims=True))
    return e, jnp.sum(e, axis=-1, keepdims=True)


def any_specs(n):
    return [pl.BlockSpec(memory_space=pl.ANY)] * n


def gelu_parts(g):
    inner = np.float32(np.sqrt(2 / np.pi)) * (g + 0.044715 * (g * g * g))
    t = jnp.tanh(inner)
    cdf = 0.5 * (1.0 + t)
    slope = cdf + 0.5 * g * (1.0 - t * t) * np.float32(np.sqrt(2 / np.pi)) * (1.0 + 3 * 0.044715 * (g * g))
    return g * cdf, slope


def order(z, y):
    return [(1 - z, 1 - y), (1 - z, y), (z, 1 - y), (z, y)]


def sum_scratch(width, blocks=()):
    return [pltpu.VMEM((2, 2, 2) + blocks, F32), pltpu.VMEM((2, 2) + blocks, F32), pltpu.VMEM((2,) + blocks, F32)]


def forward_kernel(seq, *refs):
    refs = list(refs)
    take = lambda n: [refs.pop(0) for _ in range(n)]
    x_in, d_y, wo_in, wq_in, wk_in, wv_in, wg_in, wl_in, wd_in, mask_in, ga_ref, gm_ref, rb_ref = take(13)
    x0_out, a0_out, x1_out, a1_out, dy_out, q_out, k_out, v_out, o_out, mask_ref, t_ref = take(11)
    x0_ref, a0_ref, x1_ref, a1_ref, dyo_ref, q_ref, k_ref, v_ref, o_ref = take(9)
    wq_ref, wk_ref, wv_ref, wg_ref, wl_ref, wd_ref, wf_ref = take(GRADS)
    bias_ref, of_ref, part, near, far = take(5)
    xsend, xrecv, osend, orecv, send, recv, lsem, ssem = refs
    tp, cp, z, y, x, core, ids = place()
    near_by, far_by = ['core', 'x', 'xc'], ['z', 'y', 'zy']

    def local(src, dst, sem):
        copy = pltpu.make_async_copy(src, dst, sem)
        copy.start()
        return copy

    own_x = local(x_in.at[cp], x0_ref.at[:, cp], lsem.at[0])
    qkv_loads = [local(w, r, lsem.at[1 + i]) for i, (w, r) in enumerate([(wq_in, wq_ref), (wk_in, wk_ref), (wv_in, wv_ref)])]
    own_w = [local(wo_in.at[layer], wf_ref.at[layer, tp], lsem.at[FOUR + layer]) for layer in range(PAIR)]
    mlp_loads = [local(w.at[0], r, lsem.at[6 + i]) for i, (w, r) in enumerate([(wg_in, wg_ref), (wl_in, wl_ref), (wd_in, wd_ref)])]
    own_dy = local(d_y.at[cp], dyo_ref, lsem.at[9])
    meet(ids, near_by + far_by)
    masks, xs = [], []
    for i, name in enumerate(near_by):
        masks.append(remote(mask_in.at[ids[name]['cp']], mask_ref.at[cp], xsend.at[i], xrecv.at[i], ids[name]))
        xs.append(remote(x_in.at[ids[name]['cp']], x0_ref.at[:, cp], xsend.at[THREE + i], xrecv.at[THREE + i], ids[name]))
    weights = [remote(wo_in.at[core], wf_ref.at[core, tp], xsend.at[6 + i], xrecv.at[6 + i], ids[name]) for i, name in enumerate(far_by)]
    mask_ref[cp] = mask_in[cp]
    place_row = lax.broadcasted_iota(jnp.int32, (1, PAIR * seq), 1)
    bucket = rel_bucket(place_row - seq)
    for head in range(t_ref.shape[0]):
        row = jnp.zeros((1, PAIR * seq), F32)
        for j in range(32):
            row = jnp.where(bucket == j, rb_ref[head:head + 1, j:j + 1], row)
        t_ref[head:head + 1, :] = row
    for head in range(t_ref.shape[0]):
        bias_ref[head] = toeplitz(t_ref[head:head + 1, :], seq)

    def project(layer, rows):
        h = norm(rows, ga_ref[layer:layer + 1, :])
        return [dot(h, w[layer]).astype(BF16) for w in (wq_ref, wk_ref, wv_ref)]

    def attention(layer, b):
        add = key_add(mask_ref, b)
        for head in range(t_ref.shape[0]):
            cols = pl.ds(head * HEAD, HEAD)
            e, total = exp_scores(q_ref[layer, b, :, cols], k_ref[layer, b, :, cols], bias_ref[head], add)
            o = (dot(e.astype(BF16), v_ref[layer, b, :, cols]) / total).astype(BF16)
            o_ref[layer, b, 0, :, cols] = o[:seq // PAIR]
            o_ref[layer, b, 1, :, cols] = o[seq // PAIR:]

    def ship(layer, name, b, half):
        i = layer * THREE + far_by.index(name)
        return remote(o_ref.at[layer, b, half], of_ref.at[layer, tp], osend.at[i], orecv.at[i], ids[name])

    def project_out(layer, sent, residual, out_ref):
        of_ref[layer, tp] = o_ref[layer, z, y]
        for copy in sent:
            copy.wait_recv()
        streams = colours(None, None, None, lambda q, c, piece: out_ref.at[q[0], q[1], c], send.at[FOUR * layer:FOUR * layer + PAIR], recv.at[FOUR * layer:FOUR * layer + PAIR], ids, z, y)
        for c, s in enumerate(streams):
            rows = pl.ds(c * BLOCK, BLOCK)
            total = sum(dot(of_ref[layer, j, rows, :], wf_ref[layer, j]) for j in range(FOUR))
            out_ref[z, y, c] = (residual(c).astype(F32) + total).astype(BF16)
            s.publish()
        for s in streams:
            s.gather()
        for s in streams:
            s.close()

    for copy in qkv_loads:
        copy.wait()
    for i, name in enumerate(['own'] + near_by):
        if i == 0:
            own_x.wait()
            blk = cp
        else:
            xs[i - 1].wait_recv()
            blk = ids[name]['cp']
        for d_ref, value in zip((q_ref, k_ref, v_ref), project(0, x0_ref[:, blk].reshape(PAIR * BLOCK, -1))):
            for b in range(PAIR):
                d_ref[0, b, pl.ds(pl.multiple_of(blk * BLOCK, BLOCK), BLOCK), :] = value[b * BLOCK:(b + 1) * BLOCK]
    own_dy.wait()
    saves = [local(x0_ref, x0_out, ssem.at[0]), local(dyo_ref, dy_out.at[:, cp], ssem.at[1])]
    moves = [remote(d_y.at[ids[name]['cp']], dy_out.at[:, cp], xsend.at[12 + i], xrecv.at[12 + i], ids[name]) for i, name in enumerate(near_by)]
    for copy in masks:
        copy.wait_recv()
    attention(0, 1 - z)
    sent = [ship(0, 'zy', 1 - z, 1 - y), ship(0, 'z', 1 - z, y)]
    passed = []
    for i, name in enumerate(far_by):
        weights[i].wait_recv()
        got = wf_ref.at[core, ids[name]['tp']]
        passed.append(remote(got, got, xsend.at[9 + i], xrecv.at[9 + i], ids['core']))
    attention(0, z)
    sent.append(ship(0, 'y', z, 1 - y))
    for copy in own_w:
        copy.wait()
    for copy in passed:
        copy.wait_recv()
    project_out(0, sent, lambda c: x0_ref[z, y * PAIR + c], a0_ref)
    saves.append(local(a0_ref, a0_out, ssem.at[PAIR]))

    for copy in mlp_loads:
        copy.wait()
    zy, yz = streams = colours(part, near, far, lambda q, c, piece: x1_ref.at[q[0], q[1], c, pl.ds(piece * PIECE, PIECE)], send.at[PAIR:FOUR], recv.at[PAIR:FOUR], ids, z, y, PAIR)

    def mlp_quarter(q):
        h2 = norm(a0_ref[q].reshape(ROWS, -1), gm_ref[0:1, :])
        gated = (gelu_parts(dot(h2, wg_ref[...], NT))[0] * dot(h2, wl_ref[...], NT)).astype(BF16)
        part[q] = dot(gated, wd_ref[...]).reshape(part.shape[PAIR:])

    quarters = order(z, y)
    mlp_quarter(quarters[0])
    zy.send_away(0)
    yz.send_away(0)
    mlp_quarter(quarters[1])
    zy.send_away(1)
    mlp_quarter(quarters[PAIR])
    yz.send_away(1)
    mlp_quarter(quarters[THREE])
    for s in streams:
        s.forward()
    for piece in range(PAIR):
        rows = pl.ds(piece * PIECE, PIECE)
        for c, s in enumerate(streams):
            x1_ref[z, y, c, rows, :] = (a0_ref[z, y, c, rows, :].astype(F32) + s.total(piece)).astype(BF16)
            s.publish(piece)
    for s in streams:
        s.gather()
    for s in streams:
        s.close()
    saves.append(local(x1_ref, x1_out, ssem.at[THREE]))

    late = []
    for step in range(PAIR):
        b = 1 - z if step == 0 else z
        for half in range(PAIR):
            rows = pl.ds(half * ROWS, ROWS)
            for d_ref, value in zip((q_ref, k_ref, v_ref), project(1, x1_ref[b, half].reshape(ROWS, -1))):
                d_ref[1, b, rows, :] = value
        attention(1, b)
        if step == 0:
            late += [ship(1, 'zy', b, 1 - y), ship(1, 'z', b, y)]
        else:
            late.append(ship(1, 'y', b, 1 - y))
    saves += [local(src, dst, ssem.at[FOUR + i]) for i, (src, dst) in enumerate([(q_ref, q_out), (k_ref, k_out), (v_ref, v_out), (o_ref, o_out)])]
    project_out(1, late, lambda c: x1_ref[z, y, c], a1_ref)
    saves.append(local(a1_ref, a1_out, ssem.at[EIGHT]))
    for copy in masks + xs + weights + passed + sent + late:
        copy.wait_send()
    for copy in moves + saves:
        copy.wait()


def forward(x_in, d_y, key_mask, gains_a, gains_m, w_q, w_k, w_v, w_o, wg_t, wl_t, w_out, bias_rows):
    batch, blk, width = x_in.shape
    seq, cols = FOUR * blk, w_q.shape[PAIR]
    dma = pltpu.SemaphoreType.DMA
    blocks = (PAIR, PAIR, PAIR, blk, width)
    arrived = (PAIR, FOUR, blk, width)
    heads = (PAIR, PAIR, seq, cols)
    halves = (PAIR, PAIR, PAIR, seq // PAIR, cols)
    hbm = [arrived, blocks, blocks, blocks, arrived, heads, heads, heads, halves]
    operands = [x_in.reshape(FOUR, PAIR, blk, width), d_y.reshape(FOUR, PAIR, blk, width), w_o, w_q, w_k, w_v, wg_t, wl_t, w_out,
                key_mask.reshape(FOUR, PAIR, blk), gains_a, gains_m, bias_rows]
    scratch = [pltpu.VMEM(h, BF16) for h in hbm[:FOUR] + [(PAIR, blk, width)] + hbm[5:]]
    scratch += [pltpu.VMEM(w.shape, BF16) for w in (w_q, w_k, w_v)] + [pltpu.VMEM(w.shape[1:], BF16) for w in (wg_t, wl_t, w_out)]
    scratch += [pltpu.VMEM((PAIR, FOUR) + w_o.shape[1:], BF16), pltpu.VMEM((bias_rows.shape[0], seq, seq), F32), pltpu.VMEM((PAIR, FOUR, PAIR * blk, cols), BF16)]
    scratch += sum_scratch(0, blocks[THREE:])
    scratch += [dma((15,)), dma((15,)), dma((6,)), dma((6,)), dma((6, 10)), dma((6, 10)), dma((10,)), dma((9,))]
    return pl.pallas_call(
        functools.partial(forward_kernel, seq),
        out_shape=[jax.ShapeDtypeStruct(h, BF16) for h in hbm] + [jax.ShapeDtypeStruct((FOUR, PAIR, blk), jnp.int32), jax.ShapeDtypeStruct((bias_rows.shape[0], PAIR * seq), F32)],
        in_specs=any_specs(9) + vmem_specs(FOUR), out_specs=any_specs(9) + vmem_specs(PAIR),
        scratch_shapes=scratch,
        compiler_params=pltpu.CompilerParams(collective_id=0, has_side_effects=True, vmem_limit_bytes=62 << MIB),
        cost_estimate=pl.CostEstimate(flops=15 << 30, bytes_accessed=48 << MIB, transcendentals=0),
        name="forward",
    )(*operands)


def backward_kernel(seq, *refs):
    refs = list(refs)
    take = lambda n: [refs.pop(0) for _ in range(n)]
    stacks = take(GRADS)
    x1_all, dy_in, x_all, heads_all = take(PAIR), refs.pop(0), take(PAIR), take(FOUR)
    ga_ref, gm_ref, t_ref, mask_ref = take(FOUR)
    dx_ref, small_out = take(PAIR)
    grad_out = take(GRADS)
    weights, holds = take(GRADS), take(GRADS)
    lsem, part, near, far, dm_ref, h_ref, gated_ref, dgate_ref, dlin_ref = take(9)
    bias_ref, dt_ref = take(PAIR)
    dq_ref, dk_ref = dgate_ref.at[:, :, 0:ROWS], dgate_ref.at[:, :, ROWS:512]
    dv_ref, do_ref = dlin_ref.at[:, :, 0:ROWS], dlin_ref.at[0, :, ROWS:512]
    grad_scratch = [take(FOUR) for _ in range(GRADS)]
    send, recv, gsend, grecv, kept, own_ref, acc_small, got_small, msend, mrecv, csend, crecv = refs
    wg_ref, wl_ref, wd_ref, wq_ref, wk_ref, wv_ref, wo_ref = weights
    x1_ref, dy_ref, x_ref, q_ref, k_ref, v_ref, o_ref = holds
    tp, cp, z, y, x, core, ids = place()
    heads = t_ref.shape[0]
    width = x_ref.shape[-1]
    quarters = order(z, y)
    p_out, p_gate, p_lin, p_o, p_q, p_k, p_v = [g[0] for g in grad_scratch]

    def fetch(layer, attention):
        if attention:
            pairs = [(x_all[layer], x_ref)] + [(h.at[layer], r) for h, r in zip(heads_all, (q_ref, k_ref, v_ref, o_ref))]
            pairs += [(w.at[layer], r) for w, r in zip(stacks[THREE:], weights[THREE:])]
        else:
            pairs = [(x1_all[layer], x1_ref)] + ([(dy_in, dy_ref)] if layer == 1 else []) + [(w.at[layer], r) for w, r in zip(stacks[:THREE], weights[:THREE])]
        copies = [pltpu.make_async_copy(src, dst, lsem.at[int(attention), layer, i]) for i, (src, dst) in enumerate(pairs)]
        for copy in copies:
            copy.start()
        return copies

    def mlp_quarter(q, gain, write_gated):
        h2 = norm(x1_ref[q].reshape(ROWS, -1), gain)
        rows = pl.ds(pl.multiple_of((q[0] * PAIR + q[1]) * ROWS, ROWS), ROWS)
        h_ref[rows, :] = h2
        value, slope = gelu_parts(dot(h2, wg_ref[...], NT))
        lin = dot(h2, wl_ref[...], NT)
        if write_gated:
            gated_ref[rows, :] = (value * lin).astype(BF16)
        d_gated = dot(dy_ref[q].reshape(ROWS, -1), wd_ref[...], NT)
        d_lin = (d_gated * value).astype(BF16)
        d_gate = (d_gated * lin * slope).astype(BF16)
        in_batch = pl.ds(pl.multiple_of(q[1] * ROWS, ROWS), ROWS)
        dlin_ref[q[0], in_batch, :] = d_lin
        dgate_ref[q[0], in_batch, :] = d_gate
        part[q] = (dot(d_gate, wg_ref[...]) + dot(d_lin, wl_ref[...])).reshape(part.shape[PAIR:])

    def attend(b, ready, fresh, hook):
        add = key_add(mask_ref, b)
        do_ref[...] = dot(dm_ref[b].reshape(seq, width), wo_ref[...], NT).astype(BF16)
        for head in range(heads):
            cols = pl.ds(head * HEAD, HEAD)
            q, k, v, do = q_ref[b, :, cols], k_ref[b, :, cols], v_ref[b, :, cols], do_ref[:, cols]
            if ready:
                p = bias_ref[head]
            else:
                bias_ref[head] = toeplitz(t_ref[head:head + 1, :], seq)
                e, total = exp_scores(q, k, bias_ref[head], add)
                p = e * (1.0 / total)
            row_dot = jnp.sum(do.astype(F32) * o_ref[b, :, cols].astype(F32), axis=-1, keepdims=True)
            ds = p * (dot(do, v, NT) - row_dot)
            sums = diag_sums(ds, seq)
            dt_ref[head:head + 1, :] = sums if fresh else dt_ref[head:head + 1, :] + sums
            dsl = ds.astype(BF16)
            dq_ref[b, :, cols] = dot(dsl, k).astype(BF16)
            dk_ref[b, :, cols] = dot(dsl, q, TN).astype(BF16)
            dv_ref[b, :, cols] = dot(p.astype(BF16), do, TN).astype(BF16)
            if head == 0:
                hook()

    loads = {(1, False): fetch(1, False), (1, True): fetch(1, True)}
    meet(ids, ['z', 'y', 'x', 'core', 'xc'])
    pending = []
    for layer in (1, 0):
        last = layer == 0
        deep = 32 if last else BLOCK
        across = BLOCK // deep
        half = deep // PAIR
        g_out, g_gate, g_lin, g_o, g_q, g_k, g_v = grads = [
            GradStream(*grad_scratch[i], grad_out[i].at[layer], gsend.at[layer, i], grecv.at[layer, i], kept.at[layer, i], ids, x, core) for i in range(GRADS)]
        zy, yz = mlp_sum = colours(part, near, far, lambda q, c, piece: dm_ref.at[q[0], q[1], c, pl.ds(piece * PIECE, PIECE)],
                                   send.at[layer, 0:PAIR], recv.at[layer, 0:PAIR], ids, z, y, PAIR)
        if not last:
            for copy in loads[layer, False]:
                copy.wait()
        gain, gain_a = gm_ref[layer:layer + 1, :], ga_ref[layer:layer + 1, :]
        mlp_quarter(quarters[0], gain, not last)
        zy.send_away(0)
        yz.send_away(0)
        if last:
            for g in pending[:1]:
                g.gather()
            grad_into(p_out, gated_ref[...], dy_ref[...].reshape(h_ref.shape))
            g_out.send_both()
        mlp_quarter(quarters[1], gain, not last)
        zy.send_away(1)
        mlp_quarter(quarters[PAIR], gain, not last)
        yz.send_away(1)
        if last:
            g_out.forward()
        mlp_quarter(quarters[THREE], gain, not last)
        if not last:
            grad_into(p_out, gated_ref[...], dy_ref[...].reshape(h_ref.shape))
            g_out.send_both()
        grad_into(p_gate, dgate_ref[...].reshape(PAIR * seq, -1), h_ref)
        g_gate.send_both()
        if not last:
            g_out.forward()
        for s in mlp_sum:
            s.forward()
        for g in pending[1:]:
            g.gather()
        grad_into(p_lin, dlin_ref[...].reshape(PAIR * seq, -1), h_ref)
        g_lin.send_both()
        g_gate.forward()
        for copy in loads[layer, True]:
            copy.wait()
        for b in range(PAIR):
            h_ref[b * seq:(b + 1) * seq, :] = norm(x_ref[b], gain_a)
        g_lin.forward()
        add = key_add(mask_ref, 1 - z)
        for head in range(heads):
            cols = pl.ds(head * HEAD, HEAD)
            bias_ref[head] = toeplitz(t_ref[head:head + 1, :], seq)
            e, total = exp_scores(q_ref[1 - z, :, cols], k_ref[1 - z, :, cols], bias_ref[head], add)
            bias_ref[head] = e * (1.0 / total)
        for g in pending:
            g.close()
        g_out.finish()
        dg_m = 0.0
        for piece in range(PAIR):
            rows = pl.ds(piece * PIECE, PIECE)
            for c, s in enumerate(mlp_sum):
                d_x, dg = norm_back(s.total(piece), x1_ref[z, y, c, rows, :], gain)
                dm_ref[z, y, c, rows, :] = (d_x + dy_ref[z, y, c, rows, :].astype(F32)).astype(BF16)
                s.publish(piece)
                dg_m = dg_m + jnp.sum(dg, axis=0, keepdims=True)
        for s in mlp_sum:
            s.gather()
        g_gate.finish()
        for s in mlp_sum:
            s.close()
        if not last:
            loads[0, False] = fetch(0, False)

        if last:
            def region(q, c, piece):
                return dx_ref.at[:, q[0], q[1], c, pl.ds(piece * SMALLS, SMALLS)]
        else:
            def region(q, c, piece):
                return dy_ref.at[q[0], q[1], c, pl.ds(piece * PIECE, PIECE)]
        zy, yz = attn_sum = colours(part, near, far, region, send.at[layer, PAIR:FOUR], recv.at[layer, PAIR:FOUR], ids, z, y, PAIR)

        def pick(ref, offset, size, q):
            pieces = [ref[q[0], pl.ds(pl.multiple_of(j * FOUR * deep + q[1] * PAIR * deep + offset, half), size), :] for j in range(across)]
            return pieces[0] if across == 1 else jnp.concatenate(pieces, axis=0)

        def attn_quarter(q):
            total = sum(dot(pick(d, 0, PAIR * deep, q), w[...], NT) for d, w in [(dq_ref, wq_ref), (dk_ref, wk_ref), (dv_ref, wv_ref)])
            total = total.reshape(across, PAIR, PAIR, half, width)
            for c in range(PAIR):
                for piece in range(PAIR):
                    part[q[0], q[1], c, pl.ds(piece * PIECE, PIECE), :] = total[:, c, piece].reshape(PIECE, width)

        attend(1 - z, True, not last, lambda: None)
        attn_quarter(quarters[0])
        zy.send_away(0)
        yz.send_away(0)
        attn_quarter(quarters[1])
        zy.send_away(1)
        grad_into(p_o, o_ref[...].reshape(PAIR * seq, -1), dm_ref[...].reshape(PAIR * seq, width))
        g_o.send_both()
        g_lin.finish()
        g_out.gather()
        attend(z, False, False, g_o.forward)
        attn_quarter(quarters[PAIR])
        yz.send_away(1)
        attn_quarter(quarters[THREE])
        for g, p, d in [(g_q, p_q, dq_ref), (g_k, p_k, dk_ref), (g_v, p_v, dv_ref)]:
            grad_into(p, h_ref[...], d[...].reshape(PAIR * seq, -1))
            g.send_both()
        for s in attn_sum:
            s.forward()
        for g in [g_q, g_k, g_v]:
            g.forward()
        if not last:
            for copy in loads[0, False]:
                copy.wait()
            for i in range(FOUR):
                h2 = norm(x1_ref[i // PAIR, i % PAIR].reshape(ROWS, -1), gm_ref[0:1, :])
                gated_ref[i * ROWS:(i + 1) * ROWS, :] = (gelu_parts(dot(h2, wg_ref[...], NT))[0] * dot(h2, wl_ref[...], NT)).astype(BF16)
        g_gate.gather()
        g_lin.gather()
        g_o.finish()
        dg_a = 0.0
        moves = {}
        for piece in range(PAIR):
            for c, s in enumerate(attn_sum):
                rows = pl.ds(piece * half, half)
                d_x, dg = norm_back(s.total(piece), pick(x_ref, c * deep + piece * half, half, (z, y)), gain_a)
                dg_a = dg_a + jnp.sum(dg, axis=0, keepdims=True)
                if last:
                    at = pl.ds(pl.multiple_of(y * PAIR * deep + c * deep + piece * half, half), half)
                    res = jnp.concatenate([dm_ref[z, j // PAIR, j % PAIR, at, :] for j in range(FOUR)], axis=0)
                else:
                    res = dm_ref[z, y, c, rows, :]
                d_x = (d_x + res.astype(F32)).astype(BF16)
                if last:
                    own_ref[c, piece] = d_x.reshape(across, half, width)
                    dx_ref[cp, z, y, c, rows, :] = own_ref[c, piece, cp]
                    moves[c, piece] = [remote(own_ref.at[c, piece, ids[name]['cp']], dx_ref.at[cp, z, y, c, rows], msend.at[c, piece, i], mrecv.at[c, piece, i], ids[name])
                                       for i, name in enumerate(['x', 'xc', 'core'])]
                else:
                    dy_ref[z, y, c, rows, :] = d_x
                    s.publish(piece)
        acc_small[0, PAIR - PAIR * layer:THREE - PAIR * layer, :] = dg_a
        acc_small[0, THREE - PAIR * layer:FOUR - PAIR * layer, :] = dg_m
        if not last:
            loads[0, True] = fetch(0, True)
            for s in attn_sum:
                s.gather()
            for g in [g_q, g_k, g_v]:
                g.finish()
            for s in attn_sum + [g_out, g_gate, g_lin]:
                s.close()
            pending = [g_o, g_q, g_k, g_v]

    acc_small[0, FOUR:EIGHT, :] = jnp.zeros((FOUR, width), F32)
    acc_small[0, EIGHT:12, :] = dt_ref[0:FOUR, :]
    acc_small[0, 12:SMALLS, :] = jnp.zeros((FOUR, width), F32)
    smalls = []

    def small_start(i):
        rows = pl.ds(0, SMALLS if i < PAIR else EIGHT)
        smalls.append(remote(acc_small.at[i, rows], got_small.at[i, rows], csend.at[i], crecv.at[i], ids[['x', 'core', 'y', 'z'][i]]))

    def small_end(i):
        rows = pl.ds(0, SMALLS if i < PAIR else EIGHT)
        smalls[i].wait_recv()
        acc_small[i + 1, rows, :] = acc_small[i, rows, :] + got_small[i, rows, :]

    small_start(0)
    for piece in range(PAIR):
        for c, s in enumerate(attn_sum):
            for copy in moves[c, piece]:
                copy.wait_recv()
            s.publish(piece)
    g_q.finish()
    small_end(0)
    small_start(1)
    g_k.finish()
    small_end(1)
    small_start(PAIR)
    g_v.finish()
    for s in attn_sum:
        s.gather()
    small_end(PAIR)
    small_start(THREE)
    for g in [g_o, g_q, g_k, g_v]:
        g.gather()
    small_end(THREE)
    small_out[0:EIGHT, :] = acc_small[FOUR, 0:EIGHT, :]
    small_out[EIGHT:SMALLS, :] = acc_small[PAIR, EIGHT:SMALLS, :]
    for copy in smalls + sum(moves.values(), []):
        copy.wait_send()
    for s in attn_sum + grads:
        s.close()


def backward(x1s, dy, xs, heads, gains_a, gains_m, wg_t, wl_t, w_out, w_q, w_k, w_v, w_o, table, mask):
    seq, width, cols = 512, w_q.shape[1], w_q.shape[PAIR]
    ff = w_out.shape[1]
    rows = PAIR * seq
    dma = pltpu.SemaphoreType.DMA
    blocks = (PAIR, PAIR, PAIR, BLOCK, width)
    flat = (PAIR, seq, width)
    stacks = [wg_t, wl_t, w_out, w_q, w_k, w_v, w_o]
    operands = stacks + [a.reshape(blocks) for a in x1s] + [dy.reshape(blocks)] + [a.reshape(flat) for a in xs]
    operands += [h.reshape(PAIR, PAIR, seq, cols) for h in heads] + [gains_a, gains_m, table, mask]
    grads = [(ff // FOUR, width)] * THREE + [(cols // FOUR, width)] + [(width // FOUR, cols)] * THREE
    out_shape = [jax.ShapeDtypeStruct((FOUR, PAIR, PAIR, PAIR, 32, width), BF16), jax.ShapeDtypeStruct((SMALLS, width), F32)]
    out_shape += [jax.ShapeDtypeStruct((PAIR, FOUR) + g, BF16) for g in grads]
    scratch = [pltpu.VMEM(w.shape[1:], BF16) for w in stacks]
    scratch += [pltpu.VMEM(blocks, BF16)] * PAIR + [pltpu.VMEM(flat, BF16)] + [pltpu.VMEM((PAIR, seq, cols), BF16)] * FOUR + [dma((PAIR, PAIR, 9))]
    scratch += sum_scratch(0, blocks[THREE:]) + [pltpu.VMEM(blocks, BF16), pltpu.VMEM((rows, width), BF16), pltpu.VMEM((rows, ff), BF16)] + [pltpu.VMEM((PAIR, seq, ff), BF16)] * PAIR
    scratch += [pltpu.VMEM((table.shape[0], seq, seq), F32), pltpu.VMEM((EIGHT, PAIR * seq), F32)]
    for g in grads:
        scratch += [pltpu.VMEM((FOUR,) + g, F32), pltpu.VMEM((PAIR,) + g, F32), pltpu.VMEM(g, F32), pltpu.VMEM(g, BF16)]
    scratch += [dma((PAIR, FOUR, 10)), dma((PAIR, FOUR, 10)), dma((PAIR, GRADS, 6)), dma((PAIR, GRADS, 6)), dma((PAIR, GRADS))]
    scratch += [pltpu.VMEM((PAIR, PAIR, FOUR, SMALLS, width), BF16), pltpu.VMEM((5, SMALLS, width), F32), pltpu.VMEM((FOUR, SMALLS, width), F32)]
    scratch += [dma((PAIR, PAIR, THREE)), dma((PAIR, PAIR, THREE)), dma((FOUR,)), dma((FOUR,))]
    return pl.pallas_call(
        functools.partial(backward_kernel, seq),
        out_shape=out_shape, in_specs=any_specs(SMALLS) + vmem_specs(FOUR), out_specs=vmem_specs(PAIR) + any_specs(GRADS),
        scratch_shapes=scratch,
        compiler_params=pltpu.CompilerParams(collective_id=1, has_side_effects=True, vmem_limit_bytes=67043328),
        cost_estimate=pl.CostEstimate(flops=40 << 30, bytes_accessed=96 << MIB, transcendentals=0),
        name="backward",
    )(*operands)


def finish_kernel(seq, *refs):
    refs = list(refs)
    n = (len(refs) - 6) // THREE
    small_ref, ins = refs[0], refs[1:1 + n]
    outs, (ga_ref, gm_ref, bias_ref) = refs[1 + n:1 + PAIR * n], refs[1 + PAIR * n:FOUR + PAIR * n]
    bufs, (rsem, wsem) = refs[FOUR + PAIR * n:FOUR + THREE * n], refs[FOUR + THREE * n:6 + THREE * n]
    reads, writes = [], []
    for i in range(n):
        for h in range(PAIR):
            reads.append(pltpu.make_async_copy(ins[i].at[h], bufs[i].at[h], rsem.at[i, h]))
            writes.append(pltpu.make_async_copy(bufs[i].at[h], outs[i].at[h], wsem.at[i, h]))
    for copy in reads:
        copy.start()
    ga_ref[0:1, :], ga_ref[1:PAIR, :] = small_ref[PAIR:THREE, :], small_ref[0:1, :]
    gm_ref[0:1, :], gm_ref[1:PAIR, :] = small_ref[THREE:FOUR, :], small_ref[1:PAIR, :]
    shape = (32, PAIR * seq)
    column = lax.broadcasted_iota(jnp.int32, shape, 1)
    hit = (rel_bucket(column - seq) == lax.broadcasted_iota(jnp.int32, shape, 0)) & (column > 0)
    bias_ref[...] = lax.dot_general(small_ref[EIGHT:12, :], jnp.where(hit, 1.0, 0.0).astype(F32), NT, precision=lax.Precision.HIGHEST, preferred_element_type=F32)
    for read, write in zip(reads, writes):
        read.wait()
        write.start()
    for copy in writes:
        copy.wait()


def finish(small, arrays):
    dma = pltpu.SemaphoreType.DMA
    n = len(arrays)
    shapes = [jax.ShapeDtypeStruct(a.shape, a.dtype) for a in arrays]
    outs = pl.pallas_call(
        functools.partial(finish_kernel, 512),
        out_shape=shapes + [jax.ShapeDtypeStruct((PAIR, small.shape[1]), F32)] * PAIR + [jax.ShapeDtypeStruct((FOUR, 32), F32)],
        in_specs=vmem_specs(1) + any_specs(n), out_specs=any_specs(n) + vmem_specs(THREE),
        scratch_shapes=[pltpu.VMEM(a.shape, a.dtype) for a in arrays] + [dma((n, PAIR)), dma((n, PAIR))],
        compiler_params=pltpu.CompilerParams(vmem_limit_bytes=67043328),
        cost_estimate=pl.CostEstimate(flops=1 << MIB, bytes_accessed=32 << MIB, transcendentals=0),
        name="finish",
    )(small, *arrays)
    return outs[:n], *outs[n:]


def vmem_specs(n):
    return [pl.BlockSpec(memory_space=pltpu.VMEM)] * n


def solution(mesh):
    seq_spec = P(None, 'cp', None)
    col_spec = P(None, None, 'tp')
    row_spec = P(None, 'tp', None)
    weight_specs = (P(), P(), col_spec, col_spec, col_spec, row_spec, col_spec, col_spec, row_spec)

    def local_program(x_in, d_y, key_mask, rel_bias, g_attn, g_mlp, w_q, w_k, w_v, w_o, w_gate, w_lin, w_out):
        width = x_in.shape[2]
        wg_t, wl_t = jnp.swapaxes(w_gate, 1, 2), jnp.swapaxes(w_lin, 1, 2)
        x0, a0, x1, a1, dy, q, k, v, o, mask, table = forward(x_in, d_y, key_mask, g_attn, g_mlp, w_q, w_k, w_v, w_o, wg_t, wl_t, w_out, rel_bias.T)

        outs = backward((a0, a1), dy, (x0, x1), (q, k, v, o), g_attn, g_mlp, wg_t, wl_t, w_out, w_q, w_k, w_v, w_o, table, mask)
        arrays = [outs[0].reshape((2, -1) + outs[0].shape[1:])] + list(outs[2:])
        moved, d_ga, d_gm, d_bias = finish(outs[1], arrays)
        d_x = moved[0]
        d_out, d_gate, d_lin, d_wo, d_wq, d_wk, d_wv = [g.reshape(2, -1, g.shape[-1]) for g in moved[1:]]
        d_gate, d_lin = jnp.swapaxes(d_gate, 1, 2), jnp.swapaxes(d_lin, 1, 2)
        d_bias = d_bias.T

        return d_x.reshape(x_in.shape), d_bias, d_ga, d_gm, d_wq, d_wk, d_wv, d_wo, d_gate, d_lin, d_out

    return jax.shard_map(local_program, mesh=mesh, in_specs=(seq_spec, seq_spec, P(None, 'cp'), P(None, 'tp')) + weight_specs, out_specs=(seq_spec, P(None, 'tp')) + weight_specs, check_vma=False)
```
